32 devices in a mesh: row: 4 (over y, x), col: 8 (over z, core).
Axes of the slice: x: 2, y: 2, z: 4, core: 2. Of those that a mesh axis runs over, the one named last changes fastest.
Arguments:
- cam_jac: bfloat16 [2, 2, 6, 512, 1024], P(None, None, None, ('row', 'col')), may hold values from -0.09375 to 0.09375
- pt_jac: bfloat16 [2, 2, 3, 512, 1024], P(None, None, None, ('row', 'col')), may hold values from -6 to 6
- resid: bfloat16 [2, 2, 512, 1024], P(None, None, ('row', 'col')), may hold values from -6 to 6
- partner: int32 [512, 1024], P(('row', 'col')), may hold values from 0 to 511, as said below
- count: int32 [512], P(('row', 'col')), may hold values from 512 to 1024
- tile_map: int32 [512], replicated, may hold values from 0 to 511, as said below
Outputs:
- coupling: bfloat16 [6, 6, 512, 512], P(None, None, 'row', 'col')
- camera_update: float32 [6, 512], P(None, 'row')
- residual: float32 [6, 512], P(None, 'row')
The draws below stay inside these ranges and needn't reach their ends.
Inputs may be any that keep to these rules, and one draw needn't show every extreme that they name: partner[a, t] is never a. `tile_map`: a permutation of the tile positions; of the 16 consecutive scenes of each device, exactly 4 have positions in each block of 128 consecutive positions.
All inputs are finite; a program needn't handle non-finite values.
Results may differ from the reference program's by a relative error of at most 0.0015.
Values may be sent and summed in bfloat16 or wider, within the bound.
No kernel may reach another device: no remote copies, remote signals or barrier semaphores. Data moves between devices by JAX's collectives and lax.ppermute only.
A program may use at most 64 MiB of HBM per device.

```python
import jax
import jax.numpy as jnp
from jax import lax

SCN_DEV = 16
PTS = 1024
ITERS = 3
SCENES = 512
TILE_ROWS = 128
PER_GROUP = 4


def draw_partner(key, part):
    scene_ids = jnp.arange(SCENES, dtype=jnp.int32)[:, None]
    offsets = jax.random.randint(key, (SCENES, PTS), 1, SCENES, dtype=jnp.int32)
    return ((scene_ids + offsets) % SCENES).astype(jnp.int32)


def draw_tile_map(key, part):
    devices = SCENES // SCN_DEV
    groups = SCENES // TILE_ROWS
    first_key, second_key = jax.random.split(jax.random.fold_in(key, 7))
    scores = jax.random.randint(first_key, (devices, SCN_DEV), 0, 1 << 14, dtype=jnp.int32) * SCN_DEV
    scores = scores + jnp.arange(SCN_DEV, dtype=jnp.int32)[None, :]
    local_rank = jnp.argsort(jnp.argsort(scores, axis=1), axis=1).astype(jnp.int32)
    group_of = local_rank // PER_GROUP
    within = jnp.arange(devices, dtype=jnp.int32)[:, None] * PER_GROUP + local_rank % PER_GROUP
    scores_two = jax.random.randint(second_key, (groups, TILE_ROWS), 0, 1 << 14, dtype=jnp.int32) * TILE_ROWS
    scores_two = scores_two + jnp.arange(TILE_ROWS, dtype=jnp.int32)[None, :]
    shuffle = jnp.argsort(jnp.argsort(scores_two, axis=1), axis=1).astype(jnp.int32)
    tiles = group_of * TILE_ROWS + shuffle[group_of, within]
    return tiles.reshape(SCENES).astype(jnp.int32)


def place_ends(values, own_key, least, top_value):
    longest = values.shape.index(max(values.shape))
    spots = []
    for shift in (0, 1):
        where = [jax.random.randint(jax.random.fold_in(own_key, axis), (), 0, length) for axis, length in enumerate(values.shape)]
        where[longest] = (where[longest] + shift) % values.shape[longest]
        spots.append(tuple(where))
    return values.at[spots[0]].set(least).at[spots[1]].set(top_value)


def steps_of(key, extent, pieces, least, top_value):
    factor_of, own = 1.0, jax.random.fold_in(key, 6)
    for position, parts in pieces:
        heights = jnp.exp(jax.random.uniform(jax.random.fold_in(own, position), (parts,), jnp.float32, least / len(pieces), top_value / len(pieces)))
        factor_of = factor_of * jnp.repeat(heights, extent[position] // parts).reshape([-1 if axis == position else 1 for axis in range(len(extent))])
    return factor_of


def bell_draw(key, shape, scale, most, pieces=(), held_as=jnp.bfloat16):
    entries = scale * jax.random.normal(key, shape, jnp.float32)
    if pieces:
        entries = entries * steps_of(key, shape, pieces, -0.22, 0.18)
    return jnp.clip(entries, -most, most).astype(held_as)


def setup_inputs(seed: int = 0) -> dict:
    key_of = jax.random.split(jax.random.key(seed), 7)
    cam_jac = bell_draw(key_of[0], (2, 2, 6, SCENES, PTS), (4 * PTS) ** -0.5, 0.09375, ((3, 32),))
    pt_jac = bell_draw(key_of[1], (2, 2, 3, SCENES, PTS), 1.0, 6.0, ((3, 32),))
    resid = bell_draw(key_of[2], (2, 2, SCENES, PTS), 1.0, 6.0, ((2, 32),))
    partner = draw_partner(jax.random.fold_in(key_of[6], 71), 0)
    count = place_ends(jax.random.randint(key_of[4], (SCENES,), PTS // 2, PTS + 1), jax.random.fold_in(key_of[4], 1), PTS // 2, PTS).astype(jnp.int32)
    tile_map = draw_tile_map(jax.random.fold_in(key_of[6], 71), 0)
    return dict(cam_jac=cam_jac, pt_jac=pt_jac, resid=resid, partner=partner, count=count, tile_map=tile_map)


CAMERA_DAMPING = 1.0
POINT_DAMPING = 1.0


def cross_product(first_vec, second_vec):
    return jnp.stack([first_vec[1] * second_vec[2] - first_vec[2] * second_vec[1],
                      first_vec[2] * second_vec[0] - first_vec[0] * second_vec[2],
                      first_vec[0] * second_vec[1] - first_vec[1] * second_vec[0]], axis=0)


def point_terms(camera, points_jac, errors):
    camera = camera.astype(jnp.float32)
    points_jac = points_jac.astype(jnp.float32)
    errors = errors.astype(jnp.float32)
    own_jac, other_jac = camera[0], camera[1]
    own_point, other_point = points_jac[0], points_jac[1]
    own_error, other_error = errors[0], errors[1]
    point_hessian = jnp.sum(own_point[:, :, None] * own_point[:, None, :], axis=0)
    point_hessian = point_hessian + jnp.sum(other_point[:, :, None] * other_point[:, None, :], axis=0)
    point_hessian = point_hessian + POINT_DAMPING * jnp.eye(3, dtype=jnp.float32)[:, :, None, None]
    first_row, second_row, third_row = point_hessian[0], point_hessian[1], point_hessian[2]
    cofactor_first = cross_product(second_row, third_row)
    cofactor_second = cross_product(third_row, first_row)
    cofactor_third = cross_product(first_row, second_row)
    determinant = jnp.sum(first_row * cofactor_first, axis=0)
    inverse = jnp.stack([cofactor_first, cofactor_second, cofactor_third], axis=1) / determinant
    w_own = jnp.sum(own_jac[:, :, None] * own_point[:, None, :], axis=0)
    w_other = jnp.sum(other_jac[:, :, None] * other_point[:, None, :], axis=0)
    point_rhs = -(jnp.sum(own_point * own_error[:, None], axis=0) + jnp.sum(other_point * other_error[:, None], axis=0))
    own_vi = jnp.sum(w_own[:, :, None] * inverse[None, :, :], axis=1)
    other_vi = jnp.sum(w_other[:, :, None] * inverse[None, :, :], axis=1)
    diag_own = jnp.sum(own_jac[:, :, None] * own_jac[:, None, :], axis=0) - jnp.sum(own_vi[:, None, :] * w_own[None, :, :], axis=2)
    diag_other = jnp.sum(other_jac[:, :, None] * other_jac[:, None, :], axis=0) - jnp.sum(other_vi[:, None, :] * w_other[None, :, :], axis=2)
    link = -jnp.sum(own_vi[:, None, :] * w_other[None, :, :], axis=2)
    grad_own = -jnp.sum(own_jac * own_error[:, None], axis=0) - jnp.sum(own_vi * point_rhs[None], axis=1)
    grad_other = -jnp.sum(other_jac * other_error[:, None], axis=0) - jnp.sum(other_vi * point_rhs[None], axis=1)
    return diag_own, diag_other, link, grad_own, grad_other


def reference(cam_jac, pt_jac, resid, partner, count, tile_map):
    blocks = SCENES // SCN_DEV

    def split_scenes(array):
        lead = array.shape[:-2]
        shaped = array.reshape(lead + (blocks, SCN_DEV, PTS))
        return jnp.moveaxis(shaped, len(lead), 0)

    inputs = (split_scenes(cam_jac), split_scenes(pt_jac), split_scenes(resid),
              partner.reshape(blocks, SCN_DEV, PTS), count.reshape(blocks, SCN_DEV),
              tile_map.reshape(blocks, SCN_DEV))

    def add_block(sums_so_far, block):
        coupling_flat, diag_sum, grad_sum = sums_so_far
        camera, points_jac, errors, partner_block, count_block, tile_block = block
        diag_own, diag_other, link, grad_own, grad_other = point_terms(camera, points_jac, errors)
        active = (jnp.arange(PTS, dtype=jnp.int32)[None, :] < count_block[:, None]).astype(jnp.float32)
        tile_other = jnp.take(tile_map, partner_block).astype(jnp.int32).reshape(-1)
        tile_own = jnp.broadcast_to(tile_block[:, None], (SCN_DEV, PTS)).astype(jnp.int32).reshape(-1)
        target = tile_own * SCENES + tile_other
        coupling_flat = coupling_flat.at[:, target].add((link * active).reshape(36, -1))
        diag_sum = diag_sum.at[:, tile_own].add((diag_own * active).reshape(36, -1))
        diag_sum = diag_sum.at[:, tile_other].add((diag_other * active).reshape(36, -1))
        grad_sum = grad_sum.at[:, tile_own].add((grad_own * active).reshape(6, -1))
        grad_sum = grad_sum.at[:, tile_other].add((grad_other * active).reshape(6, -1))
        return (coupling_flat, diag_sum, grad_sum), None

    start = (jnp.zeros((36, SCENES * SCENES), jnp.float32), jnp.zeros((36, SCENES), jnp.float32),
             jnp.zeros((6, SCENES), jnp.float32))
    (coupling_flat, diag_sum, grad_sum), unused = lax.scan(add_block, start, inputs)
    coupling = coupling_flat.reshape(6, 6, SCENES, SCENES).astype(jnp.bfloat16)
    coupling_wide = coupling.astype(jnp.float32)
    diag_blocks = diag_sum.reshape(6, 6, SCENES)

    def operator(vector):
        result = CAMERA_DAMPING * vector
        result = result + jnp.einsum('xyi,yi->xi', diag_blocks, vector, precision=lax.Precision.HIGHEST)
        result = result + jnp.einsum('xyij,yj->xi', coupling_wide, vector, precision=lax.Precision.HIGHEST)
        result = result + jnp.einsum('xyij,xi->yj', coupling_wide, vector, precision=lax.Precision.HIGHEST)
        return result

    solution = jnp.zeros((6, SCENES), jnp.float32)
    remainder = grad_sum
    direction = grad_sum
    norm_now = jnp.sum(remainder * remainder)
    for iteration in range(ITERS):
        product_vec = operator(direction)
        step_size = norm_now / jnp.sum(direction * product_vec)
        solution = solution + step_size * direction
        remainder = remainder - step_size * product_vec
        norm_next = jnp.sum(remainder * remainder)
        direction = remainder + (norm_next / norm_now) * direction
        norm_now = norm_next
    return coupling, solution, remainder
```

```python
import jax
import jax.numpy as jnp
from jax import lax
from jax.experimental import pallas as pl
from jax.experimental.pallas import tpu as pltpu
from jax.sharding import PartitionSpec as P

ITERS = 3
CAMERA_DAMPING = 1.0
POINT_DAMPING = 1.0
AXES = ("row", "col")
LANES = 128
HALF = 64
F32 = jnp.float32
BF16 = jnp.bfloat16
PAIRS = [(x, y) for x in range(6) for y in range(x, 6)]
CONTRACT_LAST = (((1,), (1,)), ((), ()))


def iota(shape, dim):
    return lax.broadcasted_iota(jnp.int32, shape, dim)


def split_two(value):
    high = value.astype(BF16)
    low = (value - high.astype(F32)).astype(BF16)
    return high, low


def dot2(left, right):
    a, b = left
    c, d = right
    return a * c + b * d


def point_values(ja, jb, pa, pb, ea, eb, live):
    one = POINT_DAMPING
    hess = {}
    for x in range(3):
        for y in range(x, 3):
            h = pa[0][x] * pa[0][y] + pa[1][x] * pa[1][y]
            h = h + (pb[0][x] * pb[0][y] + pb[1][x] * pb[1][y])
            hess[x, y] = h + one if x == y else h
    a, b, c = hess[0, 0], hess[0, 1], hess[0, 2]
    d, e, f = hess[1, 1], hess[1, 2], hess[2, 2]
    c00 = d * f - e * e
    c01 = c * e - b * f
    c02 = b * e - c * d
    c11 = a * f - c * c
    c12 = b * c - a * e
    c22 = a * d - b * b
    det = a * c00 + b * c01 + c * c02
    inv = 1.0 / det
    vi = [[c00 * inv, c01 * inv, c02 * inv], [None, c11 * inv, c12 * inv], [None, None, c22 * inv]]
    vi[1][0], vi[2][0], vi[2][1] = vi[0][1], vi[0][2], vi[1][2]
    q = [
        -((pa[0][k] * ea[0] + pa[1][k] * ea[1]) + (pb[0][k] * eb[0] + pb[1][k] * eb[1]))
        for k in range(3)
    ]
    viq = [vi[k][0] * q[0] + vi[k][1] * q[1] + vi[k][2] * q[2] for k in range(3)]

    def times_vi(p):
        return [
            [p[m][0] * vi[0][k] + p[m][1] * vi[1][k] + p[m][2] * vi[2][k] for k in range(3)]
            for m in range(2)
        ]

    def inner(left, right):
        return left[0] * right[0] + left[1] * right[1] + left[2] * right[2]

    def keep(value):
        return jnp.where(live, value, 0.0)

    av = times_vi(pa)
    bv = times_vi(pb)
    m_ab = [[keep(-inner(av[m], pb[k])) for k in range(2)] for m in range(2)]
    g_aa = [keep(1.0 - inner(av[0], pa[0])), keep(-inner(av[0], pa[1])), keep(1.0 - inner(av[1], pa[1]))]
    g_bb = [keep(1.0 - inner(bv[0], pb[0])), keep(-inner(bv[0], pb[1])), keep(1.0 - inner(bv[1], pb[1]))]
    h_a = [keep(-(ea[m] + inner(pa[m], viq))) for m in range(2)]
    h_b = [keep(-(eb[m] + inner(pb[m], viq))) for m in range(2)]

    mj = [[m_ab[m][0] * jb[0][y] + m_ab[m][1] * jb[1][y] for y in range(6)] for m in range(2)]
    link = {}
    for x in range(6):
        for y in range(6):
            link[x, y] = ja[0][x] * mj[0][y] + ja[1][x] * mj[1][y]

    def diagonal(j, g):
        gj = [
            [g[0] * j[0][y] + g[1] * j[1][y] for y in range(6)],
            [g[1] * j[0][y] + g[2] * j[1][y] for y in range(6)],
        ]
        return [j[0][x] * gj[0][y] + j[1][x] * gj[1][y] for x, y in PAIRS]

    diag_own = diagonal(ja, g_aa)
    diag_other = diagonal(jb, g_bb)
    grad_own = [ja[0][x] * h_a[0] + ja[1][x] * h_a[1] for x in range(6)]
    grad_other = [jb[0][x] * h_b[0] + jb[1][x] * h_b[1] for x in range(6)]
    return diag_own, diag_other, link, grad_own, grad_other


def assemble_kernel(
    row_count, col_count, cam_ref, pt_ref, res_ref, partner_ref, map_ref, count_sm, map_sm, send_ref,
    vals_ref, own_ref, acc_ref, links_ref, flat_ref, extra_ref, perm_ref,
):
    scn = partner_ref.shape[0]
    points = partner_ref.shape[1]
    scenes = map_ref.shape[1]
    per_group = scn // row_count
    device = lax.axis_index("row") * col_count + lax.axis_index("col")
    slab = (scn, LANES)

    sub = iota(slab, 0)
    counts = jnp.zeros(slab, jnp.int32)
    for s in range(scn):
        counts = jnp.where(sub == s, count_sm[s], counts)
    own_ref[...] = jnp.zeros_like(own_ref)
    acc_ref[...] = jnp.zeros_like(acc_ref)
    vals_ref[:, pl.ds(63 * scn, scn), :] = jnp.zeros((points // LANES, scn, LANES), F32)

    def slab_step(step, carry):
        lanes = pl.ds(pl.multiple_of(step * LANES, LANES), LANES)

        def get(ref, *where):
            return ref[where + (slice(None), lanes)].astype(F32)

        ja = [[get(cam_ref, 0, m, x) for x in range(6)] for m in range(2)]
        jb = [[get(cam_ref, 1, m, x) for x in range(6)] for m in range(2)]
        pa = [[get(pt_ref, 0, m, x) for x in range(3)] for m in range(2)]
        pb = [[get(pt_ref, 1, m, x) for x in range(3)] for m in range(2)]
        ea = [get(res_ref, 0, m) for m in range(2)]
        eb = [get(res_ref, 1, m) for m in range(2)]
        live = (iota(slab, 1) + step * LANES) < counts
        diag_own, diag_other, link, grad_own, grad_other = point_values(ja, jb, pa, pb, ea, eb, live)

        def put(q, value):
            vals_ref[step, pl.ds(q * scn, scn), :] = value

        def put_own(q, value):
            own_ref[pl.ds(q * scn, scn), :] += value

        for x in range(3):
            for y in range(6):
                put(x * 6 + y, link[x, y])
                put(24 + x * 6 + y, link[x + 3, y])
        for x in range(6):
            put(18 + x, grad_other[x])
            put_own(2 + x, grad_own[x])
        for q in range(21):
            put(42 + q, diag_other[q])
            put_own(10 + q, diag_own[q])
        return carry

    lax.fori_loop(0, points // LANES, slab_step, 0)

    spots = iota((scenes, points), 0)

    def scene_step(s, carry):
        values = jnp.concatenate(
            [vals_ref.at[t][pl.ds(s, 64, stride=scn), :] for t in range(points // LANES)], axis=1
        )
        high, low = split_two(values)
        left = jnp.concatenate([high, low], axis=0)
        onehot = jnp.where(spots == partner_ref[pl.ds(s, 1), :], 1.0, 0.0).astype(BF16)
        both = lax.dot_general(left, onehot, CONTRACT_LAST, preferred_element_type=F32)
        total = both[:64] + both[64:]
        acc_ref[...] += total
        mine = map_sm[device * scn + s]
        rank = jnp.int32(0)
        for other in range(scn):
            rank = rank + (map_sm[device * scn + other] < mine).astype(jnp.int32)
        links_ref[pl.ds(pl.multiple_of(rank * 48, 16), 48), :] = total[:48].astype(BF16)
        return carry

    lax.fori_loop(0, scn, scene_step, 0)

    lane = iota((32, LANES), 1)
    own = jnp.zeros((32, LANES), F32)
    for s in range(scn):
        column = jnp.sum(own_ref[pl.ds(s, 32, stride=scn), :], axis=1, keepdims=True)
        own = own + jnp.where(lane == s, column, 0.0)
    start = device * scn
    own = pltpu.roll(own, lax.rem(start, LANES), 1)
    tile_at = lax.div(start, LANES)
    for t in range(scenes // LANES):
        cols = pl.ds(t * LANES, LANES)
        whole = jnp.concatenate([acc_ref[16:24, cols], acc_ref[40:64, cols]], axis=0)
        whole = whole + jnp.where(tile_at == t, own, 0.0)
        high, low = split_two(whole)
        flat_ref[0:32, cols] = high.astype(F32)
        flat_ref[32:64, cols] = low.astype(F32)
    per_col = -(-21 // col_count)
    extra_ref[...] = jnp.zeros_like(extra_ref)
    for c in range(col_count):
        for i in range(per_col):
            q = c * per_col + i
            if q < 21:
                extra_ref[c * 8 + 2 + i : c * 8 + 3 + i, :] = flat_ref[10 + q : 11 + q, :]
                extra_ref[c * 8 + 5 + i : c * 8 + 6 + i, :] = flat_ref[42 + q : 43 + q, :]
    base = col_count * 8
    extra_ref[base : base + 8, :] = flat_ref[0:8, :]
    extra_ref[base + 8 : base + 16, :] = flat_ref[32:40, :]

    onto = jnp.where(iota((scenes, scenes), 0) == map_ref[...], 1.0, 0.0).astype(BF16)
    left = jnp.concatenate([links_ref[...], extra_ref[...].astype(BF16)], axis=0)
    perm_ref[...] = lax.dot_general(left, onto, CONTRACT_LAST, preferred_element_type=F32)

    top = scn * 48
    first = iota((8, LANES), 1) < HALF
    keep_rows = iota((8, LANES), 0) < 2
    first24 = iota((24, LANES), 1) < HALF

    def merge(low_part, high_part, mask):
        even = jnp.where(mask, low_part, pltpu.roll(high_part, HALF, 1))
        odd = jnp.where(mask, pltpu.roll(low_part, HALF, 1), high_part)
        return even, odd

    for j in range(col_count // 2):
        cols = pl.ds(j * LANES, LANES)
        grad_cols = merge(
            perm_ref[top + base : top + base + 8, cols],
            perm_ref[top + base + 8 : top + base + 16, cols],
            first,
        )
        for r in range(row_count):
            rows = pl.ds(r * LANES, LANES)
            grad_high = perm_ref[top + base : top + base + 8, rows]
            grad_low = perm_ref[top + base + 8 : top + base + 16, rows]
            for slot in range(per_group):
                at = (r * per_group + slot) * 48
                pieces = merge(perm_ref[at : at + 24, cols], perm_ref[at + 24 : at + 48, cols], first24)
                for k in range(2):
                    c = 2 * j + k
                    if slot == 0:
                        extra = grad_high
                    elif slot == 1:
                        extra = grad_low
                    elif slot == 2:
                        extra = grad_cols[k]
                    else:
                        extra = perm_ref[top + c * 8 : top + c * 8 + 8, rows]
                    tail = jnp.where(keep_rows, pieces[k][16:24], extra)
                    block = jnp.concatenate([pieces[k][0:16], tail], axis=0)
                    send_ref[r * col_count + c, slot * 24 : slot * 24 + 24, :] = block.astype(BF16)


def exact_dot(left, right, dims):
    return lax.dot_general(
        left, right, dims, precision=lax.Precision.HIGHEST, preferred_element_type=F32
    )


def tile_matvec(coupling_ref, own_ref, rows_part, cols_part, pair_sm, rows_ref):
    tile_rows = coupling_ref.shape[1]
    first = iota((8, LANES), 1) < HALF
    which = iota((8, LANES), 0)
    spread = []
    for x in range(3):
        choose = ((first & (which == x)) | (~first & (which == x + 3))).astype(F32)
        spread.append(exact_dot(rows_part, choose, (((0,), (0,)), ((), ()))))
    forward = [jnp.zeros((tile_rows, LANES), F32) for _ in range(3)]
    backward = []
    for y in range(6):
        line = cols_part[y : y + 1, :]
        total = jnp.zeros((8, LANES), F32)
        for x in range(3):
            block = coupling_ref[x * 6 + y].astype(F32)
            forward[x] = forward[x] + block * line
            weighted = block * spread[x]
            total = total + jnp.sum(weighted.reshape(tile_rows // 8, 8, LANES), axis=0)
        line_out = jnp.sum(total, axis=0, keepdims=True)
        backward.append(line_out + pltpu.roll(line_out, HALF, 1))
    out = jnp.zeros((8, LANES), F32)
    for x in range(3):
        pick = ((first & (which == x)) | (~first & (which == x + 3))).astype(F32)
        out = out + exact_dot(pick, forward[x], CONTRACT_LAST)
    rows_ref[...] = rows_part
    col = lax.axis_index("col")
    per_col = -(-21 // lax.axis_size("col"))
    for i in range(per_col):
        q = jnp.minimum(col * per_col + i, 20)
        x = pair_sm[q]
        y = pair_sm[32 + q]
        weight = own_ref[i : i + 1, :]
        at_x = rows_ref[pl.ds(x, 1), :] * weight
        at_y = rows_ref[pl.ds(y, 1), :] * weight
        out = out + jnp.where(which == x, at_y, 0.0)
        out = out + jnp.where((which == y) & (x != y), at_x, 0.0)
    return out, backward


def write_partials(out, backward, line, part_ref):
    first = iota((1, LANES), 1) < HALF
    rows = [out[x : x + 1, :] for x in range(6)]
    rows += [jnp.where(first, backward[y], backward[y + 3]) for y in range(3)]
    if line is not None:
        rows.append(line)
    for n in range(part_ref.shape[0]):
        for k, row in enumerate(rows):
            part_ref[n, :, k * LANES : (k + 1) * LANES] = row


def first_kernel(
    row_count, col_count, got_ref, map_ref, pair_sm, tile_ref, dense_ref, own_ref, part_ref,
    wide_ref, rows_ref,
):
    devices = got_ref.shape[0]
    scenes = map_ref.shape[1]
    scn = scenes // devices
    per_group = scn // row_count
    tile_rows = scenes // row_count
    row = lax.axis_index("row")
    tiles = jnp.concatenate(
        [map_ref[:, t * LANES : (t + 1) * LANES] for t in range(scenes // LANES)], axis=0
    )
    groups = scenes // LANES
    place = iota((groups, LANES), 1) % scn
    rank = jnp.zeros((groups, LANES), jnp.int32)
    for shift in range(1, scn):
        before = pltpu.roll(tiles, shift, 1)
        after = pltpu.roll(tiles, LANES - shift, 1)
        rank = rank + ((before < tiles) & (place >= shift)).astype(jnp.int32)
        rank = rank + ((after < tiles) & (place + shift < scn)).astype(jnp.int32)
    scene_id = iota((groups, LANES), 0) * LANES + iota((groups, LANES), 1)
    slot_at = (scene_id // scn) * per_group + rank % per_group
    local = tiles - row * tile_rows
    slot_at = jnp.where((local >= 0) & (local < tile_rows), slot_at, -1)
    select = jnp.zeros((tile_rows, tile_rows), F32)
    for t in range(groups):
        to_row = jnp.where(iota((tile_rows, LANES), 0) == local[t : t + 1, :], 1.0, 0.0).astype(BF16)
        from_slot = jnp.where(iota((tile_rows, LANES), 0) == slot_at[t : t + 1, :], 1.0, 0.0).astype(BF16)
        select = select + lax.dot_general(to_row, from_slot, CONTRACT_LAST, preferred_element_type=F32)
    select = select.astype(BF16)

    for n in range(devices):
        wide_ref[pl.ds(n * 96, 96), :] = got_ref[n].astype(F32)
    for k in range(18):
        picked = wide_ref[pl.ds(k, tile_rows, stride=24), :].astype(BF16)
        block = jnp.dot(select, picked, preferred_element_type=F32)
        dense_ref[k] = block.astype(BF16)
        tile_ref[k] = block[:, :HALF].astype(BF16)
        tile_ref[k + 18] = pltpu.roll(block, HALF, 1)[:, :HALF].astype(BF16)
    extras = []
    for slot in range(per_group):
        total = wide_ref[slot * 24 + 16 : slot * 24 + 24, :]
        for n in range(1, devices):
            total = total + wide_ref[n * 96 + slot * 24 + 16 : n * 96 + slot * 24 + 24, :]
        extras.append(pltpu.roll(total, 6, 0))
    used = iota((8, LANES), 0) < 6
    rows_part = jnp.where(used, extras[0] + extras[1], 0.0)
    cols_part = jnp.where(used, extras[2] + pltpu.roll(extras[2], HALF, 1), 0.0)
    own_ref[...] = extras[3] + pltpu.roll(extras[3], 5, 0)
    out, backward = tile_matvec(dense_ref, own_ref, rows_part, cols_part, pair_sm, rows_ref)
    rows_ref[...] = rows_part
    line = rows_ref[pl.ds(jnp.minimum(lax.axis_index("col"), 5), 1), :]
    write_partials(out, backward, line, part_ref)


def gather_image(row_count, col_count, got_ref, image_ref):
    first = iota((1, LANES), 1) < HALF
    side = 6 * LANES
    cols = []
    for c in range(col_count):
        total = got_ref[c, :, side : side + 3 * LANES]
        for r in range(1, row_count):
            total = total + got_ref[r * col_count + c, :, side : side + 3 * LANES]
        cols.append(total)
    for r in range(row_count):
        total = got_ref[r * col_count, :, 0:side]
        for c in range(1, col_count):
            total = total + got_ref[r * col_count + c, :, 0:side]
        image_ref[r] = jnp.zeros((8, LANES), F32)
        for t in range(3):
            left = cols[2 * r][:, t * LANES : (t + 1) * LANES]
            right = cols[2 * r + 1][:, t * LANES : (t + 1) * LANES]
            low = jnp.where(first, left, pltpu.roll(right, HALF, 1))
            high = jnp.where(first, pltpu.roll(left, HALF, 1), right)
            image_ref[r, t : t + 1, :] = total[:, t * LANES : (t + 1) * LANES] + low
            image_ref[r, t + 3 : t + 4, :] = total[:, (t + 3) * LANES : (t + 4) * LANES] + high


def inner_all(left, right):
    return jnp.sum(jnp.sum(left * right, axis=0), keepdims=True)


def step_kernel(
    row_count, col_count, begin, got_ref, dense_ref, own_ref, state_ref, pair_sm, next_ref, part_ref,
    image_ref, rows_ref,
):
    gather_image(row_count, col_count, got_ref, image_ref)
    if begin:
        for r in range(row_count):
            next_ref[1, r] = jnp.zeros((8, LANES), F32)
            for x in range(6):
                next_ref[1, r, x : x + 1, :] = got_ref[r * col_count + x, :, 9 * LANES : 10 * LANES]
        remainder = next_ref[1]
        direction = remainder
        answer = jnp.zeros_like(remainder)
    else:
        answer, remainder, direction = state_ref[0], state_ref[1], state_ref[2]
    norm_now = inner_all(remainder, remainder)
    image = CAMERA_DAMPING * direction + image_ref[...]
    alpha = norm_now / inner_all(direction, image)
    answer = answer + alpha * direction
    remainder = remainder - alpha * image
    norm_next = inner_all(remainder, remainder)
    direction = remainder + norm_next / norm_now * direction
    next_ref[0] = answer
    next_ref[1] = remainder
    next_ref[2] = direction
    col = lax.axis_index("col")
    rows_part = next_ref[2, lax.axis_index("row")]
    wide = next_ref[2, lax.div(col, 2)]
    turned = pltpu.roll(wide, HALF, 1)
    first = (iota((8, LANES), 1) < HALF).astype(jnp.int32)
    cols_part = jnp.where(first == 1 - lax.rem(col, 2), wide, turned)
    out, backward = tile_matvec(dense_ref, own_ref, rows_part, cols_part, pair_sm, rows_ref)
    write_partials(out, backward, None, part_ref)


def last_kernel(row_count, col_count, got_ref, state_ref, answer_ref, remainder_ref, image_ref):
    gather_image(row_count, col_count, got_ref, image_ref)
    remainder, direction = state_ref[1], state_ref[2]
    norm_now = inner_all(remainder, remainder)
    image_ref[...] = CAMERA_DAMPING * direction + image_ref[...]
    alpha = norm_now / inner_all(direction, image_ref[...])
    row = lax.axis_index("row")
    answer_ref[...] = (state_ref[0, row] + alpha * state_ref[2, row])[:6]
    remainder_ref[...] = (state_ref[1, row] - alpha * image_ref[row])[:6]


def vmem():
    return pl.BlockSpec(memory_space=pltpu.VMEM)


def smem():
    return pl.BlockSpec(memory_space=pltpu.SMEM)


def small_limit(mib):
    return pltpu.CompilerParams(vmem_limit_bytes=mib << 20)


def packed_shards(cam_jac, pt_jac, resid, partner, count, tile_map):
    row_count = lax.axis_size("row")
    col_count = lax.axis_size("col")
    devices = row_count * col_count
    scenes = tile_map.shape[0]
    scn, points = partner.shape
    map_row = tile_map.reshape(1, scenes)
    pairs = jnp.asarray([p[0] for p in PAIRS] + [0] * 11 + [p[1] for p in PAIRS] + [0] * 11, jnp.int32)

    def bind(kernel, *fixed):
        def run(*refs):
            return kernel(row_count, col_count, *fixed, *refs)

        return run

    extra_rows = col_count * 8 + 16
    send = pl.pallas_call(
        bind(assemble_kernel),
        out_shape=jax.ShapeDtypeStruct((devices, 96, LANES), BF16),
        in_specs=[vmem()] * 5 + [smem()] * 2,
        out_specs=vmem(),
        scratch_shapes=[
            pltpu.VMEM((points // LANES, 64 * scn, LANES), F32),
            pltpu.VMEM((32 * scn, LANES), F32),
            pltpu.VMEM((64, scenes), F32),
            pltpu.VMEM((48 * scn, scenes), BF16),
            pltpu.VMEM((64, scenes), F32),
            pltpu.VMEM((extra_rows, scenes), F32),
            pltpu.VMEM((48 * scn + extra_rows, scenes), F32),
        ],
        compiler_params=small_limit(36),
        name="assemble",
    )(cam_jac, pt_jac, resid, partner, map_row, count, tile_map)
    got = lax.all_to_all(send, AXES, 0, 0, tiled=True)
    tile_rows = scenes // row_count
    tile, dense, own, part = pl.pallas_call(
        bind(first_kernel),
        out_shape=(
            jax.ShapeDtypeStruct((36, tile_rows, HALF), BF16),
            jax.ShapeDtypeStruct((18, tile_rows, LANES), BF16),
            jax.ShapeDtypeStruct((8, LANES), F32),
            jax.ShapeDtypeStruct((devices, 1, 10 * LANES), F32),
        ),
        in_specs=[vmem(), vmem(), smem()],
        out_specs=(vmem(),) * 4,
        scratch_shapes=[pltpu.VMEM((devices * 96, LANES), F32), pltpu.VMEM((8, LANES), F32)],
        compiler_params=small_limit(16),
        name="first",
    )(got, map_row, pairs)
    state = jnp.zeros((3, row_count, 8, LANES), F32)
    for turn in range(ITERS - 1):
        got = lax.all_to_all(part, AXES, 0, 0, tiled=True)
        state, part = pl.pallas_call(
            bind(step_kernel, turn == 0),
            out_shape=(
                jax.ShapeDtypeStruct((3, row_count, 8, LANES), F32),
                jax.ShapeDtypeStruct((devices, 1, 9 * LANES), F32),
            ),
            in_specs=[vmem()] * 4 + [smem()],
            out_specs=(vmem(),) * 2,
            scratch_shapes=[pltpu.VMEM((row_count, 8, LANES), F32), pltpu.VMEM((8, LANES), F32)],
            compiler_params=small_limit(8),
            name="step",
        )(got, dense, own, state, pairs)
    got = lax.all_to_all(part, AXES, 0, 0, tiled=True)
    answer, remainder = pl.pallas_call(
        bind(last_kernel),
        out_shape=(jax.ShapeDtypeStruct((6, tile_rows), F32),) * 2,
        in_specs=[vmem()] * 2,
        out_specs=(vmem(),) * 2,
        scratch_shapes=[pltpu.VMEM((row_count, 8, LANES), F32)],
        compiler_params=small_limit(4),
        name="last",
    )(got, state)
    return tile.reshape(6, 6, tile_rows, HALF), answer, remainder


def cross_product(first_vec, second_vec):
    return jnp.stack(
        [
            first_vec[1] * second_vec[2] - first_vec[2] * second_vec[1],
            first_vec[2] * second_vec[0] - first_vec[0] * second_vec[2],
            first_vec[0] * second_vec[1] - first_vec[1] * second_vec[0],
        ],
        axis=0,
    )


def point_terms(camera, points_jac, errors):
    camera = camera.astype(jnp.float32)
    points_jac = points_jac.astype(jnp.float32)
    errors = errors.astype(jnp.float32)
    own_jac, other_jac = (camera[0], camera[1])
    own_point, other_point = (points_jac[0], points_jac[1])
    own_error, other_error = (errors[0], errors[1])
    point_hessian = jnp.sum(own_point[:, :, None] * own_point[:, None, :], axis=0)
    point_hessian = point_hessian + jnp.sum(
        other_point[:, :, None] * other_point[:, None, :], axis=0
    )
    point_hessian = point_hessian + POINT_DAMPING * jnp.eye(3, dtype=jnp.float32)[:, :, None, None]
    first_row, second_row, third_row = (point_hessian[0], point_hessian[1], point_hessian[2])
    cofactor_first = cross_product(second_row, third_row)
    cofactor_second = cross_product(third_row, first_row)
    cofactor_third = cross_product(first_row, second_row)
    determinant = jnp.sum(first_row * cofactor_first, axis=0)
    inverse = jnp.stack([cofactor_first, cofactor_second, cofactor_third], axis=1) / determinant
    w_own = jnp.sum(own_jac[:, :, None] * own_point[:, None, :], axis=0)
    w_other = jnp.sum(other_jac[:, :, None] * other_point[:, None, :], axis=0)
    point_rhs = -(
        jnp.sum(own_point * own_error[:, None], axis=0)
        + jnp.sum(other_point * other_error[:, None], axis=0)
    )
    own_vi = jnp.sum(w_own[:, :, None] * inverse[None, :, :], axis=1)
    other_vi = jnp.sum(w_other[:, :, None] * inverse[None, :, :], axis=1)
    diag_own = jnp.sum(own_jac[:, :, None] * own_jac[:, None, :], axis=0) - jnp.sum(
        own_vi[:, None, :] * w_own[None, :, :], axis=2
    )
    diag_other = jnp.sum(other_jac[:, :, None] * other_jac[:, None, :], axis=0) - jnp.sum(
        other_vi[:, None, :] * w_other[None, :, :], axis=2
    )
    link = -jnp.sum(own_vi[:, None, :] * w_other[None, :, :], axis=2)
    grad_own = -jnp.sum(own_jac * own_error[:, None], axis=0) - jnp.sum(
        own_vi * point_rhs[None], axis=1
    )
    grad_other = -jnp.sum(other_jac * other_error[:, None], axis=0) - jnp.sum(
        other_vi * point_rhs[None], axis=1
    )
    return (diag_own, diag_other, link, grad_own, grad_other)


def conjugate_steps(right_side, apply_operator, inner_product):
    solution = jnp.zeros_like(right_side)
    remainder = right_side
    direction = right_side
    norm_now = inner_product(remainder, remainder)
    for iteration in range(ITERS):
        product_vec = apply_operator(direction)
        step_size = norm_now / inner_product(direction, product_vec)
        solution = solution + step_size * direction
        remainder = remainder - step_size * product_vec
        norm_next = inner_product(remainder, remainder)
        direction = remainder + norm_next / norm_now * direction
        norm_now = norm_next
    return (solution, remainder)


def plain_shards(cam_jac, pt_jac, resid, partner, count, tile_map):
    row_count = lax.axis_size("row")
    col_count = lax.axis_size("col")
    scenes = tile_map.shape[0]
    scn_local = partner.shape[0]
    points = partner.shape[1]
    tile_rows = scenes // row_count
    tile_cols = scenes // col_count
    per_group = scn_local // row_count
    row_index = lax.axis_index("row")
    col_index = lax.axis_index("col")
    device = row_index * col_count + col_index
    positions = jnp.arange(scenes, dtype=jnp.int32)
    tile_own = lax.dynamic_slice_in_dim(tile_map, device * scn_local, scn_local)
    local_rank = jnp.sum((tile_own[None, :] < tile_own[:, None]).astype(jnp.int32), axis=1)
    active = (jnp.arange(points, dtype=jnp.int32)[None, :] < count[:, None]).astype(jnp.float32)
    diag_own, diag_other, link, grad_own, grad_other = point_terms(cam_jac, pt_jac, resid)
    values = (
        jnp.concatenate(
            [
                link.reshape(36, scn_local, points),
                diag_other.reshape(36, scn_local, points),
                grad_other,
            ],
            axis=0,
        )
        * active[None]
    )
    values = jnp.moveaxis(values, 1, 0)

    def scene_sums(item):
        scene_values, scene_partner = item
        hits = scene_partner[:, None] == positions[None, :]
        tile_other = jnp.sum(jnp.where(hits, tile_map[None, :], 0), axis=1)
        onehot = (tile_other[:, None] == positions[None, :]).astype(jnp.float32)
        return jnp.dot(
            scene_values,
            onehot,
            precision=lax.Precision.HIGHEST,
            preferred_element_type=jnp.float32,
        )

    per_scene = lax.map(scene_sums, (values, partner))
    link_rows = per_scene[:, :36, :]
    other_sum = jnp.sum(per_scene[:, 36:, :], axis=0)
    ordering = (local_rank[None, :] == jnp.arange(scn_local, dtype=jnp.int32)[:, None]).astype(
        jnp.float32
    )
    panel = jnp.einsum("rs,sxc->xrc", ordering, link_rows, precision=lax.Precision.HIGHEST)
    panel = panel.reshape(36, row_count, per_group, col_count, tile_cols).transpose(0, 1, 3, 2, 4)
    panel_short = panel.astype(jnp.bfloat16)
    own_onehot = (tile_own[:, None] == positions[None, :]).astype(jnp.float32)
    own_diag = jnp.sum(diag_own * active, axis=-1).reshape(36, scn_local)
    own_grad = jnp.sum(grad_own * active, axis=-1)
    own_both = jnp.concatenate([own_diag, own_grad], axis=0)
    own_spread = jnp.dot(
        own_both, own_onehot, precision=lax.Precision.HIGHEST, preferred_element_type=jnp.float32
    )
    both_part = own_spread + other_sum
    diag_part = both_part[:36]
    grad_part = both_part[36:]
    shaped = panel_short.reshape(36, row_count * col_count, per_group, tile_cols)
    received = lax.all_to_all(shaped, ("row", "col"), split_axis=1, concat_axis=1, tiled=True)
    received = received.reshape(36, tile_rows, tile_cols)
    diag_all, grad_all = lax.psum((diag_part, grad_part), ("row", "col"))
    row_start = row_index * tile_rows
    col_start = col_index * tile_cols
    devices = scenes // scn_local
    tiles_grid = tile_map.reshape(devices, scn_local)
    inblock = (tiles_grid >= row_start) & (tiles_grid < row_start + tile_rows)
    lower = (tiles_grid[:, None, :] < tiles_grid[:, :, None]) & inblock[:, None, :]
    within_all = jnp.sum(lower.astype(jnp.int32), axis=2)
    slot_from = (jnp.arange(devices, dtype=jnp.int32)[:, None] * per_group + within_all).reshape(-1)
    slot_to = (tiles_grid - row_start).reshape(-1)
    slots = jnp.arange(tile_rows, dtype=jnp.int32)
    to_table = ((slot_to[:, None] == slots[None, :]) & inblock.reshape(-1)[:, None]).astype(
        jnp.bfloat16
    )
    from_table = (slot_from[:, None] == slots[None, :]).astype(jnp.bfloat16)
    selection = jnp.dot(to_table.T, from_table, preferred_element_type=jnp.float32).astype(
        jnp.bfloat16
    )
    coupling_tile = jnp.einsum(
        "pk,xkc->xpc", selection, received, preferred_element_type=jnp.float32
    )
    coupling_tile = coupling_tile.astype(jnp.bfloat16).reshape(6, 6, tile_rows, tile_cols)
    coupling_wide = coupling_tile.astype(jnp.float32)
    zero_at = row_index * 0

    def tile_products(rows_part, cols_part):
        forward = jnp.einsum(
            "xyij,yj->xi", coupling_wide, cols_part, precision=lax.Precision.HIGHEST
        )
        backward = jnp.einsum(
            "xyij,xi->yj", coupling_wide, rows_part, precision=lax.Precision.HIGHEST
        )
        empty = jnp.zeros((6, scenes), jnp.float32)
        spread = lax.dynamic_update_slice(empty, forward, (zero_at, row_start))
        spread = spread + lax.dynamic_update_slice(empty, backward, (zero_at, col_start))
        return lax.psum(spread, ("row", "col"))

    diag_blocks = diag_all.reshape(6, 6, scenes)

    def apply_full(direction):
        rows_part = lax.dynamic_slice_in_dim(direction, row_start, tile_rows, 1)
        cols_part = lax.dynamic_slice_in_dim(direction, col_start, tile_cols, 1)
        summed = tile_products(rows_part, cols_part)
        result = CAMERA_DAMPING * direction
        result = result + jnp.einsum(
            "xyi,yi->xi", diag_blocks, direction, precision=lax.Precision.HIGHEST
        )
        return result + summed

    def inner_full(first_vec, second_vec):
        return jnp.sum(first_vec * second_vec)

    whole_solution, whole_remainder = conjugate_steps(grad_all, apply_full, inner_full)
    solution = lax.dynamic_slice_in_dim(whole_solution, row_start, tile_rows, 1)
    remainder = lax.dynamic_slice_in_dim(whole_remainder, row_start, tile_rows, 1)
    return (coupling_tile, solution, remainder)


def shards(cam_jac, pt_jac, resid, partner, count, tile_map):
    row_count = lax.axis_size("row")
    col_count = lax.axis_size("col")
    scenes = tile_map.shape[0]
    scn, points = partner.shape
    packs = (
        scenes == col_count * HALF
        and scenes == row_count * LANES
        and scn == row_count * 4
        and LANES % scn == 0
        and points % LANES == 0
        and col_count >= 7
    )
    run = packed_shards if packs else plain_shards
    return run(cam_jac, pt_jac, resid, partner, count, tile_map)


def solution(mesh):
    return jax.shard_map(
        shards,
        mesh=mesh,
        in_specs=(
            P(None, None, None, AXES, None),
            P(None, None, None, AXES, None),
            P(None, None, AXES, None),
            P(AXES, None),
            P(AXES),
            P(),
        ),
        out_specs=(P(None, None, "row", "col"), P(None, "row"), P(None, "row")),
        check_vma=False,
    )
```

```python
import jax
import jax.numpy as jnp
from jax import lax
from jax.experimental import pallas as pl
from jax.experimental.pallas import tpu as pltpu
from jax.sharding import PartitionSpec as P

ITERS = 3
CAMERA_DAMPING = 1.0
POINT_DAMPING = 1.0
AXES = ("row", "col")
LANES = 128
HALF = 64
F32 = jnp.float32
BF16 = jnp.bfloat16
PAIRS = [(x, y) for x in range(6) for y in range(x, 6)]
CONTRACT_LAST = (((1,), (1,)), ((), ()))


def iota(shape, dim):
    return lax.broadcasted_iota(jnp.int32, shape, dim)


def split_two(value):
    high = value.astype(BF16)
    low = (value - high.astype(F32)).astype(BF16)
    return high, low


def point_values(ja, jb, pa, pb, ea, eb, live):
    one = POINT_DAMPING
    hess = {}
    for x in range(3):
        for y in range(x, 3):
            h = pa[0][x] * pa[0][y] + pa[1][x] * pa[1][y]
            h = h + (pb[0][x] * pb[0][y] + pb[1][x] * pb[1][y])
            hess[x, y] = h + one if x == y else h
    a, b, c = hess[0, 0], hess[0, 1], hess[0, 2]
    d, e, f = hess[1, 1], hess[1, 2], hess[2, 2]
    c00 = d * f - e * e
    c01 = c * e - b * f
    c02 = b * e - c * d
    c11 = a * f - c * c
    c12 = b * c - a * e
    c22 = a * d - b * b
    det = a * c00 + b * c01 + c * c02
    inv = 1.0 / det
    vi = [[c00 * inv, c01 * inv, c02 * inv], [None, c11 * inv, c12 * inv], [None, None, c22 * inv]]
    vi[1][0], vi[2][0], vi[2][1] = vi[0][1], vi[0][2], vi[1][2]
    q = [
        -((pa[0][k] * ea[0] + pa[1][k] * ea[1]) + (pb[0][k] * eb[0] + pb[1][k] * eb[1]))
        for k in range(3)
    ]
    viq = [vi[k][0] * q[0] + vi[k][1] * q[1] + vi[k][2] * q[2] for k in range(3)]

    def times_vi(p):
        return [
            [p[m][0] * vi[0][k] + p[m][1] * vi[1][k] + p[m][2] * vi[2][k] for k in range(3)]
            for m in range(2)
        ]

    def inner(left, right):
        return left[0] * right[0] + left[1] * right[1] + left[2] * right[2]

    def keep(value):
        return jnp.where(live, value, 0.0)

    av = times_vi(pa)
    bv = times_vi(pb)
    m_ab = [[keep(-inner(av[m], pb[k])) for k in range(2)] for m in range(2)]
    g_aa = [keep(1.0 - inner(av[0], pa[0])), keep(-inner(av[0], pa[1])), keep(1.0 - inner(av[1], pa[1]))]
    g_bb = [keep(1.0 - inner(bv[0], pb[0])), keep(-inner(bv[0], pb[1])), keep(1.0 - inner(bv[1], pb[1]))]
    h_a = [keep(-(ea[m] + inner(pa[m], viq))) for m in range(2)]
    h_b = [keep(-(eb[m] + inner(pb[m], viq))) for m in range(2)]

    mj = [[m_ab[m][0] * jb[0][y] + m_ab[m][1] * jb[1][y] for y in range(6)] for m in range(2)]
    link = {}
    for x in range(6):
        for y in range(6):
            link[x, y] = ja[0][x] * mj[0][y] + ja[1][x] * mj[1][y]

    def diagonal(j, g):
        gj = [
            [g[0] * j[0][y] + g[1] * j[1][y] for y in range(6)],
            [g[1] * j[0][y] + g[2] * j[1][y] for y in range(6)],
        ]
        return [j[0][x] * gj[0][y] + j[1][x] * gj[1][y] for x, y in PAIRS]

    diag_own = diagonal(ja, g_aa)
    diag_other = diagonal(jb, g_bb)
    grad_own = [ja[0][x] * h_a[0] + ja[1][x] * h_a[1] for x in range(6)]
    grad_other = [jb[0][x] * h_b[0] + jb[1][x] * h_b[1] for x in range(6)]
    return diag_own, diag_other, link, grad_own, grad_other


def assemble_kernel(
    row_count, col_count, cam_in, pt_in, res_in, partner_in, row_in, count_in, map_in, send_ref,
    vals_ref, own_ref, acc_ref, links_ref, flat_ref, extra_ref, perm_ref,
    cam_ref, pt_ref, res_ref, partner_ref, map_ref, count_sm, map_sm, slab_sem, whole_sem,
):
    scn = partner_ref.shape[0]
    points = partner_ref.shape[1]
    scenes = map_ref.shape[1]
    wholes = [
        pltpu.make_async_copy(source, target, whole_sem.at[k])
        for k, (source, target) in enumerate(
            [(count_in, count_sm), (map_in, map_sm), (row_in, map_ref), (partner_in, partner_ref)]
        )
    ]

    def slab_copies(step):
        lanes = pl.ds(pl.multiple_of(step * LANES, LANES), LANES)
        return [
            pltpu.make_async_copy(
                source.at[..., lanes], target.at[..., lanes], slab_sem.at[k, step]
            )
            for k, (source, target) in enumerate([(cam_in, cam_ref), (pt_in, pt_ref), (res_in, res_ref)])
        ]

    wholes[0].start()
    for step in range(points // LANES):
        for copy in slab_copies(step):
            copy.start()
    for copy in wholes[1:]:
        copy.start()
    per_group = scn // row_count
    device = lax.axis_index("row") * col_count + lax.axis_index("col")
    slab = (scn, LANES)

    own_ref[...] = jnp.zeros_like(own_ref)
    acc_ref[...] = jnp.zeros_like(acc_ref)
    extra_ref[...] = jnp.zeros_like(extra_ref)
    vals_ref[:, pl.ds(63 * scn, scn), :] = jnp.zeros((points // LANES, scn, LANES), F32)

    wholes[0].wait()
    sub = iota(slab, 0)
    counts = jnp.zeros(slab, jnp.int32)
    for s in range(scn):
        counts = jnp.where(sub == s, count_sm[s], counts)

    def slab_step(step, carry):
        for copy in slab_copies(step):
            copy.wait()
        lanes = pl.ds(pl.multiple_of(step * LANES, LANES), LANES)

        def get(ref, *where):
            return ref[where + (slice(None), lanes)].astype(F32)

        ja = [[get(cam_ref, 0, m, x) for x in range(6)] for m in range(2)]
        jb = [[get(cam_ref, 1, m, x) for x in range(6)] for m in range(2)]
        pa = [[get(pt_ref, 0, m, x) for x in range(3)] for m in range(2)]
        pb = [[get(pt_ref, 1, m, x) for x in range(3)] for m in range(2)]
        ea = [get(res_ref, 0, m) for m in range(2)]
        eb = [get(res_ref, 1, m) for m in range(2)]
        live = (iota(slab, 1) + step * LANES) < counts
        diag_own, diag_other, link, grad_own, grad_other = point_values(ja, jb, pa, pb, ea, eb, live)

        def put(q, value):
            vals_ref[step, pl.ds(q * scn, scn), :] = value

        def put_own(q, value):
            own_ref[pl.ds(q * scn, scn), :] += value

        for x in range(3):
            for y in range(6):
                put(x * 6 + y, link[x, y])
                put(24 + x * 6 + y, link[x + 3, y])
        for x in range(6):
            put(18 + x, grad_other[x])
            put_own(2 + x, grad_own[x])
        for q in range(21):
            put(42 + q, diag_other[q])
            put_own(10 + q, diag_own[q])
        return carry

    lax.fori_loop(0, points // LANES, slab_step, 0)

    for copy in wholes[1:]:
        copy.wait()
    spots = iota((scenes, points), 0)

    def scene_step(s, carry):
        values = jnp.concatenate(
            [vals_ref.at[t][pl.ds(s, 64, stride=scn), :] for t in range(points // LANES)], axis=1
        )
        high, low = split_two(values)
        left = jnp.concatenate([high, low], axis=0)
        onehot = jnp.where(spots == partner_ref[pl.ds(s, 1), :], 1.0, 0.0).astype(BF16)
        both = lax.dot_general(left, onehot, CONTRACT_LAST, preferred_element_type=F32)
        total = both[:64] + both[64:]
        acc_ref[...] += total
        mine = map_sm[device * scn + s]
        rank = jnp.int32(0)
        for other in range(scn):
            rank = rank + (map_sm[device * scn + other] < mine).astype(jnp.int32)
        links_ref[pl.ds(pl.multiple_of(rank * 48, 16), 48), :] = total[:48].astype(BF16)
        return carry

    lax.fori_loop(0, scn, scene_step, 0, unroll=4)

    lane = iota((32, LANES), 1)
    own = jnp.zeros((32, LANES), F32)
    for s in range(scn):
        column = jnp.sum(own_ref[pl.ds(s, 32, stride=scn), :], axis=1, keepdims=True)
        own = own + jnp.where(lane == s, column, 0.0)
    start = device * scn
    own = pltpu.roll(own, lax.rem(start, LANES), 1)
    tile_at = lax.div(start, LANES)
    for t in range(scenes // LANES):
        cols = pl.ds(t * LANES, LANES)
        whole = jnp.concatenate([acc_ref[16:24, cols], acc_ref[40:64, cols]], axis=0)
        whole = whole + jnp.where(tile_at == t, own, 0.0)
        high, low = split_two(whole)
        flat_ref[0:32, cols] = high.astype(F32)
        flat_ref[32:64, cols] = low.astype(F32)
    per_col = -(-21 // col_count)
    for c in range(col_count):
        for i in range(per_col):
            q = c * per_col + i
            if q < 21:
                extra_ref[c * 8 + 2 + i : c * 8 + 3 + i, :] = flat_ref[10 + q : 11 + q, :]
                extra_ref[c * 8 + 5 + i : c * 8 + 6 + i, :] = flat_ref[42 + q : 43 + q, :]
    base = col_count * 8
    extra_ref[base : base + 8, :] = flat_ref[0:8, :]
    extra_ref[base + 8 : base + 16, :] = flat_ref[32:40, :]

    onto = jnp.where(iota((scenes, scenes), 0) == map_ref[...], 1.0, 0.0).astype(BF16)
    left = jnp.concatenate([links_ref[...], extra_ref[...].astype(BF16)], axis=0)
    perm_ref[...] = lax.dot_general(left, onto, CONTRACT_LAST, preferred_element_type=F32)

    top = scn * 48
    first = iota((8, LANES), 1) < HALF
    keep_rows = iota((8, LANES), 0) < 2
    first24 = iota((24, LANES), 1) < HALF

    def merge(low_part, high_part, mask):
        even = jnp.where(mask, low_part, pltpu.roll(high_part, HALF, 1))
        odd = jnp.where(mask, pltpu.roll(low_part, HALF, 1), high_part)
        return even, odd

    for j in range(col_count // 2):
        cols = pl.ds(j * LANES, LANES)
        grad_cols = merge(
            perm_ref[top + base : top + base + 8, cols],
            perm_ref[top + base + 8 : top + base + 16, cols],
            first,
        )
        for r in range(row_count):
            rows = pl.ds(r * LANES, LANES)
            grad_high = perm_ref[top + base : top + base + 8, rows]
            grad_low = perm_ref[top + base + 8 : top + base + 16, rows]
            for slot in range(per_group):
                at = (r * per_group + slot) * 48
                pieces = merge(perm_ref[at : at + 24, cols], perm_ref[at + 24 : at + 48, cols], first24)
                for k in range(2):
                    c = 2 * j + k
                    if slot == 0:
                        extra = grad_high
                    elif slot == 1:
                        extra = grad_low
                    elif slot == 2:
                        extra = grad_cols[k]
                    else:
                        extra = perm_ref[top + c * 8 : top + c * 8 + 8, rows]
                    tail = jnp.where(keep_rows, pieces[k][16:24], extra)
                    block = jnp.concatenate([pieces[k][0:16], tail], axis=0)
                    send_ref[r * col_count + c, slot * 24 : slot * 24 + 24, :] = block.astype(BF16)


def tile_matvec(tile_ref, own_ref, rows_part, cols_part, pair_sm, rows_ref):
    which = iota((8, LANES), 0)
    turned = jnp.transpose(cols_part)[:HALF]
    forward = [jnp.zeros((8, LANES), F32) for _ in range(6)]
    backward = []
    for y in range(6):
        column = jnp.broadcast_to(turned[:, y : y + 1], (HALF, LANES))
        total = jnp.zeros((HALF, LANES), F32)
        for x in range(6):
            block = tile_ref[x * 6 + y].astype(F32)
            forward[x] = forward[x] + jnp.sum((block * column).reshape(HALF // 8, 8, LANES), axis=0)
            total = total + block * rows_part[x : x + 1, :]
        backward.append(total)
    sides = []
    for y in range(3):
        pair = jnp.concatenate([backward[y], backward[y + 3]], axis=0)
        sides.append(jnp.sum(jnp.transpose(pair), axis=0, keepdims=True))
    out = jnp.zeros((8, LANES), F32)
    for x in range(6):
        out = jnp.where(which == x, jnp.sum(forward[x], axis=0, keepdims=True), out)
    rows_ref[...] = rows_part
    col = lax.axis_index("col")
    per_col = -(-21 // lax.axis_size("col"))
    for i in range(per_col):
        q = jnp.minimum(col * per_col + i, 20)
        x = pair_sm[q]
        y = pair_sm[32 + q]
        weight = own_ref[i : i + 1, :]
        at_x = rows_ref[pl.ds(x, 1), :] * weight
        at_y = rows_ref[pl.ds(y, 1), :] * weight
        out = out + jnp.where(which == x, at_y, 0.0)
        out = out + jnp.where((which == y) & (x != y), at_x, 0.0)
    return out, sides


def write_partials(out, sides, line, part_ref):
    rows = [out[x : x + 1, :] for x in range(6)] + sides
    if line is not None:
        rows.append(line)
    for n in range(part_ref.shape[0]):
        for k, row in enumerate(rows):
            part_ref[n, :, k * LANES : (k + 1) * LANES] = row


def first_kernel(
    row_count, col_count, got_ref, map_ref, pair_sm, tile_ref, own_ref, part_ref, wide_ref, rows_ref,
):
    devices = got_ref.shape[0]
    scenes = map_ref.shape[1]
    scn = scenes // devices
    per_group = scn // row_count
    tile_rows = scenes // row_count
    row = lax.axis_index("row")
    tiles = jnp.concatenate(
        [map_ref[:, t * LANES : (t + 1) * LANES] for t in range(scenes // LANES)], axis=0
    )
    groups = scenes // LANES
    place = iota((groups, LANES), 1) % scn
    rank = jnp.zeros((groups, LANES), jnp.int32)
    for shift in range(1, scn):
        before = pltpu.roll(tiles, shift, 1)
        after = pltpu.roll(tiles, LANES - shift, 1)
        rank = rank + ((before < tiles) & (place >= shift)).astype(jnp.int32)
        rank = rank + ((after < tiles) & (place + shift < scn)).astype(jnp.int32)
    scene_id = iota((groups, LANES), 0) * LANES + iota((groups, LANES), 1)
    slot_at = (scene_id // scn) * per_group + rank % per_group
    local = tiles - row * tile_rows
    slot_at = jnp.where((local >= 0) & (local < tile_rows), slot_at, -1)
    select = jnp.zeros((tile_rows, tile_rows), F32)
    for t in range(groups):
        to_row = jnp.where(iota((tile_rows, LANES), 0) == local[t : t + 1, :], 1.0, 0.0).astype(BF16)
        from_slot = jnp.where(iota((tile_rows, LANES), 0) == slot_at[t : t + 1, :], 1.0, 0.0).astype(BF16)
        select = select + lax.dot_general(to_row, from_slot, CONTRACT_LAST, preferred_element_type=F32)
    select = select.astype(BF16)

    for n in range(devices):
        wide_ref[pl.ds(n * 96, 96), :] = got_ref[n].astype(F32)
    for k in range(18):
        picked = wide_ref[pl.ds(k, tile_rows, stride=24), :].astype(BF16)
        block = lax.dot_general(picked, select, (((0,), (1,)), ((), ())), preferred_element_type=F32)
        tile_ref[k] = block[:HALF].astype(BF16)
        tile_ref[k + 18] = block[HALF:].astype(BF16)
    extras = []
    for slot in range(per_group):
        total = wide_ref[slot * 24 + 16 : slot * 24 + 24, :]
        for n in range(1, devices):
            total = total + wide_ref[n * 96 + slot * 24 + 16 : n * 96 + slot * 24 + 24, :]
        extras.append(pltpu.roll(total, 6, 0))
    used = iota((8, LANES), 0) < 6
    rows_part = jnp.where(used, extras[0] + extras[1], 0.0)
    cols_part = jnp.where(used, extras[2] + pltpu.roll(extras[2], HALF, 1), 0.0)
    own_ref[...] = extras[3] + pltpu.roll(extras[3], 5, 0)
    out, sides = tile_matvec(tile_ref, own_ref, rows_part, cols_part, pair_sm, rows_ref)
    rows_ref[...] = rows_part
    line = rows_ref[pl.ds(jnp.minimum(lax.axis_index("col"), 5), 1), :]
    write_partials(out, sides, line, part_ref)


def gather_image(row_count, col_count, got_ref, image_ref):
    first = iota((1, LANES), 1) < HALF
    side = 6 * LANES
    cols = []
    for c in range(col_count):
        total = got_ref[c, :, side : side + 3 * LANES]
        for r in range(1, row_count):
            total = total + got_ref[r * col_count + c, :, side : side + 3 * LANES]
        cols.append(total)
    for r in range(row_count):
        total = got_ref[r * col_count, :, 0:side]
        for c in range(1, col_count):
            total = total + got_ref[r * col_count + c, :, 0:side]
        image_ref[r] = jnp.zeros((8, LANES), F32)
        for t in range(3):
            left = cols[2 * r][:, t * LANES : (t + 1) * LANES]
            right = cols[2 * r + 1][:, t * LANES : (t + 1) * LANES]
            low = jnp.where(first, left, pltpu.roll(right, HALF, 1))
            high = jnp.where(first, pltpu.roll(left, HALF, 1), right)
            image_ref[r, t : t + 1, :] = total[:, t * LANES : (t + 1) * LANES] + low
            image_ref[r, t + 3 : t + 4, :] = total[:, (t + 3) * LANES : (t + 4) * LANES] + high


def inner_all(left, right):
    return jnp.sum(jnp.sum(left * right, axis=0), keepdims=True)


def step_kernel(
    row_count, col_count, begin, got_ref, tile_ref, own_ref, state_ref, pair_sm, next_ref, part_ref,
    *rest,
):
    if begin:
        coupling_ref, image_ref, rows_ref, copy_sem = rest
        copy = pltpu.make_async_copy(tile_ref, coupling_ref, copy_sem)
        copy.start()
    else:
        image_ref, rows_ref = rest
    gather_image(row_count, col_count, got_ref, image_ref)
    if begin:
        for r in range(row_count):
            next_ref[1, r] = jnp.zeros((8, LANES), F32)
            for x in range(6):
                next_ref[1, r, x : x + 1, :] = got_ref[r * col_count + x, :, 9 * LANES : 10 * LANES]
        remainder = next_ref[1]
        direction = remainder
        answer = jnp.zeros_like(remainder)
    else:
        answer, remainder, direction = state_ref[0], state_ref[1], state_ref[2]
    norm_now = inner_all(remainder, remainder)
    image = CAMERA_DAMPING * direction + image_ref[...]
    alpha = norm_now / inner_all(direction, image)
    answer = answer + alpha * direction
    remainder = remainder - alpha * image
    norm_next = inner_all(remainder, remainder)
    direction = remainder + norm_next / norm_now * direction
    next_ref[0] = answer
    next_ref[1] = remainder
    next_ref[2] = direction
    col = lax.axis_index("col")
    rows_part = next_ref[2, lax.axis_index("row")]
    wide = next_ref[2, lax.div(col, 2)]
    turned = pltpu.roll(wide, HALF, 1)
    cols_part = jnp.where(iota((8, LANES), 0) * 0 == lax.rem(col, 2), wide, turned)
    out, sides = tile_matvec(tile_ref, own_ref, rows_part, cols_part, pair_sm, rows_ref)
    write_partials(out, sides, None, part_ref)
    if begin:
        copy.wait()


def last_kernel(row_count, col_count, got_ref, state_ref, answer_ref, remainder_ref, image_ref):
    gather_image(row_count, col_count, got_ref, image_ref)
    remainder, direction = state_ref[1], state_ref[2]
    norm_now = inner_all(remainder, remainder)
    image_ref[...] = CAMERA_DAMPING * direction + image_ref[...]
    alpha = norm_now / inner_all(direction, image_ref[...])
    row = lax.axis_index("row")
    answer_ref[...] = (state_ref[0, row] + alpha * state_ref[2, row])[:6]
    remainder_ref[...] = (state_ref[1, row] - alpha * image_ref[row])[:6]


def vmem():
    return pl.BlockSpec(memory_space=pltpu.VMEM)


def smem():
    return pl.BlockSpec(memory_space=pltpu.SMEM)


def hbm():
    return pl.BlockSpec(memory_space=pltpu.HBM)


def small_limit(mib):
    return pltpu.CompilerParams(vmem_limit_bytes=mib << 20)


def packed_shards(cam_jac, pt_jac, resid, partner, count, tile_map):
    row_count = lax.axis_size("row")
    col_count = lax.axis_size("col")
    devices = row_count * col_count
    scenes = tile_map.shape[0]
    scn, points = partner.shape
    map_row = tile_map.reshape(1, scenes)
    pairs = jnp.asarray([p[0] for p in PAIRS] + [0] * 11 + [p[1] for p in PAIRS] + [0] * 11, jnp.int32)

    def bind(kernel, *fixed):
        def run(*refs):
            return kernel(row_count, col_count, *fixed, *refs)

        return run

    extra_rows = col_count * 8 + 16
    send = pl.pallas_call(
        bind(assemble_kernel),
        out_shape=jax.ShapeDtypeStruct((devices, 96, LANES), BF16),
        in_specs=[hbm()] * 7,
        out_specs=vmem(),
        scratch_shapes=[
            pltpu.VMEM((points // LANES, 64 * scn, LANES), F32),
            pltpu.VMEM((32 * scn, LANES), F32),
            pltpu.VMEM((64, scenes), F32),
            pltpu.VMEM((48 * scn, scenes), BF16),
            pltpu.VMEM((64, scenes), F32),
            pltpu.VMEM((extra_rows, scenes), F32),
            pltpu.VMEM((48 * scn + extra_rows, scenes), F32),
            pltpu.VMEM(cam_jac.shape, BF16),
            pltpu.VMEM(pt_jac.shape, BF16),
            pltpu.VMEM(resid.shape, BF16),
            pltpu.VMEM(partner.shape, jnp.int32),
            pltpu.VMEM(map_row.shape, jnp.int32),
            pltpu.SMEM(count.shape, jnp.int32),
            pltpu.SMEM(tile_map.shape, jnp.int32),
            pltpu.SemaphoreType.DMA((3, points // LANES)),
            pltpu.SemaphoreType.DMA((4,)),
        ],
        compiler_params=small_limit(36),
        name="assemble",
    )(*[pltpu.with_memory_space_constraint(v, pltpu.HBM) for v in (cam_jac, pt_jac, resid, partner, map_row, count, tile_map)])
    got = lax.all_to_all(send, AXES, 0, 0, tiled=True)
    tile_rows = scenes // row_count
    tile, own, part = pl.pallas_call(
        bind(first_kernel),
        out_shape=(
            jax.ShapeDtypeStruct((36, HALF, tile_rows), BF16),
            jax.ShapeDtypeStruct((8, LANES), F32),
            jax.ShapeDtypeStruct((devices, 1, 10 * LANES), F32),
        ),
        in_specs=[vmem(), vmem(), smem()],
        out_specs=(vmem(),) * 3,
        scratch_shapes=[pltpu.VMEM((devices * 96, LANES), F32), pltpu.VMEM((8, LANES), F32)],
        compiler_params=small_limit(16),
        name="first",
    )(got, map_row, pairs)
    state = jnp.zeros((3, row_count, 8, LANES), F32)
    for turn in range(ITERS - 1):
        got = lax.all_to_all(part, AXES, 0, 0, tiled=True)
        begin = turn == 0
        outs = [
            jax.ShapeDtypeStruct((3, row_count, 8, LANES), F32),
            jax.ShapeDtypeStruct((devices, 1, 9 * LANES), F32),
        ]
        places = [vmem()] * 2
        scratch = [pltpu.VMEM((row_count, 8, LANES), F32), pltpu.VMEM((8, LANES), F32)]
        if begin:
            outs.append(jax.ShapeDtypeStruct(tile.shape, BF16))
            places.append(hbm())
            scratch.append(pltpu.SemaphoreType.DMA(()))
        state, part, *rest = pl.pallas_call(
            bind(step_kernel, begin),
            out_shape=outs,
            in_specs=[vmem()] * 4 + [smem()],
            out_specs=places,
            scratch_shapes=scratch,
            compiler_params=small_limit(8),
            name="step",
        )(got, tile, own, state, pairs)
        if begin:
            coupling = rest[0]
    got = lax.all_to_all(part, AXES, 0, 0, tiled=True)
    answer, remainder = pl.pallas_call(
        bind(last_kernel),
        out_shape=(jax.ShapeDtypeStruct((6, tile_rows), F32),) * 2,
        in_specs=[vmem()] * 2,
        out_specs=(vmem(),) * 2,
        scratch_shapes=[pltpu.VMEM((row_count, 8, LANES), F32)],
        compiler_params=small_limit(4),
        name="last",
    )(got, state)
    return jnp.swapaxes(coupling.reshape(6, 6, HALF, tile_rows), 2, 3), answer, remainder


def cross_product(first_vec, second_vec):
    return jnp.stack(
        [
            first_vec[1] * second_vec[2] - first_vec[2] * second_vec[1],
            first_vec[2] * second_vec[0] - first_vec[0] * second_vec[2],
            first_vec[0] * second_vec[1] - first_vec[1] * second_vec[0],
        ],
        axis=0,
    )


def point_terms(camera, points_jac, errors):
    camera = camera.astype(jnp.float32)
    points_jac = points_jac.astype(jnp.float32)
    errors = errors.astype(jnp.float32)
    own_jac, other_jac = (camera[0], camera[1])
    own_point, other_point = (points_jac[0], points_jac[1])
    own_error, other_error = (errors[0], errors[1])
    point_hessian = jnp.sum(own_point[:, :, None] * own_point[:, None, :], axis=0)
    point_hessian = point_hessian + jnp.sum(
        other_point[:, :, None] * other_point[:, None, :], axis=0
    )
    point_hessian = point_hessian + POINT_DAMPING * jnp.eye(3, dtype=jnp.float32)[:, :, None, None]
    first_row, second_row, third_row = (point_hessian[0], point_hessian[1], point_hessian[2])
    cofactor_first = cross_product(second_row, third_row)
    cofactor_second = cross_product(third_row, first_row)
    cofactor_third = cross_product(first_row, second_row)
    determinant = jnp.sum(first_row * cofactor_first, axis=0)
    inverse = jnp.stack([cofactor_first, cofactor_second, cofactor_third], axis=1) / determinant
    w_own = jnp.sum(own_jac[:, :, None] * own_point[:, None, :], axis=0)
    w_other = jnp.sum(other_jac[:, :, None] * other_point[:, None, :], axis=0)
    point_rhs = -(
        jnp.sum(own_point * own_error[:, None], axis=0)
        + jnp.sum(other_point * other_error[:, None], axis=0)
    )
    own_vi = jnp.sum(w_own[:, :, None] * inverse[None, :, :], axis=1)
    other_vi = jnp.sum(w_other[:, :, None] * inverse[None, :, :], axis=1)
    diag_own = jnp.sum(own_jac[:, :, None] * own_jac[:, None, :], axis=0) - jnp.sum(
        own_vi[:, None, :] * w_own[None, :, :], axis=2
    )
    diag_other = jnp.sum(other_jac[:, :, None] * other_jac[:, None, :], axis=0) - jnp.sum(
        other_vi[:, None, :] * w_other[None, :, :], axis=2
    )
    link = -jnp.sum(own_vi[:, None, :] * w_other[None, :, :], axis=2)
    grad_own = -jnp.sum(own_jac * own_error[:, None], axis=0) - jnp.sum(
        own_vi * point_rhs[None], axis=1
    )
    grad_other = -jnp.sum(other_jac * other_error[:, None], axis=0) - jnp.sum(
        other_vi * point_rhs[None], axis=1
    )
    return (diag_own, diag_other, link, grad_own, grad_other)


def conjugate_steps(right_side, apply_operator, inner_product):
    solution = jnp.zeros_like(right_side)
    remainder = right_side
    direction = right_side
    norm_now = inner_product(remainder, remainder)
    for iteration in range(ITERS):
        product_vec = apply_operator(direction)
        step_size = norm_now / inner_product(direction, product_vec)
        solution = solution + step_size * direction
        remainder = remainder - step_size * product_vec
        norm_next = inner_product(remainder, remainder)
        direction = remainder + norm_next / norm_now * direction
        norm_now = norm_next
    return (solution, remainder)


def plain_shards(cam_jac, pt_jac, resid, partner, count, tile_map):
    row_count = lax.axis_size("row")
    col_count = lax.axis_size("col")
    scenes = tile_map.shape[0]
    scn_local = partner.shape[0]
    points = partner.shape[1]
    tile_rows = scenes // row_count
    tile_cols = scenes // col_count
    per_group = scn_local // row_count
    row_index = lax.axis_index("row")
    col_index = lax.axis_index("col")
    device = row_index * col_count + col_index
    positions = jnp.arange(scenes, dtype=jnp.int32)
    tile_own = lax.dynamic_slice_in_dim(tile_map, device * scn_local, scn_local)
    local_rank = jnp.sum((tile_own[None, :] < tile_own[:, None]).astype(jnp.int32), axis=1)
    active = (jnp.arange(points, dtype=jnp.int32)[None, :] < count[:, None]).astype(jnp.float32)
    diag_own, diag_other, link, grad_own, grad_other = point_terms(cam_jac, pt_jac, resid)
    values = (
        jnp.concatenate(
            [
                link.reshape(36, scn_local, points),
                diag_other.reshape(36, scn_local, points),
                grad_other,
            ],
            axis=0,
        )
        * active[None]
    )
    values = jnp.moveaxis(values, 1, 0)

    def scene_sums(item):
        scene_values, scene_partner = item
        hits = scene_partner[:, None] == positions[None, :]
        tile_other = jnp.sum(jnp.where(hits, tile_map[None, :], 0), axis=1)
        onehot = (tile_other[:, None] == positions[None, :]).astype(jnp.float32)
        return jnp.dot(
            scene_values,
            onehot,
            precision=lax.Precision.HIGHEST,
            preferred_element_type=jnp.float32,
        )

    per_scene = lax.map(scene_sums, (values, partner))
    link_rows = per_scene[:, :36, :]
    other_sum = jnp.sum(per_scene[:, 36:, :], axis=0)
    ordering = (local_rank[None, :] == jnp.arange(scn_local, dtype=jnp.int32)[:, None]).astype(
        jnp.float32
    )
    panel = jnp.einsum("rs,sxc->xrc", ordering, link_rows, precision=lax.Precision.HIGHEST)
    panel = panel.reshape(36, row_count, per_group, col_count, tile_cols).transpose(0, 1, 3, 2, 4)
    panel_short = panel.astype(jnp.bfloat16)
    own_onehot = (tile_own[:, None] == positions[None, :]).astype(jnp.float32)
    own_diag = jnp.sum(diag_own * active, axis=-1).reshape(36, scn_local)
    own_grad = jnp.sum(grad_own * active, axis=-1)
    own_both = jnp.concatenate([own_diag, own_grad], axis=0)
    own_spread = jnp.dot(
        own_both, own_onehot, precision=lax.Precision.HIGHEST, preferred_element_type=jnp.float32
    )
    both_part = own_spread + other_sum
    diag_part = both_part[:36]
    grad_part = both_part[36:]
    shaped = panel_short.reshape(36, row_count * col_count, per_group, tile_cols)
    received = lax.all_to_all(shaped, ("row", "col"), split_axis=1, concat_axis=1, tiled=True)
    received = received.reshape(36, tile_rows, tile_cols)
    diag_all, grad_all = lax.psum((diag_part, grad_part), ("row", "col"))
    row_start = row_index * tile_rows
    col_start = col_index * tile_cols
    devices = scenes // scn_local
    tiles_grid = tile_map.reshape(devices, scn_local)
    inblock = (tiles_grid >= row_start) & (tiles_grid < row_start + tile_rows)
    lower = (tiles_grid[:, None, :] < tiles_grid[:, :, None]) & inblock[:, None, :]
    within_all = jnp.sum(lower.astype(jnp.int32), axis=2)
    slot_from = (jnp.arange(devices, dtype=jnp.int32)[:, None] * per_group + within_all).reshape(-1)
    slot_to = (tiles_grid - row_start).reshape(-1)
    slots = jnp.arange(tile_rows, dtype=jnp.int32)
    to_table = ((slot_to[:, None] == slots[None, :]) & inblock.reshape(-1)[:, None]).astype(
        jnp.bfloat16
    )
    from_table = (slot_from[:, None] == slots[None, :]).astype(jnp.bfloat16)
    selection = jnp.dot(to_table.T, from_table, preferred_element_type=jnp.float32).astype(
        jnp.bfloat16
    )
    coupling_tile = jnp.einsum(
        "pk,xkc->xpc", selection, received, preferred_element_type=jnp.float32
    )
    coupling_tile = coupling_tile.astype(jnp.bfloat16).reshape(6, 6, tile_rows, tile_cols)
    coupling_wide = coupling_tile.astype(jnp.float32)
    zero_at = row_index * 0

    def tile_products(rows_part, cols_part):
        forward = jnp.einsum(
            "xyij,yj->xi", coupling_wide, cols_part, precision=lax.Precision.HIGHEST
        )
        backward = jnp.einsum(
            "xyij,xi->yj", coupling_wide, rows_part, precision=lax.Precision.HIGHEST
        )
        empty = jnp.zeros((6, scenes), jnp.float32)
        spread = lax.dynamic_update_slice(empty, forward, (zero_at, row_start))
        spread = spread + lax.dynamic_update_slice(empty, backward, (zero_at, col_start))
        return lax.psum(spread, ("row", "col"))

    diag_blocks = diag_all.reshape(6, 6, scenes)

    def apply_full(direction):
        rows_part = lax.dynamic_slice_in_dim(direction, row_start, tile_rows, 1)
        cols_part = lax.dynamic_slice_in_dim(direction, col_start, tile_cols, 1)
        summed = tile_products(rows_part, cols_part)
        result = CAMERA_DAMPING * direction
        result = result + jnp.einsum(
            "xyi,yi->xi", diag_blocks, direction, precision=lax.Precision.HIGHEST
        )
        return result + summed

    def inner_full(first_vec, second_vec):
        return jnp.sum(first_vec * second_vec)

    whole_solution, whole_remainder = conjugate_steps(grad_all, apply_full, inner_full)
    solution = lax.dynamic_slice_in_dim(whole_solution, row_start, tile_rows, 1)
    remainder = lax.dynamic_slice_in_dim(whole_remainder, row_start, tile_rows, 1)
    return (coupling_tile, solution, remainder)


def shards(cam_jac, pt_jac, resid, partner, count, tile_map):
    row_count = lax.axis_size("row")
    col_count = lax.axis_size("col")
    scenes = tile_map.shape[0]
    scn, points = partner.shape
    packs = (
        scenes == col_count * HALF
        and scenes == row_count * LANES
        and scn == row_count * 4
        and LANES % scn == 0
        and points % LANES == 0
        and col_count >= 7
    )
    run = packed_shards if packs else plain_shards
    return run(cam_jac, pt_jac, resid, partner, count, tile_map)


def solution(mesh):
    return jax.shard_map(
        shards,
        mesh=mesh,
        in_specs=(
            P(None, None, None, AXES, None),
            P(None, None, None, AXES, None),
            P(None, None, AXES, None),
            P(AXES, None),
            P(AXES),
            P(),
        ),
        out_specs=(P(None, None, "row", "col"), P(None, "row"), P(None, "row")),
        check_vma=False,
    )
```

```python
import jax
import jax.numpy as jnp
from jax import lax
from jax.experimental import pallas as pl
from jax.experimental.pallas import tpu as pltpu
from jax.sharding import PartitionSpec as P

ITERS = 3
CAMERA_DAMPING = 1.0
POINT_DAMPING = 1.0
AXES = ("row", "col")
LANES = 128
HALF = 64
F32 = jnp.float32
BF16 = jnp.bfloat16
PAIRS = [(x, y) for x in range(6) for y in range(x, 6)]
CONTRACT_LAST = (((1,), (1,)), ((), ()))


def iota(shape, dim):
    return lax.broadcasted_iota(jnp.int32, shape, dim)


def split_two(value):
    high = value.astype(BF16)
    low = (value - high.astype(F32)).astype(BF16)
    return high, low


def point_values(ja, jb, pa, pb, ea, eb, live):
    one = POINT_DAMPING
    hess = {}
    for x in range(3):
        for y in range(x, 3):
            h = pa[0][x] * pa[0][y] + pa[1][x] * pa[1][y]
            h = h + (pb[0][x] * pb[0][y] + pb[1][x] * pb[1][y])
            hess[x, y] = h + one if x == y else h
    a, b, c = hess[0, 0], hess[0, 1], hess[0, 2]
    d, e, f = hess[1, 1], hess[1, 2], hess[2, 2]
    c00 = d * f - e * e
    c01 = c * e - b * f
    c02 = b * e - c * d
    c11 = a * f - c * c
    c12 = b * c - a * e
    c22 = a * d - b * b
    det = a * c00 + b * c01 + c * c02
    inv = 1.0 / det
    vi = [[c00 * inv, c01 * inv, c02 * inv], [None, c11 * inv, c12 * inv], [None, None, c22 * inv]]
    vi[1][0], vi[2][0], vi[2][1] = vi[0][1], vi[0][2], vi[1][2]
    q = [
        -((pa[0][k] * ea[0] + pa[1][k] * ea[1]) + (pb[0][k] * eb[0] + pb[1][k] * eb[1]))
        for k in range(3)
    ]
    viq = [vi[k][0] * q[0] + vi[k][1] * q[1] + vi[k][2] * q[2] for k in range(3)]

    def times_vi(p):
        return [
            [p[m][0] * vi[0][k] + p[m][1] * vi[1][k] + p[m][2] * vi[2][k] for k in range(3)]
            for m in range(2)
        ]

    def inner(left, right):
        return left[0] * right[0] + left[1] * right[1] + left[2] * right[2]

    def keep(value):
        return jnp.where(live, value, 0.0)

    av = times_vi(pa)
    bv = times_vi(pb)
    m_ab = [[keep(-inner(av[m], pb[k])) for k in range(2)] for m in range(2)]
    g_aa = [keep(1.0 - inner(av[0], pa[0])), keep(-inner(av[0], pa[1])), keep(1.0 - inner(av[1], pa[1]))]
    g_bb = [keep(1.0 - inner(bv[0], pb[0])), keep(-inner(bv[0], pb[1])), keep(1.0 - inner(bv[1], pb[1]))]
    h_a = [keep(-(ea[m] + inner(pa[m], viq))) for m in range(2)]
    h_b = [keep(-(eb[m] + inner(pb[m], viq))) for m in range(2)]

    mj = [[m_ab[m][0] * jb[0][y] + m_ab[m][1] * jb[1][y] for y in range(6)] for m in range(2)]
    link = {}
    for x in range(6):
        for y in range(6):
            link[x, y] = ja[0][x] * mj[0][y] + ja[1][x] * mj[1][y]

    def diagonal(j, g):
        gj = [
            [g[0] * j[0][y] + g[1] * j[1][y] for y in range(6)],
            [g[1] * j[0][y] + g[2] * j[1][y] for y in range(6)],
        ]
        return [j[0][x] * gj[0][y] + j[1][x] * gj[1][y] for x, y in PAIRS]

    diag_own = diagonal(ja, g_aa)
    diag_other = diagonal(jb, g_bb)
    grad_own = [ja[0][x] * h_a[0] + ja[1][x] * h_a[1] for x in range(6)]
    grad_other = [jb[0][x] * h_b[0] + jb[1][x] * h_b[1] for x in range(6)]
    return diag_own, diag_other, link, grad_own, grad_other


def assemble_kernel(
    row_count, col_count, cam_in, pt_in, res_in, partner_in, row_in, count_in, map_in, send_ref,
    vals_ref, own_ref, acc_ref, links_ref, flat_ref, extra_ref, perm_ref,
    cam_ref, pt_ref, res_ref, partner_ref, map_ref, count_sm, map_sm, slab_sem, whole_sem,
):
    scn = partner_ref.shape[0]
    points = partner_ref.shape[1]
    scenes = map_ref.shape[1]
    wholes = [
        pltpu.make_async_copy(source, target, whole_sem.at[k])
        for k, (source, target) in enumerate(
            [(count_in, count_sm), (map_in, map_sm), (row_in, map_ref), (partner_in, partner_ref)]
        )
    ]

    def slab_copies(step):
        lanes = pl.ds(pl.multiple_of(step * LANES, LANES), LANES)
        return [
            pltpu.make_async_copy(
                source.at[..., lanes], target.at[..., lanes], slab_sem.at[k, step]
            )
            for k, (source, target) in enumerate([(cam_in, cam_ref), (pt_in, pt_ref), (res_in, res_ref)])
        ]

    wholes[0].start()
    for step in range(points // LANES):
        for copy in slab_copies(step):
            copy.start()
    for copy in wholes[1:]:
        copy.start()
    per_group = scn // row_count
    device = lax.axis_index("row") * col_count + lax.axis_index("col")
    slab = (scn, LANES)

    own_ref[...] = jnp.zeros_like(own_ref)
    acc_ref[...] = jnp.zeros_like(acc_ref)
    extra_ref[...] = jnp.zeros_like(extra_ref)
    vals_ref[:, pl.ds(63 * scn, scn), :] = jnp.zeros((points // LANES, scn, LANES), F32)

    wholes[0].wait()
    sub = iota(slab, 0)
    counts = jnp.zeros(slab, jnp.int32)
    for s in range(scn):
        counts = jnp.where(sub == s, count_sm[s], counts)

    def slab_step(step, carry):
        for copy in slab_copies(step):
            copy.wait()
        lanes = pl.ds(pl.multiple_of(step * LANES, LANES), LANES)

        def get(ref, *where):
            return ref[where + (slice(None), lanes)].astype(F32)

        ja = [[get(cam_ref, 0, m, x) for x in range(6)] for m in range(2)]
        jb = [[get(cam_ref, 1, m, x) for x in range(6)] for m in range(2)]
        pa = [[get(pt_ref, 0, m, x) for x in range(3)] for m in range(2)]
        pb = [[get(pt_ref, 1, m, x) for x in range(3)] for m in range(2)]
        ea = [get(res_ref, 0, m) for m in range(2)]
        eb = [get(res_ref, 1, m) for m in range(2)]
        live = (iota(slab, 1) + step * LANES) < counts
        diag_own, diag_other, link, grad_own, grad_other = point_values(ja, jb, pa, pb, ea, eb, live)

        def put(q, value):
            vals_ref[step, pl.ds(q * scn, scn), :] = value

        def put_own(q, value):
            own_ref[pl.ds(q * scn, scn), :] += value

        for x in range(3):
            for y in range(6):
                put(x * 6 + y, link[x, y])
                put(24 + x * 6 + y, link[x + 3, y])
        for x in range(6):
            put(18 + x, grad_other[x])
            put_own(2 + x, grad_own[x])
        for q in range(21):
            put(42 + q, diag_other[q])
            put_own(10 + q, diag_own[q])
        return carry

    lax.fori_loop(0, points // LANES, slab_step, 0)

    for copy in wholes[1:]:
        copy.wait()
    spots = iota((points, scenes), 1)
    mates = jnp.transpose(partner_ref[...])

    def scene_step(s):
        values = jnp.concatenate(
            [vals_ref.at[t][pl.ds(s, 64, stride=scn), :] for t in range(points // LANES)], axis=1
        )
        high, low = split_two(values)
        left = jnp.concatenate([high, low], axis=0)
        onehot = jnp.where(spots == mates[:, s : s + 1], 1.0, 0.0).astype(BF16)
        both = jnp.dot(left, onehot, preferred_element_type=F32)
        total = both[:64] + both[64:]
        acc_ref[...] += total
        mine = map_sm[device * scn + s]
        rank = jnp.int32(0)
        for other in range(scn):
            rank = rank + (map_sm[device * scn + other] < mine).astype(jnp.int32)
        links_ref[pl.ds(pl.multiple_of(rank * 48, 16), 48), :] = total[:48].astype(BF16)

    for s in range(scn):
        scene_step(s)

    lane = iota((32, LANES), 1)
    own = jnp.zeros((32, LANES), F32)
    for s in range(scn):
        column = jnp.sum(own_ref[pl.ds(s, 32, stride=scn), :], axis=1, keepdims=True)
        own = own + jnp.where(lane == s, column, 0.0)
    start = device * scn
    own = pltpu.roll(own, lax.rem(start, LANES), 1)
    tile_at = lax.div(start, LANES)
    for t in range(scenes // LANES):
        cols = pl.ds(t * LANES, LANES)
        whole = jnp.concatenate([acc_ref[16:24, cols], acc_ref[40:64, cols]], axis=0)
        whole = whole + jnp.where(tile_at == t, own, 0.0)
        high, low = split_two(whole)
        flat_ref[0:32, cols] = high.astype(F32)
        flat_ref[32:64, cols] = low.astype(F32)
    per_col = -(-21 // col_count)
    for c in range(col_count):
        for i in range(per_col):
            q = c * per_col + i
            if q < 21:
                extra_ref[c * 8 + 2 + i : c * 8 + 3 + i, :] = flat_ref[10 + q : 11 + q, :]
                extra_ref[c * 8 + 5 + i : c * 8 + 6 + i, :] = flat_ref[42 + q : 43 + q, :]
    base = col_count * 8
    extra_ref[base : base + 8, :] = flat_ref[0:8, :]
    extra_ref[base + 8 : base + 16, :] = flat_ref[32:40, :]

    places = jnp.transpose(jnp.broadcast_to(map_ref[...], (8, scenes)))[:, :1]
    onto = jnp.where(iota((scenes, scenes), 1) == places, 1.0, 0.0).astype(BF16)
    left = jnp.concatenate([links_ref[...], extra_ref[...].astype(BF16)], axis=0)
    perm_ref[...] = jnp.dot(left, onto, preferred_element_type=F32)

    top = scn * 48
    first = iota((8, LANES), 1) < HALF
    keep_rows = iota((8, LANES), 0) < 2
    first24 = iota((24, LANES), 1) < HALF

    def merge(low_part, high_part, mask):
        even = jnp.where(mask, low_part, pltpu.roll(high_part, HALF, 1))
        odd = jnp.where(mask, pltpu.roll(low_part, HALF, 1), high_part)
        return even, odd

    for j in range(col_count // 2):
        cols = pl.ds(j * LANES, LANES)
        grad_cols = merge(
            perm_ref[top + base : top + base + 8, cols],
            perm_ref[top + base + 8 : top + base + 16, cols],
            first,
        )
        for r in range(row_count):
            rows = pl.ds(r * LANES, LANES)
            grad_high = perm_ref[top + base : top + base + 8, rows]
            grad_low = perm_ref[top + base + 8 : top + base + 16, rows]
            for slot in range(per_group):
                at = (r * per_group + slot) * 48
                pieces = merge(perm_ref[at : at + 24, cols], perm_ref[at + 24 : at + 48, cols], first24)
                for k in range(2):
                    c = 2 * j + k
                    if slot == 0:
                        extra = grad_high
                    elif slot == 1:
                        extra = grad_low
                    elif slot == 2:
                        extra = grad_cols[k]
                    else:
                        extra = perm_ref[top + c * 8 : top + c * 8 + 8, rows]
                    tail = jnp.where(keep_rows, pieces[k][16:24], extra)
                    block = jnp.concatenate([pieces[k][0:16], tail], axis=0)
                    send_ref[r * col_count + c, slot * 24 : slot * 24 + 24, :] = block.astype(BF16)


def tile_matvec(tile_ref, own_ref, rows_part, cols_part, rows_ref):
    which = iota((8, LANES), 0)
    turned = jnp.transpose(cols_part)[:HALF]
    forward = [jnp.zeros((8, LANES), F32) for _ in range(6)]
    backward = []
    for y in range(6):
        column = jnp.broadcast_to(turned[:, y : y + 1], (HALF, LANES))
        total = jnp.zeros((HALF, LANES), F32)
        for x in range(6):
            block = tile_ref[x * 6 + y].astype(F32)
            forward[x] = forward[x] + jnp.sum((block * column).reshape(HALF // 8, 8, LANES), axis=0)
            total = total + block * rows_part[x : x + 1, :]
        backward.append(total)
    sides = []
    for y in range(3):
        pair = jnp.concatenate([backward[y], backward[y + 3]], axis=0)
        sides.append(jnp.sum(jnp.transpose(pair), axis=0, keepdims=True))
    out = jnp.zeros((8, LANES), F32)
    for x in range(6):
        out = jnp.where(which == x, jnp.sum(forward[x], axis=0, keepdims=True), out)
    rows_ref[...] = rows_part
    col = lax.axis_index("col")
    per_col = -(-21 // lax.axis_size("col"))
    for i in range(per_col):
        q = jnp.minimum(col * per_col + i, 20)
        x = jnp.int32(0)
        start = jnp.int32(0)
        for line in range(1, 6):
            past = (q >= PAIRS.index((line, line))).astype(jnp.int32)
            x = x + past
            start = start + past * (7 - line)
        y = q - start + x
        weight = own_ref[i : i + 1, :]
        at_x = rows_ref[pl.ds(x, 1), :] * weight
        at_y = rows_ref[pl.ds(y, 1), :] * weight
        out = out + jnp.where(which == x, at_y, 0.0)
        out = out + jnp.where((which == y) & (x != y), at_x, 0.0)
    return out, sides


def write_partials(out, sides, line, part_ref):
    rows = [out[x : x + 1, :] for x in range(6)] + sides
    if line is not None:
        rows.append(line)
    for n in range(part_ref.shape[0]):
        for k, row in enumerate(rows):
            part_ref[n, :, k * LANES : (k + 1) * LANES] = row


def first_kernel(
    row_count, col_count, got_ref, map_ref, tile_ref, own_ref, part_ref, wide_ref, rows_ref,
):
    devices = got_ref.shape[0]
    scenes = map_ref.shape[1]
    scn = scenes // devices
    per_group = scn // row_count
    tile_rows = scenes // row_count
    row = lax.axis_index("row")
    tiles = jnp.concatenate(
        [map_ref[:, t * LANES : (t + 1) * LANES] for t in range(scenes // LANES)], axis=0
    )
    groups = scenes // LANES
    place = iota((groups, LANES), 1) % scn
    rank = jnp.zeros((groups, LANES), jnp.int32)
    for shift in range(1, scn):
        before = pltpu.roll(tiles, shift, 1)
        after = pltpu.roll(tiles, LANES - shift, 1)
        rank = rank + ((before < tiles) & (place >= shift)).astype(jnp.int32)
        rank = rank + ((after < tiles) & (place + shift < scn)).astype(jnp.int32)
    scene_id = iota((groups, LANES), 0) * LANES + iota((groups, LANES), 1)
    slot_at = (scene_id // scn) * per_group + rank % per_group
    local = tiles - row * tile_rows
    slot_at = jnp.where((local >= 0) & (local < tile_rows), slot_at, -1)
    select = jnp.zeros((tile_rows, tile_rows), F32)
    for t in range(groups):
        to_row = jnp.where(iota((tile_rows, LANES), 0) == local[t : t + 1, :], 1.0, 0.0).astype(BF16)
        from_slot = jnp.where(iota((tile_rows, LANES), 0) == slot_at[t : t + 1, :], 1.0, 0.0).astype(BF16)
        select = select + lax.dot_general(to_row, from_slot, CONTRACT_LAST, preferred_element_type=F32)
    select = select.astype(BF16)

    for n in range(devices):
        wide_ref[pl.ds(n * 96, 96), :] = got_ref[n].astype(F32)
    for k in range(18):
        picked = wide_ref[pl.ds(k, tile_rows, stride=24), :].astype(BF16)
        block = lax.dot_general(picked, select, (((0,), (1,)), ((), ())), preferred_element_type=F32)
        tile_ref[k] = block[:HALF].astype(BF16)
        tile_ref[k + 18] = block[HALF:].astype(BF16)
    extras = []
    for slot in range(per_group):
        total = wide_ref[slot * 24 + 16 : slot * 24 + 24, :]
        for n in range(1, devices):
            total = total + wide_ref[n * 96 + slot * 24 + 16 : n * 96 + slot * 24 + 24, :]
        extras.append(pltpu.roll(total, 6, 0))
    used = iota((8, LANES), 0) < 6
    rows_part = jnp.where(used, extras[0] + extras[1], 0.0)
    cols_part = jnp.where(used, extras[2] + pltpu.roll(extras[2], HALF, 1), 0.0)
    own_ref[...] = extras[3] + pltpu.roll(extras[3], 5, 0)
    out, sides = tile_matvec(tile_ref, own_ref, rows_part, cols_part, rows_ref)
    rows_ref[...] = rows_part
    line = rows_ref[pl.ds(jnp.minimum(lax.axis_index("col"), 5), 1), :]
    write_partials(out, sides, line, part_ref)


def gather_image(row_count, col_count, got_ref, image_ref):
    first = iota((1, LANES), 1) < HALF
    side = 6 * LANES
    cols = []
    for c in range(col_count):
        total = got_ref[c, :, side : side + 3 * LANES]
        for r in range(1, row_count):
            total = total + got_ref[r * col_count + c, :, side : side + 3 * LANES]
        cols.append(total)
    for r in range(row_count):
        total = got_ref[r * col_count, :, 0:side]
        for c in range(1, col_count):
            total = total + got_ref[r * col_count + c, :, 0:side]
        image_ref[r] = jnp.zeros((8, LANES), F32)
        for t in range(3):
            left = cols[2 * r][:, t * LANES : (t + 1) * LANES]
            right = cols[2 * r + 1][:, t * LANES : (t + 1) * LANES]
            low = jnp.where(first, left, pltpu.roll(right, HALF, 1))
            high = jnp.where(first, pltpu.roll(left, HALF, 1), right)
            image_ref[r, t : t + 1, :] = total[:, t * LANES : (t + 1) * LANES] + low
            image_ref[r, t + 3 : t + 4, :] = total[:, (t + 3) * LANES : (t + 4) * LANES] + high


def inner_all(left, right):
    return jnp.sum(jnp.sum(left * right, axis=0), keepdims=True)


def step_kernel(
    row_count, col_count, begin, got_ref, tile_ref, own_ref, state_ref, next_ref, part_ref,
    *rest,
):
    if begin:
        coupling_ref, image_ref, rows_ref, copy_sem = rest
        copy = pltpu.make_async_copy(tile_ref, coupling_ref, copy_sem)
        copy.start()
    else:
        image_ref, rows_ref = rest
    gather_image(row_count, col_count, got_ref, image_ref)
    if begin:
        for r in range(row_count):
            next_ref[1, r] = jnp.zeros((8, LANES), F32)
            for x in range(6):
                next_ref[1, r, x : x + 1, :] = got_ref[r * col_count + x, :, 9 * LANES : 10 * LANES]
        remainder = next_ref[1]
        direction = remainder
        answer = jnp.zeros_like(remainder)
    else:
        answer, remainder, direction = state_ref[0], state_ref[1], state_ref[2]
    norm_now = inner_all(remainder, remainder)
    image = CAMERA_DAMPING * direction + image_ref[...]
    alpha = norm_now / inner_all(direction, image)
    answer = answer + alpha * direction
    remainder = remainder - alpha * image
    norm_next = inner_all(remainder, remainder)
    direction = remainder + norm_next / norm_now * direction
    next_ref[0] = answer
    next_ref[1] = remainder
    next_ref[2] = direction
    col = lax.axis_index("col")
    rows_part = next_ref[2, lax.axis_index("row")]
    wide = next_ref[2, lax.div(col, 2)]
    turned = pltpu.roll(wide, HALF, 1)
    cols_part = jnp.where(iota((8, LANES), 0) * 0 == lax.rem(col, 2), wide, turned)
    out, sides = tile_matvec(tile_ref, own_ref, rows_part, cols_part, rows_ref)
    write_partials(out, sides, None, part_ref)
    if begin:
        copy.wait()


def last_kernel(row_count, col_count, got_ref, state_ref, answer_ref, remainder_ref, image_ref):
    gather_image(row_count, col_count, got_ref, image_ref)
    remainder, direction = state_ref[1], state_ref[2]
    norm_now = inner_all(remainder, remainder)
    image_ref[...] = CAMERA_DAMPING * direction + image_ref[...]
    alpha = norm_now / inner_all(direction, image_ref[...])
    row = lax.axis_index("row")
    answer_ref[...] = (state_ref[0, row] + alpha * state_ref[2, row])[:6]
    remainder_ref[...] = (state_ref[1, row] - alpha * image_ref[row])[:6]


def vmem():
    return pl.BlockSpec(memory_space=pltpu.VMEM)


def hbm():
    return pl.BlockSpec(memory_space=pltpu.HBM)


def small_limit(mib):
    return pltpu.CompilerParams(vmem_limit_bytes=mib << 20)


def packed_shards(cam_jac, pt_jac, resid, partner, count, tile_map):
    row_count = lax.axis_size("row")
    col_count = lax.axis_size("col")
    devices = row_count * col_count
    scenes = tile_map.shape[0]
    scn, points = partner.shape
    map_row = tile_map.reshape(1, scenes)

    def bind(kernel, *fixed):
        def run(*refs):
            return kernel(row_count, col_count, *fixed, *refs)

        return run

    extra_rows = col_count * 8 + 16
    send = pl.pallas_call(
        bind(assemble_kernel),
        out_shape=jax.ShapeDtypeStruct((devices, 96, LANES), BF16),
        in_specs=[hbm()] * 7,
        out_specs=vmem(),
        scratch_shapes=[
            pltpu.VMEM((points // LANES, 64 * scn, LANES), F32),
            pltpu.VMEM((32 * scn, LANES), F32),
            pltpu.VMEM((64, scenes), F32),
            pltpu.VMEM((48 * scn, scenes), BF16),
            pltpu.VMEM((64, scenes), F32),
            pltpu.VMEM((extra_rows, scenes), F32),
            pltpu.VMEM((48 * scn + extra_rows, scenes), F32),
            pltpu.VMEM(cam_jac.shape, BF16),
            pltpu.VMEM(pt_jac.shape, BF16),
            pltpu.VMEM(resid.shape, BF16),
            pltpu.VMEM(partner.shape, jnp.int32),
            pltpu.VMEM(map_row.shape, jnp.int32),
            pltpu.SMEM(count.shape, jnp.int32),
            pltpu.SMEM(tile_map.shape, jnp.int32),
            pltpu.SemaphoreType.DMA((3, points // LANES)),
            pltpu.SemaphoreType.DMA((4,)),
        ],
        compiler_params=small_limit(36),
        name="assemble",
    )(
        *[
            pltpu.with_memory_space_constraint(value, pltpu.HBM)
            for value in (cam_jac, pt_jac, resid, partner, map_row, count, tile_map)
        ]
    )
    got = lax.all_to_all(send, AXES, 0, 0, tiled=True)
    tile_rows = scenes // row_count
    tile, own, part = pl.pallas_call(
        bind(first_kernel),
        out_shape=(
            jax.ShapeDtypeStruct((36, HALF, tile_rows), BF16),
            jax.ShapeDtypeStruct((8, LANES), F32),
            jax.ShapeDtypeStruct((devices, 1, 10 * LANES), F32),
        ),
        in_specs=[vmem()] * 2,
        out_specs=(vmem(),) * 3,
        scratch_shapes=[pltpu.VMEM((devices * 96, LANES), F32), pltpu.VMEM((8, LANES), F32)],
        compiler_params=small_limit(16),
        name="first",
    )(got, map_row)
    state = jnp.zeros((3, row_count, 8, LANES), F32)
    for turn in range(ITERS - 1):
        got = lax.all_to_all(part, AXES, 0, 0, tiled=True)
        begin = turn == 0
        outs = [
            jax.ShapeDtypeStruct((3, row_count, 8, LANES), F32),
            jax.ShapeDtypeStruct((devices, 1, 9 * LANES), F32),
        ]
        places = [vmem()] * 2
        scratch = [pltpu.VMEM((row_count, 8, LANES), F32), pltpu.VMEM((8, LANES), F32)]
        if begin:
            outs.append(jax.ShapeDtypeStruct(tile.shape, BF16))
            places.append(hbm())
            scratch.append(pltpu.SemaphoreType.DMA(()))
        state, part, *rest = pl.pallas_call(
            bind(step_kernel, begin),
            out_shape=outs,
            in_specs=[vmem()] * 4,
            out_specs=places,
            scratch_shapes=scratch,
            compiler_params=small_limit(8),
            name="step",
        )(got, tile, own, state)
        if begin:
            coupling = rest[0]
    got = lax.all_to_all(part, AXES, 0, 0, tiled=True)
    answer, remainder = pl.pallas_call(
        bind(last_kernel),
        out_shape=(jax.ShapeDtypeStruct((6, tile_rows), F32),) * 2,
        in_specs=[vmem()] * 2,
        out_specs=(vmem(),) * 2,
        scratch_shapes=[pltpu.VMEM((row_count, 8, LANES), F32)],
        compiler_params=small_limit(4),
        name="last",
    )(got, state)
    return jnp.swapaxes(coupling.reshape(6, 6, HALF, tile_rows), 2, 3), answer, remainder


def cross_product(first_vec, second_vec):
    return jnp.stack(
        [
            first_vec[1] * second_vec[2] - first_vec[2] * second_vec[1],
            first_vec[2] * second_vec[0] - first_vec[0] * second_vec[2],
            first_vec[0] * second_vec[1] - first_vec[1] * second_vec[0],
        ],
        axis=0,
    )


def point_terms(camera, points_jac, errors):
    camera = camera.astype(jnp.float32)
    points_jac = points_jac.astype(jnp.float32)
    errors = errors.astype(jnp.float32)
    own_jac, other_jac = (camera[0], camera[1])
    own_point, other_point = (points_jac[0], points_jac[1])
    own_error, other_error = (errors[0], errors[1])
    point_hessian = jnp.sum(own_point[:, :, None] * own_point[:, None, :], axis=0)
    point_hessian = point_hessian + jnp.sum(
        other_point[:, :, None] * other_point[:, None, :], axis=0
    )
    point_hessian = point_hessian + POINT_DAMPING * jnp.eye(3, dtype=jnp.float32)[:, :, None, None]
    first_row, second_row, third_row = (point_hessian[0], point_hessian[1], point_hessian[2])
    cofactor_first = cross_product(second_row, third_row)
    cofactor_second = cross_product(third_row, first_row)
    cofactor_third = cross_product(first_row, second_row)
    determinant = jnp.sum(first_row * cofactor_first, axis=0)
    inverse = jnp.stack([cofactor_first, cofactor_second, cofactor_third], axis=1) / determinant
    w_own = jnp.sum(own_jac[:, :, None] * own_point[:, None, :], axis=0)
    w_other = jnp.sum(other_jac[:, :, None] * other_point[:, None, :], axis=0)
    point_rhs = -(
        jnp.sum(own_point * own_error[:, None], axis=0)
        + jnp.sum(other_point * other_error[:, None], axis=0)
    )
    own_vi = jnp.sum(w_own[:, :, None] * inverse[None, :, :], axis=1)
    other_vi = jnp.sum(w_other[:, :, None] * inverse[None, :, :], axis=1)
    diag_own = jnp.sum(own_jac[:, :, None] * own_jac[:, None, :], axis=0) - jnp.sum(
        own_vi[:, None, :] * w_own[None, :, :], axis=2
    )
    diag_other = jnp.sum(other_jac[:, :, None] * other_jac[:, None, :], axis=0) - jnp.sum(
        other_vi[:, None, :] * w_other[None, :, :], axis=2
    )
    link = -jnp.sum(own_vi[:, None, :] * w_other[None, :, :], axis=2)
    grad_own = -jnp.sum(own_jac * own_error[:, None], axis=0) - jnp.sum(
        own_vi * point_rhs[None], axis=1
    )
    grad_other = -jnp.sum(other_jac * other_error[:, None], axis=0) - jnp.sum(
        other_vi * point_rhs[None], axis=1
    )
    return (diag_own, diag_other, link, grad_own, grad_other)


def conjugate_steps(right_side, apply_operator, inner_product):
    solution = jnp.zeros_like(right_side)
    remainder = right_side
    direction = right_side
    norm_now = inner_product(remainder, remainder)
    for iteration in range(ITERS):
        product_vec = apply_operator(direction)
        step_size = norm_now / inner_product(direction, product_vec)
        solution = solution + step_size * direction
        remainder = remainder - step_size * product_vec
        norm_next = inner_product(remainder, remainder)
        direction = remainder + norm_next / norm_now * direction
        norm_now = norm_next
    return (solution, remainder)


def plain_shards(cam_jac, pt_jac, resid, partner, count, tile_map):
    row_count = lax.axis_size("row")
    col_count = lax.axis_size("col")
    scenes = tile_map.shape[0]
    scn_local = partner.shape[0]
    points = partner.shape[1]
    tile_rows = scenes // row_count
    tile_cols = scenes // col_count
    per_group = scn_local // row_count
    row_index = lax.axis_index("row")
    col_index = lax.axis_index("col")
    device = row_index * col_count + col_index
    positions = jnp.arange(scenes, dtype=jnp.int32)
    tile_own = lax.dynamic_slice_in_dim(tile_map, device * scn_local, scn_local)
    local_rank = jnp.sum((tile_own[None, :] < tile_own[:, None]).astype(jnp.int32), axis=1)
    active = (jnp.arange(points, dtype=jnp.int32)[None, :] < count[:, None]).astype(jnp.float32)
    diag_own, diag_other, link, grad_own, grad_other = point_terms(cam_jac, pt_jac, resid)
    values = (
        jnp.concatenate(
            [
                link.reshape(36, scn_local, points),
                diag_other.reshape(36, scn_local, points),
                grad_other,
            ],
            axis=0,
        )
        * active[None]
    )
    values = jnp.moveaxis(values, 1, 0)

    def scene_sums(item):
        scene_values, scene_partner = item
        hits = scene_partner[:, None] == positions[None, :]
        tile_other = jnp.sum(jnp.where(hits, tile_map[None, :], 0), axis=1)
        onehot = (tile_other[:, None] == positions[None, :]).astype(jnp.float32)
        return jnp.dot(
            scene_values,
            onehot,
            precision=lax.Precision.HIGHEST,
            preferred_element_type=jnp.float32,
        )

    per_scene = lax.map(scene_sums, (values, partner))
    link_rows = per_scene[:, :36, :]
    other_sum = jnp.sum(per_scene[:, 36:, :], axis=0)
    ordering = (local_rank[None, :] == jnp.arange(scn_local, dtype=jnp.int32)[:, None]).astype(
        jnp.float32
    )
    panel = jnp.einsum("rs,sxc->xrc", ordering, link_rows, precision=lax.Precision.HIGHEST)
    panel = panel.reshape(36, row_count, per_group, col_count, tile_cols).transpose(0, 1, 3, 2, 4)
    panel_short = panel.astype(jnp.bfloat16)
    own_onehot = (tile_own[:, None] == positions[None, :]).astype(jnp.float32)
    own_diag = jnp.sum(diag_own * active, axis=-1).reshape(36, scn_local)
    own_grad = jnp.sum(grad_own * active, axis=-1)
    own_both = jnp.concatenate([own_diag, own_grad], axis=0)
    own_spread = jnp.dot(
        own_both, own_onehot, precision=lax.Precision.HIGHEST, preferred_element_type=jnp.float32
    )
    both_part = own_spread + other_sum
    diag_part = both_part[:36]
    grad_part = both_part[36:]
    shaped = panel_short.reshape(36, row_count * col_count, per_group, tile_cols)
    received = lax.all_to_all(shaped, ("row", "col"), split_axis=1, concat_axis=1, tiled=True)
    received = received.reshape(36, tile_rows, tile_cols)
    diag_all, grad_all = lax.psum((diag_part, grad_part), ("row", "col"))
    row_start = row_index * tile_rows
    col_start = col_index * tile_cols
    devices = scenes // scn_local
    tiles_grid = tile_map.reshape(devices, scn_local)
    inblock = (tiles_grid >= row_start) & (tiles_grid < row_start + tile_rows)
    lower = (tiles_grid[:, None, :] < tiles_grid[:, :, None]) & inblock[:, None, :]
    within_all = jnp.sum(lower.astype(jnp.int32), axis=2)
    slot_from = (jnp.arange(devices, dtype=jnp.int32)[:, None] * per_group + within_all).reshape(-1)
    slot_to = (tiles_grid - row_start).reshape(-1)
    slots = jnp.arange(tile_rows, dtype=jnp.int32)
    to_table = ((slot_to[:, None] == slots[None, :]) & inblock.reshape(-1)[:, None]).astype(
        jnp.bfloat16
    )
    from_table = (slot_from[:, None] == slots[None, :]).astype(jnp.bfloat16)
    selection = jnp.dot(to_table.T, from_table, preferred_element_type=jnp.float32).astype(
        jnp.bfloat16
    )
    coupling_tile = jnp.einsum(
        "pk,xkc->xpc", selection, received, preferred_element_type=jnp.float32
    )
    coupling_tile = coupling_tile.astype(jnp.bfloat16).reshape(6, 6, tile_rows, tile_cols)
    coupling_wide = coupling_tile.astype(jnp.float32)
    zero_at = row_index * 0

    def tile_products(rows_part, cols_part):
        forward = jnp.einsum(
            "xyij,yj->xi", coupling_wide, cols_part, precision=lax.Precision.HIGHEST
        )
        backward = jnp.einsum(
            "xyij,xi->yj", coupling_wide, rows_part, precision=lax.Precision.HIGHEST
        )
        empty = jnp.zeros((6, scenes), jnp.float32)
        spread = lax.dynamic_update_slice(empty, forward, (zero_at, row_start))
        spread = spread + lax.dynamic_update_slice(empty, backward, (zero_at, col_start))
        return lax.psum(spread, ("row", "col"))

    diag_blocks = diag_all.reshape(6, 6, scenes)

    def apply_full(direction):
        rows_part = lax.dynamic_slice_in_dim(direction, row_start, tile_rows, 1)
        cols_part = lax.dynamic_slice_in_dim(direction, col_start, tile_cols, 1)
        summed = tile_products(rows_part, cols_part)
        result = CAMERA_DAMPING * direction
        result = result + jnp.einsum(
            "xyi,yi->xi", diag_blocks, direction, precision=lax.Precision.HIGHEST
        )
        return result + summed

    def inner_full(first_vec, second_vec):
        return jnp.sum(first_vec * second_vec)

    whole_solution, whole_remainder = conjugate_steps(grad_all, apply_full, inner_full)
    solution = lax.dynamic_slice_in_dim(whole_solution, row_start, tile_rows, 1)
    remainder = lax.dynamic_slice_in_dim(whole_remainder, row_start, tile_rows, 1)
    return (coupling_tile, solution, remainder)


def shards(cam_jac, pt_jac, resid, partner, count, tile_map):
    row_count = lax.axis_size("row")
    col_count = lax.axis_size("col")
    scenes = tile_map.shape[0]
    scn, points = partner.shape
    packs = (
        scenes == col_count * HALF
        and scenes == row_count * LANES
        and scn == row_count * 4
        and LANES % scn == 0
        and points % LANES == 0
        and col_count >= 7
    )
    run = packed_shards if packs else plain_shards
    return run(cam_jac, pt_jac, resid, partner, count, tile_map)


def solution(mesh):
    return jax.shard_map(
        shards,
        mesh=mesh,
        in_specs=(
            P(None, None, None, AXES, None),
            P(None, None, None, AXES, None),
            P(None, None, AXES, None),
            P(AXES, None),
            P(AXES),
            P(),
        ),
        out_specs=(P(None, None, "row", "col"), P(None, "row"), P(None, "row")),
        check_vma=False,
    )
```

```python
import jax
import jax.numpy as jnp
from jax import lax
from jax.experimental import pallas as pl
from jax.experimental.pallas import tpu as pltpu
from jax.sharding import PartitionSpec as P

ITERS = 3
CAMERA_DAMPING = 1.0
POINT_DAMPING = 1.0
AXES = ("row", "col")
LANES = 128
HALF = 64
F32 = jnp.float32
BF16 = jnp.bfloat16
PAIRS = [(x, y) for x in range(6) for y in range(x, 6)]
CONTRACT_LAST = (((1,), (1,)), ((), ()))


def iota(shape, dim):
    return lax.broadcasted_iota(jnp.int32, shape, dim)


def split_two(value):
    high = value.astype(BF16)
    low = (value - high.astype(F32)).astype(BF16)
    return high, low


def point_values(ja, jb, pa, pb, ea, eb, live):
    one = POINT_DAMPING
    hess = {}
    for x in range(3):
        for y in range(x, 3):
            h = pa[0][x] * pa[0][y] + pa[1][x] * pa[1][y]
            h = h + (pb[0][x] * pb[0][y] + pb[1][x] * pb[1][y])
            hess[x, y] = h + one if x == y else h
    a, b, c = hess[0, 0], hess[0, 1], hess[0, 2]
    d, e, f = hess[1, 1], hess[1, 2], hess[2, 2]
    c00 = d * f - e * e
    c01 = c * e - b * f
    c02 = b * e - c * d
    c11 = a * f - c * c
    c12 = b * c - a * e
    c22 = a * d - b * b
    det = a * c00 + b * c01 + c * c02
    inv = 1.0 / det
    vi = [[c00 * inv, c01 * inv, c02 * inv], [None, c11 * inv, c12 * inv], [None, None, c22 * inv]]
    vi[1][0], vi[2][0], vi[2][1] = vi[0][1], vi[0][2], vi[1][2]
    q = [
        -((pa[0][k] * ea[0] + pa[1][k] * ea[1]) + (pb[0][k] * eb[0] + pb[1][k] * eb[1]))
        for k in range(3)
    ]
    viq = [vi[k][0] * q[0] + vi[k][1] * q[1] + vi[k][2] * q[2] for k in range(3)]

    def times_vi(p):
        return [
            [p[m][0] * vi[0][k] + p[m][1] * vi[1][k] + p[m][2] * vi[2][k] for k in range(3)]
            for m in range(2)
        ]

    def inner(left, right):
        return left[0] * right[0] + left[1] * right[1] + left[2] * right[2]

    def keep(value):
        return jnp.where(live, value, 0.0)

    av = times_vi(pa)
    bv = times_vi(pb)
    m_ab = [[keep(-inner(av[m], pb[k])) for k in range(2)] for m in range(2)]
    g_aa = [keep(1.0 - inner(av[0], pa[0])), keep(-inner(av[0], pa[1])), keep(1.0 - inner(av[1], pa[1]))]
    g_bb = [keep(1.0 - inner(bv[0], pb[0])), keep(-inner(bv[0], pb[1])), keep(1.0 - inner(bv[1], pb[1]))]
    h_a = [keep(-(ea[m] + inner(pa[m], viq))) for m in range(2)]
    h_b = [keep(-(eb[m] + inner(pb[m], viq))) for m in range(2)]

    mj = [[m_ab[m][0] * jb[0][y] + m_ab[m][1] * jb[1][y] for y in range(6)] for m in range(2)]
    link = {}
    for x in range(6):
        for y in range(6):
            link[x, y] = ja[0][x] * mj[0][y] + ja[1][x] * mj[1][y]

    def diagonal(j, g):
        gj = [
            [g[0] * j[0][y] + g[1] * j[1][y] for y in range(6)],
            [g[1] * j[0][y] + g[2] * j[1][y] for y in range(6)],
        ]
        return [j[0][x] * gj[0][y] + j[1][x] * gj[1][y] for x, y in PAIRS]

    diag_own = diagonal(ja, g_aa)
    diag_other = diagonal(jb, g_bb)
    grad_own = [ja[0][x] * h_a[0] + ja[1][x] * h_a[1] for x in range(6)]
    grad_other = [jb[0][x] * h_b[0] + jb[1][x] * h_b[1] for x in range(6)]
    return diag_own, diag_other, link, grad_own, grad_other


def assemble_kernel(
    row_count, col_count, cam_in, pt_in, res_in, partner_in, row_in, count_in, map_in, send_ref,
    vals_ref, own_ref, acc_ref, links_ref, flat_ref, extra_ref, perm_ref,
    cam_ref, pt_ref, res_ref, partner_ref, map_ref, count_sm, map_sm, slab_sem, whole_sem,
):
    scn = partner_ref.shape[0]
    points = partner_ref.shape[1]
    scenes = map_ref.shape[1]
    wholes = [
        pltpu.make_async_copy(source, target, whole_sem.at[k])
        for k, (source, target) in enumerate(
            [(count_in, count_sm), (map_in, map_sm), (row_in, map_ref), (partner_in, partner_ref)]
        )
    ]

    def slab_copies(step):
        lanes = pl.ds(pl.multiple_of(step * LANES, LANES), LANES)
        return [
            pltpu.make_async_copy(
                source.at[..., lanes], target.at[..., lanes], slab_sem.at[k, step]
            )
            for k, (source, target) in enumerate([(cam_in, cam_ref), (pt_in, pt_ref), (res_in, res_ref)])
        ]

    wholes[0].start()
    for step in range(points // LANES):
        for copy in slab_copies(step):
            copy.start()
    for copy in wholes[1:]:
        copy.start()
    per_group = scn // row_count
    device = lax.axis_index("row") * col_count + lax.axis_index("col")
    slab = (scn, LANES)
    pitch = scn + 1

    own_ref[...] = jnp.zeros_like(own_ref)
    acc_ref[...] = jnp.zeros_like(acc_ref)
    extra_ref[...] = jnp.zeros_like(extra_ref)
    vals_ref[:, pl.ds(63 * pitch, scn), :] = jnp.zeros((points // LANES, scn, LANES), F32)

    wholes[0].wait()
    sub = iota(slab, 0)
    counts = jnp.zeros(slab, jnp.int32)
    for s in range(scn):
        counts = jnp.where(sub == s, count_sm[s], counts)

    def slab_step(step, carry):
        for copy in slab_copies(step):
            copy.wait()
        lanes = pl.ds(pl.multiple_of(step * LANES, LANES), LANES)

        def get(ref, *where):
            return ref[where + (slice(None), lanes)].astype(F32)

        ja = [[get(cam_ref, 0, m, x) for x in range(6)] for m in range(2)]
        jb = [[get(cam_ref, 1, m, x) for x in range(6)] for m in range(2)]
        pa = [[get(pt_ref, 0, m, x) for x in range(3)] for m in range(2)]
        pb = [[get(pt_ref, 1, m, x) for x in range(3)] for m in range(2)]
        ea = [get(res_ref, 0, m) for m in range(2)]
        eb = [get(res_ref, 1, m) for m in range(2)]
        live = (iota(slab, 1) + step * LANES) < counts
        diag_own, diag_other, link, grad_own, grad_other = point_values(ja, jb, pa, pb, ea, eb, live)

        def put(q, value):
            vals_ref[step, pl.ds(q * pitch, scn), :] = value

        def put_own(q, value):
            own_ref[pl.ds(q * pitch, scn), :] += value

        for x in range(3):
            for y in range(6):
                put(x * 6 + y, link[x, y])
                put(24 + x * 6 + y, link[x + 3, y])
        for x in range(6):
            put(18 + x, grad_other[x])
            put_own(2 + x, grad_own[x])
        for q in range(21):
            put(42 + q, diag_other[q])
            put_own(10 + q, diag_own[q])
        return carry

    lax.fori_loop(0, points // LANES, slab_step, 0)

    for copy in wholes[1:]:
        copy.wait()
    spots = iota((points, scenes), 1).astype(jnp.int16)
    mates = jnp.transpose(partner_ref[...]).astype(jnp.int16)

    def scene_step(s):
        values = jnp.concatenate(
            [vals_ref.at[t][pl.ds(s, 64, stride=pitch), :] for t in range(points // LANES)], axis=1
        )
        high, low = split_two(values)
        left = jnp.concatenate([high, low], axis=0)
        onehot = jnp.where(spots == mates[:, s : s + 1], jnp.asarray(1, BF16), jnp.asarray(0, BF16))
        both = jnp.dot(left, onehot, preferred_element_type=F32)
        total = both[:64] + both[64:]
        acc_ref[...] += total
        mine = map_sm[device * scn + s]
        rank = jnp.int32(0)
        for other in range(scn):
            rank = rank + (map_sm[device * scn + other] < mine).astype(jnp.int32)
        links_ref[pl.ds(pl.multiple_of(rank * 48, 16), 48), :] = total[:48].astype(BF16)

    for s in range(scn):
        scene_step(s)

    lane = iota((32, LANES), 1)
    own = jnp.zeros((32, LANES), F32)
    for s in range(scn):
        column = jnp.sum(own_ref[pl.ds(s, 32, stride=pitch), :], axis=1, keepdims=True)
        own = own + jnp.where(lane == s, column, 0.0)
    start = device * scn
    own = pltpu.roll(own, lax.rem(start, LANES), 1)
    tile_at = lax.div(start, LANES)
    for t in range(scenes // LANES):
        cols = pl.ds(t * LANES, LANES)
        whole = jnp.concatenate([acc_ref[16:24, cols], acc_ref[40:64, cols]], axis=0)
        whole = whole + jnp.where(tile_at == t, own, 0.0)
        high, low = split_two(whole)
        flat_ref[0:32, cols] = high.astype(F32)
        flat_ref[32:64, cols] = low.astype(F32)
    per_col = -(-21 // col_count)
    for c in range(col_count):
        for i in range(per_col):
            q = c * per_col + i
            if q < 21:
                extra_ref[c * 8 + 2 + i : c * 8 + 3 + i, :] = flat_ref[10 + q : 11 + q, :]
                extra_ref[c * 8 + 5 + i : c * 8 + 6 + i, :] = flat_ref[42 + q : 43 + q, :]
    base = col_count * 8
    extra_ref[base : base + 8, :] = flat_ref[0:8, :]
    extra_ref[base + 8 : base + 16, :] = flat_ref[32:40, :]

    places = jnp.transpose(jnp.broadcast_to(map_ref[...], (8, scenes)))[:, :1]
    onto = jnp.where(iota((scenes, scenes), 1) == places, 1.0, 0.0).astype(BF16)
    left = jnp.concatenate([links_ref[...], extra_ref[...].astype(BF16)], axis=0)
    perm_ref[...] = jnp.dot(left, onto, preferred_element_type=F32)

    top = scn * 48
    first = iota((8, LANES), 1) < HALF
    keep_rows = iota((8, LANES), 0) < 2
    first24 = iota((24, LANES), 1) < HALF

    def merge(low_part, high_part, mask):
        even = jnp.where(mask, low_part, pltpu.roll(high_part, HALF, 1))
        odd = jnp.where(mask, pltpu.roll(low_part, HALF, 1), high_part)
        return even, odd

    for j in range(col_count // 2):
        cols = pl.ds(j * LANES, LANES)
        grad_cols = merge(
            perm_ref[top + base : top + base + 8, cols],
            perm_ref[top + base + 8 : top + base + 16, cols],
            first,
        )
        for r in range(row_count):
            rows = pl.ds(r * LANES, LANES)
            grad_high = perm_ref[top + base : top + base + 8, rows]
            grad_low = perm_ref[top + base + 8 : top + base + 16, rows]
            for slot in range(per_group):
                at = (r * per_group + slot) * 48
                pieces = merge(perm_ref[at : at + 24, cols], perm_ref[at + 24 : at + 48, cols], first24)
                for k in range(2):
                    c = 2 * j + k
                    if slot == 0:
                        extra = grad_high
                    elif slot == 1:
                        extra = grad_low
                    elif slot == 2:
                        extra = grad_cols[k]
                    else:
                        extra = perm_ref[top + c * 8 : top + c * 8 + 8, rows]
                    tail = jnp.where(keep_rows, pieces[k][16:24], extra)
                    block = jnp.concatenate([pieces[k][0:16], tail], axis=0)
                    send_ref[r * col_count + c, slot * 24 : slot * 24 + 24, :] = block.astype(BF16)


def tile_matvec(tile_ref, own_ref, rows_part, cols_part, rows_ref):
    which = iota((8, LANES), 0)
    turned = jnp.transpose(cols_part)[:HALF]
    forward = [jnp.zeros((8, LANES), F32) for _ in range(6)]
    backward = []
    for y in range(6):
        column = jnp.broadcast_to(turned[:, y : y + 1], (HALF, LANES))
        total = jnp.zeros((HALF, LANES), F32)
        for x in range(6):
            block = tile_ref[x * 6 + y].astype(F32)
            forward[x] = forward[x] + jnp.sum((block * column).reshape(HALF // 8, 8, LANES), axis=0)
            total = total + block * rows_part[x : x + 1, :]
        backward.append(total)
    sides = []
    for y in range(3):
        pair = jnp.concatenate([backward[y], backward[y + 3]], axis=0)
        sides.append(jnp.sum(jnp.transpose(pair), axis=0, keepdims=True))
    out = jnp.zeros((8, LANES), F32)
    for x in range(6):
        out = jnp.where(which == x, jnp.sum(forward[x], axis=0, keepdims=True), out)
    rows_ref[...] = rows_part
    col = lax.axis_index("col")
    per_col = -(-21 // lax.axis_size("col"))
    for i in range(per_col):
        q = jnp.minimum(col * per_col + i, 20)
        x = jnp.int32(0)
        start = jnp.int32(0)
        for line in range(1, 6):
            past = (q >= PAIRS.index((line, line))).astype(jnp.int32)
            x = x + past
            start = start + past * (7 - line)
        y = q - start + x
        weight = own_ref[i : i + 1, :]
        at_x = rows_ref[pl.ds(x, 1), :] * weight
        at_y = rows_ref[pl.ds(y, 1), :] * weight
        out = out + jnp.where(which == x, at_y, 0.0)
        out = out + jnp.where((which == y) & (x != y), at_x, 0.0)
    return out, sides


def write_partials(out, sides, line, part_ref):
    rows = [out[x : x + 1, :] for x in range(6)] + sides
    if line is not None:
        rows.append(line)
    for n in range(part_ref.shape[0]):
        for k, row in enumerate(rows):
            part_ref[n, :, k * LANES : (k + 1) * LANES] = row


def first_kernel(
    row_count, col_count, got_ref, map_ref, tile_ref, own_ref, part_ref, wide_ref, rows_ref,
):
    devices = got_ref.shape[0]
    scenes = map_ref.shape[1]
    scn = scenes // devices
    per_group = scn // row_count
    tile_rows = scenes // row_count
    row = lax.axis_index("row")
    tiles = jnp.concatenate(
        [map_ref[:, t * LANES : (t + 1) * LANES] for t in range(scenes // LANES)], axis=0
    )
    groups = scenes // LANES
    place = iota((groups, LANES), 1) % scn
    rank = jnp.zeros((groups, LANES), jnp.int32)
    for shift in range(1, scn):
        before = pltpu.roll(tiles, shift, 1)
        after = pltpu.roll(tiles, LANES - shift, 1)
        rank = rank + ((before < tiles) & (place >= shift)).astype(jnp.int32)
        rank = rank + ((after < tiles) & (place + shift < scn)).astype(jnp.int32)
    scene_id = iota((groups, LANES), 0) * LANES + iota((groups, LANES), 1)
    slot_at = (scene_id // scn) * per_group + rank % per_group
    local = tiles - row * tile_rows
    slot_at = jnp.where((local >= 0) & (local < tile_rows), slot_at, -1)
    select = jnp.zeros((tile_rows, tile_rows), F32)
    for t in range(groups):
        to_row = jnp.where(iota((tile_rows, LANES), 0) == local[t : t + 1, :], 1.0, 0.0).astype(BF16)
        from_slot = jnp.where(iota((tile_rows, LANES), 0) == slot_at[t : t + 1, :], 1.0, 0.0).astype(BF16)
        select = select + lax.dot_general(to_row, from_slot, CONTRACT_LAST, preferred_element_type=F32)
    select = select.astype(BF16)

    for n in range(devices):
        block = got_ref[n].astype(F32)
        for slot in range(per_group):
            wide_ref[pl.ds((n * per_group + slot) * 25, 24), :] = block[slot * 24 : slot * 24 + 24]
    for k in range(18):
        picked = wide_ref[pl.ds(k, tile_rows, stride=25), :].astype(BF16)
        block = lax.dot_general(picked, select, (((0,), (1,)), ((), ())), preferred_element_type=F32)
        tile_ref[k] = block[:HALF].astype(BF16)
        tile_ref[k + 18] = block[HALF:].astype(BF16)
    extras = []
    for slot in range(per_group):
        total = got_ref[0, slot * 24 + 16 : slot * 24 + 24, :].astype(F32)
        for n in range(1, devices):
            total = total + got_ref[n, slot * 24 + 16 : slot * 24 + 24, :].astype(F32)
        extras.append(pltpu.roll(total, 6, 0))
    used = iota((8, LANES), 0) < 6
    rows_part = jnp.where(used, extras[0] + extras[1], 0.0)
    cols_part = jnp.where(used, extras[2] + pltpu.roll(extras[2], HALF, 1), 0.0)
    own_ref[...] = extras[3] + pltpu.roll(extras[3], 5, 0)
    out, sides = tile_matvec(tile_ref, own_ref, rows_part, cols_part, rows_ref)
    rows_ref[...] = rows_part
    line = rows_ref[pl.ds(jnp.minimum(lax.axis_index("col"), 5), 1), :]
    write_partials(out, sides, line, part_ref)


def gather_image(row_count, col_count, got_ref, image_ref):
    first = iota((1, LANES), 1) < HALF
    side = 6 * LANES
    cols = []
    for c in range(col_count):
        total = got_ref[c, :, side : side + 3 * LANES]
        for r in range(1, row_count):
            total = total + got_ref[r * col_count + c, :, side : side + 3 * LANES]
        cols.append(total)
    for r in range(row_count):
        total = got_ref[r * col_count, :, 0:side]
        for c in range(1, col_count):
            total = total + got_ref[r * col_count + c, :, 0:side]
        image_ref[r] = jnp.zeros((8, LANES), F32)
        for t in range(3):
            left = cols[2 * r][:, t * LANES : (t + 1) * LANES]
            right = cols[2 * r + 1][:, t * LANES : (t + 1) * LANES]
            low = jnp.where(first, left, pltpu.roll(right, HALF, 1))
            high = jnp.where(first, pltpu.roll(left, HALF, 1), right)
            image_ref[r, t : t + 1, :] = total[:, t * LANES : (t + 1) * LANES] + low
            image_ref[r, t + 3 : t + 4, :] = total[:, (t + 3) * LANES : (t + 4) * LANES] + high


def inner_all(left, right):
    return jnp.sum(jnp.sum(left * right, axis=0), keepdims=True)


def step_kernel(
    row_count, col_count, begin, got_ref, tile_ref, own_ref, state_ref, next_ref, part_ref,
    *rest,
):
    if begin:
        coupling_ref, image_ref, rows_ref, copy_sem = rest
        copy = pltpu.make_async_copy(tile_ref, coupling_ref, copy_sem)
        copy.start()
    else:
        image_ref, rows_ref = rest
    gather_image(row_count, col_count, got_ref, image_ref)
    if begin:
        for r in range(row_count):
            next_ref[1, r] = jnp.zeros((8, LANES), F32)
            for x in range(6):
                next_ref[1, r, x : x + 1, :] = got_ref[r * col_count + x, :, 9 * LANES : 10 * LANES]
        remainder = next_ref[1]
        direction = remainder
        answer = jnp.zeros_like(remainder)
    else:
        answer, remainder, direction = state_ref[0], state_ref[1], state_ref[2]
    norm_now = inner_all(remainder, remainder)
    image = CAMERA_DAMPING * direction + image_ref[...]
    alpha = norm_now / inner_all(direction, image)
    answer = answer + alpha * direction
    remainder = remainder - alpha * image
    norm_next = inner_all(remainder, remainder)
    direction = remainder + norm_next / norm_now * direction
    next_ref[0] = answer
    next_ref[1] = remainder
    next_ref[2] = direction
    col = lax.axis_index("col")
    rows_part = next_ref[2, lax.axis_index("row")]
    wide = next_ref[2, lax.div(col, 2)]
    turned = pltpu.roll(wide, HALF, 1)
    cols_part = jnp.where(iota((8, LANES), 0) * 0 == lax.rem(col, 2), wide, turned)
    out, sides = tile_matvec(tile_ref, own_ref, rows_part, cols_part, rows_ref)
    write_partials(out, sides, None, part_ref)
    if begin:
        copy.wait()


def last_kernel(row_count, col_count, got_ref, state_ref, answer_ref, remainder_ref, image_ref):
    gather_image(row_count, col_count, got_ref, image_ref)
    remainder, direction = state_ref[1], state_ref[2]
    norm_now = inner_all(remainder, remainder)
    image_ref[...] = CAMERA_DAMPING * direction + image_ref[...]
    alpha = norm_now / inner_all(direction, image_ref[...])
    row = lax.axis_index("row")
    answer_ref[...] = (state_ref[0, row] + alpha * state_ref[2, row])[:6]
    remainder_ref[...] = (state_ref[1, row] - alpha * image_ref[row])[:6]


def vmem():
    return pl.BlockSpec(memory_space=pltpu.VMEM)


def hbm():
    return pl.BlockSpec(memory_space=pltpu.HBM)


def small_limit(mib):
    return pltpu.CompilerParams(vmem_limit_bytes=mib << 20)


def packed_shards(cam_jac, pt_jac, resid, partner, count, tile_map):
    row_count = lax.axis_size("row")
    col_count = lax.axis_size("col")
    devices = row_count * col_count
    scenes = tile_map.shape[0]
    scn, points = partner.shape
    map_row = tile_map.reshape(1, scenes)

    def bind(kernel, *fixed):
        def run(*refs):
            return kernel(row_count, col_count, *fixed, *refs)

        return run

    extra_rows = col_count * 8 + 16
    send = pl.pallas_call(
        bind(assemble_kernel),
        out_shape=jax.ShapeDtypeStruct((devices, 96, LANES), BF16),
        in_specs=[hbm()] * 7,
        out_specs=vmem(),
        scratch_shapes=[
            pltpu.VMEM((points // LANES, 64 * (scn + 1), LANES), F32),
            pltpu.VMEM((32 * (scn + 1), LANES), F32),
            pltpu.VMEM((64, scenes), F32),
            pltpu.VMEM((48 * scn, scenes), BF16),
            pltpu.VMEM((64, scenes), F32),
            pltpu.VMEM((extra_rows, scenes), F32),
            pltpu.VMEM((48 * scn + extra_rows, scenes), F32),
            pltpu.VMEM(cam_jac.shape, BF16),
            pltpu.VMEM(pt_jac.shape, BF16),
            pltpu.VMEM(resid.shape, BF16),
            pltpu.VMEM(partner.shape, jnp.int32),
            pltpu.VMEM(map_row.shape, jnp.int32),
            pltpu.SMEM(count.shape, jnp.int32),
            pltpu.SMEM(tile_map.shape, jnp.int32),
            pltpu.SemaphoreType.DMA((3, points // LANES)),
            pltpu.SemaphoreType.DMA((4,)),
        ],
        compiler_params=small_limit(36),
        name="assemble",
    )(
        *[
            pltpu.with_memory_space_constraint(value, pltpu.HBM)
            for value in (cam_jac, pt_jac, resid, partner, map_row, count, tile_map)
        ]
    )
    got = lax.all_to_all(send, AXES, 0, 0, tiled=True)
    tile_rows = scenes // row_count
    tile, own, part = pl.pallas_call(
        bind(first_kernel),
        out_shape=(
            jax.ShapeDtypeStruct((36, HALF, tile_rows), BF16),
            jax.ShapeDtypeStruct((8, LANES), F32),
            jax.ShapeDtypeStruct((devices, 1, 10 * LANES), F32),
        ),
        in_specs=[vmem()] * 2,
        out_specs=(vmem(),) * 3,
        scratch_shapes=[pltpu.VMEM((tile_rows * 25, LANES), F32), pltpu.VMEM((8, LANES), F32)],
        compiler_params=small_limit(16),
        name="first",
    )(got, map_row)
    state = jnp.zeros((3, row_count, 8, LANES), F32)
    for turn in range(ITERS - 1):
        got = lax.all_to_all(part, AXES, 0, 0, tiled=True)
        begin = turn == 0
        outs = [
            jax.ShapeDtypeStruct((3, row_count, 8, LANES), F32),
            jax.ShapeDtypeStruct((devices, 1, 9 * LANES), F32),
        ]
        places = [vmem()] * 2
        scratch = [pltpu.VMEM((row_count, 8, LANES), F32), pltpu.VMEM((8, LANES), F32)]
        if begin:
            outs.append(jax.ShapeDtypeStruct(tile.shape, BF16))
            places.append(hbm())
            scratch.append(pltpu.SemaphoreType.DMA(()))
        state, part, *rest = pl.pallas_call(
            bind(step_kernel, begin),
            out_shape=outs,
            in_specs=[vmem()] * 4,
            out_specs=places,
            scratch_shapes=scratch,
            compiler_params=small_limit(8),
            name="step",
        )(got, tile, own, state)
        if begin:
            coupling = rest[0]
    got = lax.all_to_all(part, AXES, 0, 0, tiled=True)
    answer, remainder = pl.pallas_call(
        bind(last_kernel),
        out_shape=(jax.ShapeDtypeStruct((6, tile_rows), F32),) * 2,
        in_specs=[vmem()] * 2,
        out_specs=(vmem(),) * 2,
        scratch_shapes=[pltpu.VMEM((row_count, 8, LANES), F32)],
        compiler_params=small_limit(4),
        name="last",
    )(got, state)
    return jnp.swapaxes(coupling.reshape(6, 6, HALF, tile_rows), 2, 3), answer, remainder


def cross_product(first_vec, second_vec):
    return jnp.stack(
        [
            first_vec[1] * second_vec[2] - first_vec[2] * second_vec[1],
            first_vec[2] * second_vec[0] - first_vec[0] * second_vec[2],
            first_vec[0] * second_vec[1] - first_vec[1] * second_vec[0],
        ],
        axis=0,
    )


def point_terms(camera, points_jac, errors):
    camera = camera.astype(jnp.float32)
    points_jac = points_jac.astype(jnp.float32)
    errors = errors.astype(jnp.float32)
    own_jac, other_jac = (camera[0], camera[1])
    own_point, other_point = (points_jac[0], points_jac[1])
    own_error, other_error = (errors[0], errors[1])
    point_hessian = jnp.sum(own_point[:, :, None] * own_point[:, None, :], axis=0)
    point_hessian = point_hessian + jnp.sum(
        other_point[:, :, None] * other_point[:, None, :], axis=0
    )
    point_hessian = point_hessian + POINT_DAMPING * jnp.eye(3, dtype=jnp.float32)[:, :, None, None]
    first_row, second_row, third_row = (point_hessian[0], point_hessian[1], point_hessian[2])
    cofactor_first = cross_product(second_row, third_row)
    cofactor_second = cross_product(third_row, first_row)
    cofactor_third = cross_product(first_row, second_row)
    determinant = jnp.sum(first_row * cofactor_first, axis=0)
    inverse = jnp.stack([cofactor_first, cofactor_second, cofactor_third], axis=1) / determinant
    w_own = jnp.sum(own_jac[:, :, None] * own_point[:, None, :], axis=0)
    w_other = jnp.sum(other_jac[:, :, None] * other_point[:, None, :], axis=0)
    point_rhs = -(
        jnp.sum(own_point * own_error[:, None], axis=0)
        + jnp.sum(other_point * other_error[:, None], axis=0)
    )
    own_vi = jnp.sum(w_own[:, :, None] * inverse[None, :, :], axis=1)
    other_vi = jnp.sum(w_other[:, :, None] * inverse[None, :, :], axis=1)
    diag_own = jnp.sum(own_jac[:, :, None] * own_jac[:, None, :], axis=0) - jnp.sum(
        own_vi[:, None, :] * w_own[None, :, :], axis=2
    )
    diag_other = jnp.sum(other_jac[:, :, None] * other_jac[:, None, :], axis=0) - jnp.sum(
        other_vi[:, None, :] * w_other[None, :, :], axis=2
    )
    link = -jnp.sum(own_vi[:, None, :] * w_other[None, :, :], axis=2)
    grad_own = -jnp.sum(own_jac * own_error[:, None], axis=0) - jnp.sum(
        own_vi * point_rhs[None], axis=1
    )
    grad_other = -jnp.sum(other_jac * other_error[:, None], axis=0) - jnp.sum(
        other_vi * point_rhs[None], axis=1
    )
    return (diag_own, diag_other, link, grad_own, grad_other)


def conjugate_steps(right_side, apply_operator, inner_product):
    solution = jnp.zeros_like(right_side)
    remainder = right_side
    direction = right_side
    norm_now = inner_product(remainder, remainder)
    for iteration in range(ITERS):
        product_vec = apply_operator(direction)
        step_size = norm_now / inner_product(direction, product_vec)
        solution = solution + step_size * direction
        remainder = remainder - step_size * product_vec
        norm_next = inner_product(remainder, remainder)
        direction = remainder + norm_next / norm_now * direction
        norm_now = norm_next
    return (solution, remainder)


def plain_shards(cam_jac, pt_jac, resid, partner, count, tile_map):
    row_count = lax.axis_size("row")
    col_count = lax.axis_size("col")
    scenes = tile_map.shape[0]
    scn_local = partner.shape[0]
    points = partner.shape[1]
    tile_rows = scenes // row_count
    tile_cols = scenes // col_count
    per_group = scn_local // row_count
    row_index = lax.axis_index("row")
    col_index = lax.axis_index("col")
    device = row_index * col_count + col_index
    positions = jnp.arange(scenes, dtype=jnp.int32)
    tile_own = lax.dynamic_slice_in_dim(tile_map, device * scn_local, scn_local)
    local_rank = jnp.sum((tile_own[None, :] < tile_own[:, None]).astype(jnp.int32), axis=1)
    active = (jnp.arange(points, dtype=jnp.int32)[None, :] < count[:, None]).astype(jnp.float32)
    diag_own, diag_other, link, grad_own, grad_other = point_terms(cam_jac, pt_jac, resid)
    values = (
        jnp.concatenate(
            [
                link.reshape(36, scn_local, points),
                diag_other.reshape(36, scn_local, points),
                grad_other,
            ],
            axis=0,
        )
        * active[None]
    )
    values = jnp.moveaxis(values, 1, 0)

    def scene_sums(item):
        scene_values, scene_partner = item
        hits = scene_partner[:, None] == positions[None, :]
        tile_other = jnp.sum(jnp.where(hits, tile_map[None, :], 0), axis=1)
        onehot = (tile_other[:, None] == positions[None, :]).astype(jnp.float32)
        return jnp.dot(
            scene_values,
            onehot,
            precision=lax.Precision.HIGHEST,
            preferred_element_type=jnp.float32,
        )

    per_scene = lax.map(scene_sums, (values, partner))
    link_rows = per_scene[:, :36, :]
    other_sum = jnp.sum(per_scene[:, 36:, :], axis=0)
    ordering = (local_rank[None, :] == jnp.arange(scn_local, dtype=jnp.int32)[:, None]).astype(
        jnp.float32
    )
    panel = jnp.einsum("rs,sxc->xrc", ordering, link_rows, precision=lax.Precision.HIGHEST)
    panel = panel.reshape(36, row_count, per_group, col_count, tile_cols).transpose(0, 1, 3, 2, 4)
    panel_short = panel.astype(jnp.bfloat16)
    own_onehot = (tile_own[:, None] == positions[None, :]).astype(jnp.float32)
    own_diag = jnp.sum(diag_own * active, axis=-1).reshape(36, scn_local)
    own_grad = jnp.sum(grad_own * active, axis=-1)
    own_both = jnp.concatenate([own_diag, own_grad], axis=0)
    own_spread = jnp.dot(
        own_both, own_onehot, precision=lax.Precision.HIGHEST, preferred_element_type=jnp.float32
    )
    both_part = own_spread + other_sum
    diag_part = both_part[:36]
    grad_part = both_part[36:]
    shaped = panel_short.reshape(36, row_count * col_count, per_group, tile_cols)
    received = lax.all_to_all(shaped, ("row", "col"), split_axis=1, concat_axis=1, tiled=True)
    received = received.reshape(36, tile_rows, tile_cols)
    diag_all, grad_all = lax.psum((diag_part, grad_part), ("row", "col"))
    row_start = row_index * tile_rows
    col_start = col_index * tile_cols
    devices = scenes // scn_local
    tiles_grid = tile_map.reshape(devices, scn_local)
    inblock = (tiles_grid >= row_start) & (tiles_grid < row_start + tile_rows)
    lower = (tiles_grid[:, None, :] < tiles_grid[:, :, None]) & inblock[:, None, :]
    within_all = jnp.sum(lower.astype(jnp.int32), axis=2)
    slot_from = (jnp.arange(devices, dtype=jnp.int32)[:, None] * per_group + within_all).reshape(-1)
    slot_to = (tiles_grid - row_start).reshape(-1)
    slots = jnp.arange(tile_rows, dtype=jnp.int32)
    to_table = ((slot_to[:, None] == slots[None, :]) & inblock.reshape(-1)[:, None]).astype(
        jnp.bfloat16
    )
    from_table = (slot_from[:, None] == slots[None, :]).astype(jnp.bfloat16)
    selection = jnp.dot(to_table.T, from_table, preferred_element_type=jnp.float32).astype(
        jnp.bfloat16
    )
    coupling_tile = jnp.einsum(
        "pk,xkc->xpc", selection, received, preferred_element_type=jnp.float32
    )
    coupling_tile = coupling_tile.astype(jnp.bfloat16).reshape(6, 6, tile_rows, tile_cols)
    coupling_wide = coupling_tile.astype(jnp.float32)
    zero_at = row_index * 0

    def tile_products(rows_part, cols_part):
        forward = jnp.einsum(
            "xyij,yj->xi", coupling_wide, cols_part, precision=lax.Precision.HIGHEST
        )
        backward = jnp.einsum(
            "xyij,xi->yj", coupling_wide, rows_part, precision=lax.Precision.HIGHEST
        )
        empty = jnp.zeros((6, scenes), jnp.float32)
        spread = lax.dynamic_update_slice(empty, forward, (zero_at, row_start))
        spread = spread + lax.dynamic_update_slice(empty, backward, (zero_at, col_start))
        return lax.psum(spread, ("row", "col"))

    diag_blocks = diag_all.reshape(6, 6, scenes)

    def apply_full(direction):
        rows_part = lax.dynamic_slice_in_dim(direction, row_start, tile_rows, 1)
        cols_part = lax.dynamic_slice_in_dim(direction, col_start, tile_cols, 1)
        summed = tile_products(rows_part, cols_part)
        result = CAMERA_DAMPING * direction
        result = result + jnp.einsum(
            "xyi,yi->xi", diag_blocks, direction, precision=lax.Precision.HIGHEST
        )
        return result + summed

    def inner_full(first_vec, second_vec):
        return jnp.sum(first_vec * second_vec)

    whole_solution, whole_remainder = conjugate_steps(grad_all, apply_full, inner_full)
    solution = lax.dynamic_slice_in_dim(whole_solution, row_start, tile_rows, 1)
    remainder = lax.dynamic_slice_in_dim(whole_remainder, row_start, tile_rows, 1)
    return (coupling_tile, solution, remainder)


def shards(cam_jac, pt_jac, resid, partner, count, tile_map):
    row_count = lax.axis_size("row")
    col_count = lax.axis_size("col")
    scenes = tile_map.shape[0]
    scn, points = partner.shape
    packs = (
        scenes == col_count * HALF
        and scenes == row_count * LANES
        and scn == row_count * 4
        and LANES % scn == 0
        and points % LANES == 0
        and col_count >= 7
    )
    run = packed_shards if packs else plain_shards
    return run(cam_jac, pt_jac, resid, partner, count, tile_map)


def solution(mesh):
    return jax.shard_map(
        shards,
        mesh=mesh,
        in_specs=(
            P(None, None, None, AXES, None),
            P(None, None, None, AXES, None),
            P(None, None, AXES, None),
            P(AXES, None),
            P(AXES),
            P(),
        ),
        out_specs=(P(None, None, "row", "col"), P(None, "row"), P(None, "row")),
        check_vma=False,
    )
```

```python
import jax
import jax.numpy as jnp
from jax import lax
from jax.experimental import pallas as pl
from jax.experimental.pallas import tpu as pltpu
from jax.sharding import PartitionSpec as P

ITERS = 3
CAMERA_DAMPING = 1.0
POINT_DAMPING = 1.0
AXES = ("row", "col")
LANES = 128
HALF = 64
F32 = jnp.float32
BF16 = jnp.bfloat16
PAIRS = [(x, y) for x in range(6) for y in range(x, 6)]
CONTRACT_LAST = (((1,), (1,)), ((), ()))


def iota(shape, dim):
    return lax.broadcasted_iota(jnp.int32, shape, dim)


def split_two(value):
    high = value.astype(BF16)
    low = (value - high.astype(F32)).astype(BF16)
    return high, low


def point_values(ja, jb, pa, pb, ea, eb, live):
    one = POINT_DAMPING
    hess = {}
    for x in range(3):
        for y in range(x, 3):
            h = pa[0][x] * pa[0][y] + pa[1][x] * pa[1][y]
            h = h + (pb[0][x] * pb[0][y] + pb[1][x] * pb[1][y])
            hess[x, y] = h + one if x == y else h
    a, b, c = hess[0, 0], hess[0, 1], hess[0, 2]
    d, e, f = hess[1, 1], hess[1, 2], hess[2, 2]
    c00 = d * f - e * e
    c01 = c * e - b * f
    c02 = b * e - c * d
    c11 = a * f - c * c
    c12 = b * c - a * e
    c22 = a * d - b * b
    det = a * c00 + b * c01 + c * c02
    inv = 1.0 / det
    vi = [[c00 * inv, c01 * inv, c02 * inv], [None, c11 * inv, c12 * inv], [None, None, c22 * inv]]
    vi[1][0], vi[2][0], vi[2][1] = vi[0][1], vi[0][2], vi[1][2]
    q = [
        -((pa[0][k] * ea[0] + pa[1][k] * ea[1]) + (pb[0][k] * eb[0] + pb[1][k] * eb[1]))
        for k in range(3)
    ]
    viq = [vi[k][0] * q[0] + vi[k][1] * q[1] + vi[k][2] * q[2] for k in range(3)]

    def times_vi(p):
        return [
            [p[m][0] * vi[0][k] + p[m][1] * vi[1][k] + p[m][2] * vi[2][k] for k in range(3)]
            for m in range(2)
        ]

    def inner(left, right):
        return left[0] * right[0] + left[1] * right[1] + left[2] * right[2]

    def keep(value):
        return jnp.where(live, value, 0.0)

    av = times_vi(pa)
    bv = times_vi(pb)
    m_ab = [[keep(-inner(av[m], pb[k])) for k in range(2)] for m in range(2)]
    g_aa = [keep(1.0 - inner(av[0], pa[0])), keep(-inner(av[0], pa[1])), keep(1.0 - inner(av[1], pa[1]))]
    g_bb = [keep(1.0 - inner(bv[0], pb[0])), keep(-inner(bv[0], pb[1])), keep(1.0 - inner(bv[1], pb[1]))]
    h_a = [keep(-(ea[m] + inner(pa[m], viq))) for m in range(2)]
    h_b = [keep(-(eb[m] + inner(pb[m], viq))) for m in range(2)]

    mj = [[m_ab[m][0] * jb[0][y] + m_ab[m][1] * jb[1][y] for y in range(6)] for m in range(2)]
    link = {}
    for x in range(6):
        for y in range(6):
            link[x, y] = ja[0][x] * mj[0][y] + ja[1][x] * mj[1][y]

    def diagonal(j, g):
        gj = [
            [g[0] * j[0][y] + g[1] * j[1][y] for y in range(6)],
            [g[1] * j[0][y] + g[2] * j[1][y] for y in range(6)],
        ]
        return [j[0][x] * gj[0][y] + j[1][x] * gj[1][y] for x, y in PAIRS]

    diag_own = diagonal(ja, g_aa)
    diag_other = diagonal(jb, g_bb)
    grad_own = [ja[0][x] * h_a[0] + ja[1][x] * h_a[1] for x in range(6)]
    grad_other = [jb[0][x] * h_b[0] + jb[1][x] * h_b[1] for x in range(6)]
    return diag_own, diag_other, link, grad_own, grad_other


def selection(row_count, map_ref, scn, tile_rows, per_group):
    scenes = map_ref.shape[1]
    row = lax.axis_index("row")
    tiles = jnp.concatenate(
        [map_ref[:, t * LANES : (t + 1) * LANES] for t in range(scenes // LANES)], axis=0
    )
    groups = scenes // LANES
    place = iota((groups, LANES), 1) % scn
    rank = jnp.zeros((groups, LANES), jnp.int32)
    for shift in range(1, scn):
        before = pltpu.roll(tiles, shift, 1)
        after = pltpu.roll(tiles, LANES - shift, 1)
        rank = rank + ((before < tiles) & (place >= shift)).astype(jnp.int32)
        rank = rank + ((after < tiles) & (place + shift < scn)).astype(jnp.int32)
    scene_id = iota((groups, LANES), 0) * LANES + iota((groups, LANES), 1)
    slot_at = (scene_id // scn) * 8 + rank % per_group
    local = tiles - row * tile_rows
    slot_at = jnp.where((local >= 0) & (local < tile_rows), slot_at, -1)
    deep = scenes // scn * 8
    select = jnp.zeros((deep, tile_rows), F32)
    for t in range(groups):
        to_row = jnp.where(iota((tile_rows, LANES), 0) == local[t : t + 1, :], 1.0, 0.0).astype(BF16)
        from_slot = jnp.where(iota((deep, LANES), 0) == slot_at[t : t + 1, :], 1.0, 0.0).astype(BF16)
        select = select + lax.dot_general(from_slot, to_row, CONTRACT_LAST, preferred_element_type=F32)
    return jnp.concatenate([select, pltpu.roll(select, 4, 0)], axis=1).astype(BF16)


def assemble_kernel(
    row_count, col_count, cam_in, pt_in, res_in, partner_in, row_in, count_in, map_in, send_ref,
    select_ref,
    vals_ref, own_ref, acc_ref, links_ref, flat_ref, extra_ref, perm_ref,
    cam_ref, pt_ref, res_ref, partner_ref, map_ref, count_sm, map_sm, slab_sem, whole_sem,
):
    scn = partner_ref.shape[0]
    points = partner_ref.shape[1]
    scenes = map_ref.shape[1]
    wholes = [
        pltpu.make_async_copy(source, target, whole_sem.at[k])
        for k, (source, target) in enumerate(
            [(count_in, count_sm), (map_in, map_sm), (row_in, map_ref), (partner_in, partner_ref)]
        )
    ]

    def slab_copies(step):
        lanes = pl.ds(pl.multiple_of(step * LANES, LANES), LANES)
        return [
            pltpu.make_async_copy(
                source.at[..., lanes], target.at[..., lanes], slab_sem.at[k, step]
            )
            for k, (source, target) in enumerate([(cam_in, cam_ref), (pt_in, pt_ref), (res_in, res_ref)])
        ]

    wholes[0].start()
    for step in range(points // LANES):
        for copy in slab_copies(step):
            copy.start()
    for copy in wholes[1:]:
        copy.start()
    per_group = scn // row_count
    device = lax.axis_index("row") * col_count + lax.axis_index("col")
    slab = (scn, LANES)
    pitch = scn + 1

    own_ref[...] = jnp.zeros_like(own_ref)
    acc_ref[...] = jnp.zeros_like(acc_ref)
    extra_ref[...] = jnp.zeros_like(extra_ref)
    vals_ref[:, pl.ds(63 * pitch, scn), :] = jnp.zeros((points // LANES, scn, LANES), F32)

    wholes[0].wait()
    sub = iota(slab, 0)
    counts = jnp.zeros(slab, jnp.int32)
    for s in range(scn):
        counts = jnp.where(sub == s, count_sm[s], counts)

    def slab_step(step, carry):
        for copy in slab_copies(step):
            copy.wait()
        lanes = pl.ds(pl.multiple_of(step * LANES, LANES), LANES)

        def get(ref, *where):
            return ref[where + (slice(None), lanes)].astype(F32)

        ja = [[get(cam_ref, 0, m, x) for x in range(6)] for m in range(2)]
        jb = [[get(cam_ref, 1, m, x) for x in range(6)] for m in range(2)]
        pa = [[get(pt_ref, 0, m, x) for x in range(3)] for m in range(2)]
        pb = [[get(pt_ref, 1, m, x) for x in range(3)] for m in range(2)]
        ea = [get(res_ref, 0, m) for m in range(2)]
        eb = [get(res_ref, 1, m) for m in range(2)]
        live = (iota(slab, 1) + step * LANES) < counts
        diag_own, diag_other, link, grad_own, grad_other = point_values(ja, jb, pa, pb, ea, eb, live)

        def put(q, value):
            vals_ref[step, pl.ds(q * pitch, scn), :] = value

        def put_own(q, value):
            own_ref[pl.ds(q * pitch, scn), :] += value

        for x in range(3):
            for y in range(6):
                put(x * 6 + y, link[x, y])
                put(24 + x * 6 + y, link[x + 3, y])
        for x in range(6):
            put(18 + x, grad_other[x])
            put_own(2 + x, grad_own[x])
        for q in range(21):
            put(42 + q, diag_other[q])
            put_own(10 + q, diag_own[q])
        return carry

    lax.fori_loop(0, points // LANES, slab_step, 0)

    for copy in wholes[1:]:
        copy.wait()
    select_ref[...] = selection(row_count, map_ref, scn, scenes // row_count, per_group)
    spots = iota((points, scenes), 1).astype(jnp.int16)
    mates = jnp.transpose(partner_ref[...]).astype(jnp.int16)

    def scene_step(s):
        values = jnp.concatenate(
            [vals_ref.at[t][pl.ds(s, 64, stride=pitch), :] for t in range(points // LANES)], axis=1
        )
        high, low = split_two(values)
        left = jnp.concatenate([high, low], axis=0)
        onehot = jnp.where(spots == mates[:, s : s + 1], jnp.asarray(1, BF16), jnp.asarray(0, BF16))
        both = jnp.dot(left, onehot, preferred_element_type=F32)
        total = both[:64] + both[64:]
        acc_ref[...] += total
        mine = map_sm[device * scn + s]
        rank = jnp.int32(0)
        for other in range(scn):
            rank = rank + (map_sm[device * scn + other] < mine).astype(jnp.int32)
        base = lax.div(rank, per_group) * (36 * per_group) + lax.rem(rank, per_group)
        for t in range(scenes // LANES):
            cols = slice(t * LANES, (t + 1) * LANES)
            links_ref.at[t][pl.ds(base, 18, stride=per_group), :] = total[0:18, cols]
            links_ref.at[t][pl.ds(base + 18 * per_group, 18, stride=per_group), :] = total[24:42, cols]

    for s in range(scn):
        scene_step(s)

    lane = iota((32, LANES), 1)
    own = jnp.zeros((32, LANES), F32)
    for s in range(scn):
        column = jnp.sum(own_ref[pl.ds(s, 32, stride=pitch), :], axis=1, keepdims=True)
        own = own + jnp.where(lane == s, column, 0.0)
    start = device * scn
    own = pltpu.roll(own, lax.rem(start, LANES), 1)
    tile_at = lax.div(start, LANES)
    for t in range(scenes // LANES):
        cols = pl.ds(t * LANES, LANES)
        whole = jnp.concatenate([acc_ref[16:24, cols], acc_ref[40:64, cols]], axis=0)
        whole = whole + jnp.where(tile_at == t, own, 0.0)
        high, low = split_two(whole)
        flat_ref[0:32, cols] = high.astype(F32)
        flat_ref[32:64, cols] = low.astype(F32)
    per_col = -(-21 // col_count)
    for c in range(col_count):
        for i in range(per_col):
            q = c * per_col + i
            if q < 21:
                extra_ref[c * 8 + 2 * i : c * 8 + 2 * i + 1, :] = flat_ref[10 + q : 11 + q, :]
                extra_ref[c * 8 + 2 * i + 1 : c * 8 + 2 * i + 2, :] = flat_ref[42 + q : 43 + q, :]
    base = col_count * 8
    extra_ref[base : base + 8, :] = flat_ref[0:8, :]
    extra_ref[base + 8 : base + 16, :] = flat_ref[32:40, :]

    places = jnp.transpose(jnp.broadcast_to(map_ref[...], (8, scenes)))[:, :1]
    onto = jnp.where(iota((scenes, scenes), 1) == places, 1.0, 0.0).astype(BF16)
    links = jnp.concatenate([links_ref[t] for t in range(scenes // LANES)], axis=1)
    left = jnp.concatenate([links.astype(BF16), extra_ref[...].astype(BF16)], axis=0)
    perm_ref[...] = jnp.dot(left, onto, preferred_element_type=F32)

    top = scn * 36
    side = 18 * per_group
    first = iota((8, LANES), 1) < HALF
    head_rows = iota((8, LANES), 0) < 2
    first_side = iota((side, LANES), 1) < HALF

    def merge(low_part, high_part, mask):
        even = jnp.where(mask, low_part, pltpu.roll(high_part, HALF, 1))
        odd = jnp.where(mask, pltpu.roll(low_part, HALF, 1), high_part)
        return even, odd

    grads = [pl.ds(top + base + 8 * k, 8) for k in range(2)]
    for j in range(col_count // 2):
        cols = pl.ds(j * LANES, LANES)
        grad_cols = merge(perm_ref[grads[0], cols], perm_ref[grads[1], cols], first)
        for r in range(row_count):
            rows = pl.ds(r * LANES, LANES)
            at = r * 2 * side
            pieces = merge(perm_ref[at : at + side, cols], perm_ref[at + side : at + 2 * side, cols], first_side)
            for k in range(2):
                c = 2 * j + k
                spot = r * col_count + c
                send_ref[spot, 0:side, :] = pieces[k].astype(BF16)
                own = perm_ref[top + c * 8 : top + c * 8 + 8, rows]
                tails = [perm_ref[grads[0], rows], perm_ref[grads[1], rows], grad_cols[k]]
                for i, tail in enumerate(tails):
                    turned = own if i == 0 else pltpu.roll(own, 8 - 2 * i, 0)
                    block = jnp.where(head_rows, turned, tail)
                    send_ref[spot, side + 8 * i : side + 8 * i + 8, :] = block.astype(BF16)


def tile_matvec(tile_ref, own_ref, rows_part, cols_part, rows_ref):
    which = iota((8, LANES), 0)
    turned = jnp.transpose(cols_part)[:HALF]
    forward = [jnp.zeros((8, LANES), F32) for _ in range(6)]
    backward = []
    for y in range(6):
        column = jnp.broadcast_to(turned[:, y : y + 1], (HALF, LANES))
        total = jnp.zeros((HALF, LANES), F32)
        for x in range(6):
            block = tile_ref[x * 6 + y].astype(F32)
            forward[x] = forward[x] + jnp.sum((block * column).reshape(HALF // 8, 8, LANES), axis=0)
            total = total + block * rows_part[x : x + 1, :]
        backward.append(total)
    sides = []
    for y in range(3):
        pair = jnp.concatenate([backward[y], backward[y + 3]], axis=0)
        sides.append(jnp.sum(jnp.transpose(pair), axis=0, keepdims=True))
    out = jnp.zeros((8, LANES), F32)
    for x in range(6):
        out = jnp.where(which == x, jnp.sum(forward[x], axis=0, keepdims=True), out)
    rows_ref[...] = rows_part
    col = lax.axis_index("col")
    per_col = -(-21 // lax.axis_size("col"))
    for i in range(per_col):
        q = jnp.minimum(col * per_col + i, 20)
        x = jnp.int32(0)
        start = jnp.int32(0)
        for line in range(1, 6):
            past = (q >= PAIRS.index((line, line))).astype(jnp.int32)
            x = x + past
            start = start + past * (7 - line)
        y = q - start + x
        weight = own_ref[i : i + 1, :]
        at_x = rows_ref[pl.ds(x, 1), :] * weight
        at_y = rows_ref[pl.ds(y, 1), :] * weight
        out = out + jnp.where(which == x, at_y, 0.0)
        out = out + jnp.where((which == y) & (x != y), at_x, 0.0)
    return out, sides


def write_partials(out, sides, line, part_ref):
    rows = [out[x : x + 1, :] for x in range(6)] + sides
    if line is not None:
        rows.append(line)
    for n in range(part_ref.shape[0]):
        for k, row in enumerate(rows):
            part_ref[n, :, k * LANES : (k + 1) * LANES] = row


def first_kernel(
    row_count, col_count, got_ref, select_ref, tile_ref, own_ref, part_ref, rows_ref,
):
    devices = got_ref.shape[0]
    deep, tile_rows = select_ref.shape[0], select_ref.shape[1] // 2
    per_group = tile_rows // devices
    select = select_ref[...]
    for k in range(9):
        picked = got_ref[:, k * 8 : k * 8 + 8, :].reshape(deep, LANES)
        block = lax.dot_general(picked, select, (((0,), (0,)), ((), ())), preferred_element_type=F32)
        block = block.astype(BF16)
        for e in range(2):
            cols = slice(e * tile_rows, (e + 1) * tile_rows)
            tile_ref[2 * k + e] = block[:HALF, cols]
            tile_ref[2 * k + e + 18] = block[HALF:, cols]
    extras = []
    for i in range(3):
        rows = pl.ds(18 * per_group + 8 * i, 8)
        total = got_ref[0, rows, :].astype(F32)
        for n in range(1, devices):
            total = total + got_ref[n, rows, :].astype(F32)
        own_ref[i : i + 1, :] = total[0:1] + total[1:2]
        extras.append(pltpu.roll(total, 6, 0))
    used = iota((8, LANES), 0) < 6
    rows_part = jnp.where(used, extras[0] + extras[1], 0.0)
    cols_part = jnp.where(used, extras[2] + pltpu.roll(extras[2], HALF, 1), 0.0)
    out, sides = tile_matvec(tile_ref, own_ref, rows_part, cols_part, rows_ref)
    rows_ref[...] = rows_part
    line = rows_ref[pl.ds(jnp.minimum(lax.axis_index("col"), 5), 1), :]
    write_partials(out, sides, line, part_ref)


def gather_image(row_count, col_count, got_ref, image_ref):
    first = iota((1, LANES), 1) < HALF
    side = 6 * LANES
    cols = []
    for c in range(col_count):
        total = got_ref[c, :, side : side + 3 * LANES]
        for r in range(1, row_count):
            total = total + got_ref[r * col_count + c, :, side : side + 3 * LANES]
        cols.append(total)
    for r in range(row_count):
        total = got_ref[r * col_count, :, 0:side]
        for c in range(1, col_count):
            total = total + got_ref[r * col_count + c, :, 0:side]
        image_ref[r] = jnp.zeros((8, LANES), F32)
        for t in range(3):
            left = cols[2 * r][:, t * LANES : (t + 1) * LANES]
            right = cols[2 * r + 1][:, t * LANES : (t + 1) * LANES]
            low = jnp.where(first, left, pltpu.roll(right, HALF, 1))
            high = jnp.where(first, pltpu.roll(left, HALF, 1), right)
            image_ref[r, t : t + 1, :] = total[:, t * LANES : (t + 1) * LANES] + low
            image_ref[r, t + 3 : t + 4, :] = total[:, (t + 3) * LANES : (t + 4) * LANES] + high


def inner_all(left, right):
    return jnp.sum(jnp.sum(left * right, axis=0), keepdims=True)


def step_kernel(
    row_count, col_count, begin, got_ref, tile_ref, own_ref, state_ref, next_ref, part_ref,
    *rest,
):
    if begin:
        coupling_ref, image_ref, rows_ref, copy_sem = rest
        copy = pltpu.make_async_copy(tile_ref, coupling_ref, copy_sem)
        copy.start()
    else:
        image_ref, rows_ref = rest
    gather_image(row_count, col_count, got_ref, image_ref)
    if begin:
        for r in range(row_count):
            next_ref[1, r] = jnp.zeros((8, LANES), F32)
            for x in range(6):
                next_ref[1, r, x : x + 1, :] = got_ref[r * col_count + x, :, 9 * LANES : 10 * LANES]
        remainder = next_ref[1]
        direction = remainder
        answer = jnp.zeros_like(remainder)
    else:
        answer, remainder, direction = state_ref[0], state_ref[1], state_ref[2]
    norm_now = inner_all(remainder, remainder)
    image = CAMERA_DAMPING * direction + image_ref[...]
    alpha = norm_now / inner_all(direction, image)
    answer = answer + alpha * direction
    remainder = remainder - alpha * image
    norm_next = inner_all(remainder, remainder)
    direction = remainder + norm_next / norm_now * direction
    next_ref[0] = answer
    next_ref[1] = remainder
    next_ref[2] = direction
    col = lax.axis_index("col")
    rows_part = next_ref[2, lax.axis_index("row")]
    wide = next_ref[2, lax.div(col, 2)]
    turned = pltpu.roll(wide, HALF, 1)
    cols_part = jnp.where(iota((8, LANES), 0) * 0 == lax.rem(col, 2), wide, turned)
    out, sides = tile_matvec(tile_ref, own_ref, rows_part, cols_part, rows_ref)
    write_partials(out, sides, None, part_ref)
    if begin:
        copy.wait()


def last_kernel(row_count, col_count, got_ref, state_ref, answer_ref, remainder_ref, image_ref):
    gather_image(row_count, col_count, got_ref, image_ref)
    remainder, direction = state_ref[1], state_ref[2]
    norm_now = inner_all(remainder, remainder)
    image_ref[...] = CAMERA_DAMPING * direction + image_ref[...]
    alpha = norm_now / inner_all(direction, image_ref[...])
    row = lax.axis_index("row")
    answer_ref[...] = (state_ref[0, row] + alpha * state_ref[2, row])[:6]
    remainder_ref[...] = (state_ref[1, row] - alpha * image_ref[row])[:6]


def vmem():
    return pl.BlockSpec(memory_space=pltpu.VMEM)


def hbm():
    return pl.BlockSpec(memory_space=pltpu.HBM)


def small_limit(mib):
    return pltpu.CompilerParams(vmem_limit_bytes=mib << 20)


def packed_shards(cam_jac, pt_jac, resid, partner, count, tile_map):
    row_count = lax.axis_size("row")
    col_count = lax.axis_size("col")
    devices = row_count * col_count
    scenes = tile_map.shape[0]
    scn, points = partner.shape
    map_row = tile_map.reshape(1, scenes)

    def bind(kernel, *fixed):
        def run(*refs):
            return kernel(row_count, col_count, *fixed, *refs)

        return run

    extra_rows = col_count * 8 + 16
    tile_rows = scenes // row_count
    send, select = pl.pallas_call(
        bind(assemble_kernel),
        out_shape=(
            jax.ShapeDtypeStruct((devices, 96, LANES), BF16),
            jax.ShapeDtypeStruct((devices * 8, 2 * tile_rows), BF16),
        ),
        in_specs=[hbm()] * 7,
        out_specs=(vmem(),) * 2,
        scratch_shapes=[
            pltpu.VMEM((points // LANES, 64 * (scn + 1), LANES), F32),
            pltpu.VMEM((32 * (scn + 1), LANES), F32),
            pltpu.VMEM((64, scenes), F32),
            pltpu.VMEM((scenes // LANES, 36 * scn, LANES), F32),
            pltpu.VMEM((64, scenes), F32),
            pltpu.VMEM((extra_rows, scenes), F32),
            pltpu.VMEM((36 * scn + extra_rows, scenes), F32),
            pltpu.VMEM(cam_jac.shape, BF16),
            pltpu.VMEM(pt_jac.shape, BF16),
            pltpu.VMEM(resid.shape, BF16),
            pltpu.VMEM(partner.shape, jnp.int32),
            pltpu.VMEM(map_row.shape, jnp.int32),
            pltpu.SMEM(count.shape, jnp.int32),
            pltpu.SMEM(tile_map.shape, jnp.int32),
            pltpu.SemaphoreType.DMA((3, points // LANES)),
            pltpu.SemaphoreType.DMA((4,)),
        ],
        compiler_params=small_limit(36),
        name="assemble",
    )(
        *[
            pltpu.with_memory_space_constraint(value, pltpu.HBM)
            for value in (cam_jac, pt_jac, resid, partner, map_row, count, tile_map)
        ]
    )
    got = lax.all_to_all(send, AXES, 0, 0, tiled=True)
    tile, own, part = pl.pallas_call(
        bind(first_kernel),
        out_shape=(
            jax.ShapeDtypeStruct((36, HALF, tile_rows), BF16),
            jax.ShapeDtypeStruct((8, LANES), F32),
            jax.ShapeDtypeStruct((devices, 1, 10 * LANES), F32),
        ),
        in_specs=[vmem()] * 2,
        out_specs=(vmem(),) * 3,
        scratch_shapes=[pltpu.VMEM((8, LANES), F32)],
        compiler_params=small_limit(16),
        name="first",
    )(got, select)
    state = jnp.zeros((3, row_count, 8, LANES), F32)
    for turn in range(ITERS - 1):
        got = lax.all_to_all(part, AXES, 0, 0, tiled=True)
        begin = turn == 0
        outs = [
            jax.ShapeDtypeStruct((3, row_count, 8, LANES), F32),
            jax.ShapeDtypeStruct((devices, 1, 9 * LANES), F32),
        ]
        places = [vmem()] * 2
        scratch = [pltpu.VMEM((row_count, 8, LANES), F32), pltpu.VMEM((8, LANES), F32)]
        if begin:
            outs.append(jax.ShapeDtypeStruct(tile.shape, BF16))
            places.append(hbm())
            scratch.append(pltpu.SemaphoreType.DMA(()))
        state, part, *rest = pl.pallas_call(
            bind(step_kernel, begin),
            out_shape=outs,
            in_specs=[vmem()] * 4,
            out_specs=places,
            scratch_shapes=scratch,
            compiler_params=small_limit(8),
            name="step",
        )(got, tile, own, state)
        if begin:
            coupling = rest[0]
    got = lax.all_to_all(part, AXES, 0, 0, tiled=True)
    answer, remainder = pl.pallas_call(
        bind(last_kernel),
        out_shape=(jax.ShapeDtypeStruct((6, tile_rows), F32),) * 2,
        in_specs=[vmem()] * 2,
        out_specs=(vmem(),) * 2,
        scratch_shapes=[pltpu.VMEM((row_count, 8, LANES), F32)],
        compiler_params=small_limit(4),
        name="last",
    )(got, state)
    return jnp.swapaxes(coupling.reshape(6, 6, HALF, tile_rows), 2, 3), answer, remainder


def cross_product(first_vec, second_vec):
    return jnp.stack(
        [
            first_vec[1] * second_vec[2] - first_vec[2] * second_vec[1],
            first_vec[2] * second_vec[0] - first_vec[0] * second_vec[2],
            first_vec[0] * second_vec[1] - first_vec[1] * second_vec[0],
        ],
        axis=0,
    )


def point_terms(camera, points_jac, errors):
    camera = camera.astype(jnp.float32)
    points_jac = points_jac.astype(jnp.float32)
    errors = errors.astype(jnp.float32)
    own_jac, other_jac = (camera[0], camera[1])
    own_point, other_point = (points_jac[0], points_jac[1])
    own_error, other_error = (errors[0], errors[1])
    point_hessian = jnp.sum(own_point[:, :, None] * own_point[:, None, :], axis=0)
    point_hessian = point_hessian + jnp.sum(
        other_point[:, :, None] * other_point[:, None, :], axis=0
    )
    point_hessian = point_hessian + POINT_DAMPING * jnp.eye(3, dtype=jnp.float32)[:, :, None, None]
    first_row, second_row, third_row = (point_hessian[0], point_hessian[1], point_hessian[2])
    cofactor_first = cross_product(second_row, third_row)
    cofactor_second = cross_product(third_row, first_row)
    cofactor_third = cross_product(first_row, second_row)
    determinant = jnp.sum(first_row * cofactor_first, axis=0)
    inverse = jnp.stack([cofactor_first, cofactor_second, cofactor_third], axis=1) / determinant
    w_own = jnp.sum(own_jac[:, :, None] * own_point[:, None, :], axis=0)
    w_other = jnp.sum(other_jac[:, :, None] * other_point[:, None, :], axis=0)
    point_rhs = -(
        jnp.sum(own_point * own_error[:, None], axis=0)
        + jnp.sum(other_point * other_error[:, None], axis=0)
    )
    own_vi = jnp.sum(w_own[:, :, None] * inverse[None, :, :], axis=1)
    other_vi = jnp.sum(w_other[:, :, None] * inverse[None, :, :], axis=1)
    diag_own = jnp.sum(own_jac[:, :, None] * own_jac[:, None, :], axis=0) - jnp.sum(
        own_vi[:, None, :] * w_own[None, :, :], axis=2
    )
    diag_other = jnp.sum(other_jac[:, :, None] * other_jac[:, None, :], axis=0) - jnp.sum(
        other_vi[:, None, :] * w_other[None, :, :], axis=2
    )
    link = -jnp.sum(own_vi[:, None, :] * w_other[None, :, :], axis=2)
    grad_own = -jnp.sum(own_jac * own_error[:, None], axis=0) - jnp.sum(
        own_vi * point_rhs[None], axis=1
    )
    grad_other = -jnp.sum(other_jac * other_error[:, None], axis=0) - jnp.sum(
        other_vi * point_rhs[None], axis=1
    )
    return (diag_own, diag_other, link, grad_own, grad_other)


def conjugate_steps(right_side, apply_operator, inner_product):
    solution = jnp.zeros_like(right_side)
    remainder = right_side
    direction = right_side
    norm_now = inner_product(remainder, remainder)
    for iteration in range(ITERS):
        product_vec = apply_operator(direction)
        step_size = norm_now / inner_product(direction, product_vec)
        solution = solution + step_size * direction
        remainder = remainder - step_size * product_vec
        norm_next = inner_product(remainder, remainder)
        direction = remainder + norm_next / norm_now * direction
        norm_now = norm_next
    return (solution, remainder)


def plain_shards(cam_jac, pt_jac, resid, partner, count, tile_map):
    row_count = lax.axis_size("row")
    col_count = lax.axis_size("col")
    scenes = tile_map.shape[0]
    scn_local = partner.shape[0]
    points = partner.shape[1]
    tile_rows = scenes // row_count
    tile_cols = scenes // col_count
    per_group = scn_local // row_count
    row_index = lax.axis_index("row")
    col_index = lax.axis_index("col")
    device = row_index * col_count + col_index
    positions = jnp.arange(scenes, dtype=jnp.int32)
    tile_own = lax.dynamic_slice_in_dim(tile_map, device * scn_local, scn_local)
    local_rank = jnp.sum((tile_own[None, :] < tile_own[:, None]).astype(jnp.int32), axis=1)
    active = (jnp.arange(points, dtype=jnp.int32)[None, :] < count[:, None]).astype(jnp.float32)
    diag_own, diag_other, link, grad_own, grad_other = point_terms(cam_jac, pt_jac, resid)
    values = (
        jnp.concatenate(
            [
                link.reshape(36, scn_local, points),
                diag_other.reshape(36, scn_local, points),
                grad_other,
            ],
            axis=0,
        )
        * active[None]
    )
    values = jnp.moveaxis(values, 1, 0)

    def scene_sums(item):
        scene_values, scene_partner = item
        hits = scene_partner[:, None] == positions[None, :]
        tile_other = jnp.sum(jnp.where(hits, tile_map[None, :], 0), axis=1)
        onehot = (tile_other[:, None] == positions[None, :]).astype(jnp.float32)
        return jnp.dot(
            scene_values,
            onehot,
            precision=lax.Precision.HIGHEST,
            preferred_element_type=jnp.float32,
        )

    per_scene = lax.map(scene_sums, (values, partner))
    link_rows = per_scene[:, :36, :]
    other_sum = jnp.sum(per_scene[:, 36:, :], axis=0)
    ordering = (local_rank[None, :] == jnp.arange(scn_local, dtype=jnp.int32)[:, None]).astype(
        jnp.float32
    )
    panel = jnp.einsum("rs,sxc->xrc", ordering, link_rows, precision=lax.Precision.HIGHEST)
    panel = panel.reshape(36, row_count, per_group, col_count, tile_cols).transpose(0, 1, 3, 2, 4)
    panel_short = panel.astype(jnp.bfloat16)
    own_onehot = (tile_own[:, None] == positions[None, :]).astype(jnp.float32)
    own_diag = jnp.sum(diag_own * active, axis=-1).reshape(36, scn_local)
    own_grad = jnp.sum(grad_own * active, axis=-1)
    own_both = jnp.concatenate([own_diag, own_grad], axis=0)
    own_spread = jnp.dot(
        own_both, own_onehot, precision=lax.Precision.HIGHEST, preferred_element_type=jnp.float32
    )
    both_part = own_spread + other_sum
    diag_part = both_part[:36]
    grad_part = both_part[36:]
    shaped = panel_short.reshape(36, row_count * col_count, per_group, tile_cols)
    received = lax.all_to_all(shaped, ("row", "col"), split_axis=1, concat_axis=1, tiled=True)
    received = received.reshape(36, tile_rows, tile_cols)
    diag_all, grad_all = lax.psum((diag_part, grad_part), ("row", "col"))
    row_start = row_index * tile_rows
    col_start = col_index * tile_cols
    devices = scenes // scn_local
    tiles_grid = tile_map.reshape(devices, scn_local)
    inblock = (tiles_grid >= row_start) & (tiles_grid < row_start + tile_rows)
    lower = (tiles_grid[:, None, :] < tiles_grid[:, :, None]) & inblock[:, None, :]
    within_all = jnp.sum(lower.astype(jnp.int32), axis=2)
    slot_from = (jnp.arange(devices, dtype=jnp.int32)[:, None] * per_group + within_all).reshape(-1)
    slot_to = (tiles_grid - row_start).reshape(-1)
    slots = jnp.arange(tile_rows, dtype=jnp.int32)
    to_table = ((slot_to[:, None] == slots[None, :]) & inblock.reshape(-1)[:, None]).astype(
        jnp.bfloat16
    )
    from_table = (slot_from[:, None] == slots[None, :]).astype(jnp.bfloat16)
    selection = jnp.dot(to_table.T, from_table, preferred_element_type=jnp.float32).astype(
        jnp.bfloat16
    )
    coupling_tile = jnp.einsum(
        "pk,xkc->xpc", selection, received, preferred_element_type=jnp.float32
    )
    coupling_tile = coupling_tile.astype(jnp.bfloat16).reshape(6, 6, tile_rows, tile_cols)
    coupling_wide = coupling_tile.astype(jnp.float32)
    zero_at = row_index * 0

    def tile_products(rows_part, cols_part):
        forward = jnp.einsum(
            "xyij,yj->xi", coupling_wide, cols_part, precision=lax.Precision.HIGHEST
        )
        backward = jnp.einsum(
            "xyij,xi->yj", coupling_wide, rows_part, precision=lax.Precision.HIGHEST
        )
        empty = jnp.zeros((6, scenes), jnp.float32)
        spread = lax.dynamic_update_slice(empty, forward, (zero_at, row_start))
        spread = spread + lax.dynamic_update_slice(empty, backward, (zero_at, col_start))
        return lax.psum(spread, ("row", "col"))

    diag_blocks = diag_all.reshape(6, 6, scenes)

    def apply_full(direction):
        rows_part = lax.dynamic_slice_in_dim(direction, row_start, tile_rows, 1)
        cols_part = lax.dynamic_slice_in_dim(direction, col_start, tile_cols, 1)
        summed = tile_products(rows_part, cols_part)
        result = CAMERA_DAMPING * direction
        result = result + jnp.einsum(
            "xyi,yi->xi", diag_blocks, direction, precision=lax.Precision.HIGHEST
        )
        return result + summed

    def inner_full(first_vec, second_vec):
        return jnp.sum(first_vec * second_vec)

    whole_solution, whole_remainder = conjugate_steps(grad_all, apply_full, inner_full)
    solution = lax.dynamic_slice_in_dim(whole_solution, row_start, tile_rows, 1)
    remainder = lax.dynamic_slice_in_dim(whole_remainder, row_start, tile_rows, 1)
    return (coupling_tile, solution, remainder)


def shards(cam_jac, pt_jac, resid, partner, count, tile_map):
    row_count = lax.axis_size("row")
    col_count = lax.axis_size("col")
    scenes = tile_map.shape[0]
    scn, points = partner.shape
    packs = (
        scenes == col_count * HALF
        and scenes == row_count * LANES
        and scn == row_count * 4
        and LANES % scn == 0
        and points % LANES == 0
        and col_count >= 7
    )
    run = packed_shards if packs else plain_shards
    return run(cam_jac, pt_jac, resid, partner, count, tile_map)


def solution(mesh):
    return jax.shard_map(
        shards,
        mesh=mesh,
        in_specs=(
            P(None, None, None, AXES, None),
            P(None, None, None, AXES, None),
            P(None, None, AXES, None),
            P(AXES, None),
            P(AXES),
            P(),
        ),
        out_specs=(P(None, None, "row", "col"), P(None, "row"), P(None, "row")),
        check_vma=False,
    )
```

```python
import jax
import jax.numpy as jnp
from jax import lax
from jax.experimental import pallas as pl
from jax.experimental.pallas import tpu as pltpu
from jax.sharding import PartitionSpec as P

ITERS = 3
CAMERA_DAMPING = 1.0
POINT_DAMPING = 1.0
AXES = ("row", "col")
LANES = 128
HALF = 64
F32 = jnp.float32
BF16 = jnp.bfloat16
PAIRS = [(x, y) for x in range(6) for y in range(x, 6)]
CONTRACT_LAST = (((1,), (1,)), ((), ()))


def iota(shape, dim):
    return lax.broadcasted_iota(jnp.int32, shape, dim)


def split_two(value):
    high = value.astype(BF16)
    low = (value - high.astype(F32)).astype(BF16)
    return high, low


def point_values(ja, jb, pa, pb, ea, eb, live):
    one = POINT_DAMPING
    hess = {}
    for x in range(3):
        for y in range(x, 3):
            h = pa[0][x] * pa[0][y] + pa[1][x] * pa[1][y]
            h = h + (pb[0][x] * pb[0][y] + pb[1][x] * pb[1][y])
            hess[x, y] = h + one if x == y else h
    a, b, c = hess[0, 0], hess[0, 1], hess[0, 2]
    d, e, f = hess[1, 1], hess[1, 2], hess[2, 2]
    c00 = d * f - e * e
    c01 = c * e - b * f
    c02 = b * e - c * d
    c11 = a * f - c * c
    c12 = b * c - a * e
    c22 = a * d - b * b
    det = a * c00 + b * c01 + c * c02
    inv = 1.0 / det
    vi = [[c00 * inv, c01 * inv, c02 * inv], [None, c11 * inv, c12 * inv], [None, None, c22 * inv]]
    vi[1][0], vi[2][0], vi[2][1] = vi[0][1], vi[0][2], vi[1][2]
    q = [
        -((pa[0][k] * ea[0] + pa[1][k] * ea[1]) + (pb[0][k] * eb[0] + pb[1][k] * eb[1]))
        for k in range(3)
    ]
    viq = [vi[k][0] * q[0] + vi[k][1] * q[1] + vi[k][2] * q[2] for k in range(3)]

    def times_vi(p):
        return [
            [p[m][0] * vi[0][k] + p[m][1] * vi[1][k] + p[m][2] * vi[2][k] for k in range(3)]
            for m in range(2)
        ]

    def inner(left, right):
        return left[0] * right[0] + left[1] * right[1] + left[2] * right[2]

    def keep(value):
        return jnp.where(live, value, 0.0)

    av = times_vi(pa)
    bv = times_vi(pb)
    m_ab = [[keep(-inner(av[m], pb[k])) for k in range(2)] for m in range(2)]
    g_aa = [keep(1.0 - inner(av[0], pa[0])), keep(-inner(av[0], pa[1])), keep(1.0 - inner(av[1], pa[1]))]
    g_bb = [keep(1.0 - inner(bv[0], pb[0])), keep(-inner(bv[0], pb[1])), keep(1.0 - inner(bv[1], pb[1]))]
    h_a = [keep(-(ea[m] + inner(pa[m], viq))) for m in range(2)]
    h_b = [keep(-(eb[m] + inner(pb[m], viq))) for m in range(2)]

    mj = [[m_ab[m][0] * jb[0][y] + m_ab[m][1] * jb[1][y] for y in range(6)] for m in range(2)]
    link = {}
    for x in range(6):
        for y in range(6):
            link[x, y] = ja[0][x] * mj[0][y] + ja[1][x] * mj[1][y]

    def diagonal(j, g):
        gj = [
            [g[0] * j[0][y] + g[1] * j[1][y] for y in range(6)],
            [g[1] * j[0][y] + g[2] * j[1][y] for y in range(6)],
        ]
        return [j[0][x] * gj[0][y] + j[1][x] * gj[1][y] for x, y in PAIRS]

    diag_own = diagonal(ja, g_aa)
    diag_other = diagonal(jb, g_bb)
    grad_own = [ja[0][x] * h_a[0] + ja[1][x] * h_a[1] for x in range(6)]
    grad_other = [jb[0][x] * h_b[0] + jb[1][x] * h_b[1] for x in range(6)]
    return diag_own, diag_other, link, grad_own, grad_other


def selection(row_count, map_ref, scn, tile_rows, per_group):
    scenes = map_ref.shape[1]
    row = lax.axis_index("row")
    tiles = jnp.concatenate(
        [map_ref[:, t * LANES : (t + 1) * LANES] for t in range(scenes // LANES)], axis=0
    )
    groups = scenes // LANES
    place = iota((groups, LANES), 1) % scn
    rank = jnp.zeros((groups, LANES), jnp.int32)
    for shift in range(1, scn):
        before = pltpu.roll(tiles, shift, 1)
        after = pltpu.roll(tiles, LANES - shift, 1)
        rank = rank + ((before < tiles) & (place >= shift)).astype(jnp.int32)
        rank = rank + ((after < tiles) & (place + shift < scn)).astype(jnp.int32)
    scene_id = iota((groups, LANES), 0) * LANES + iota((groups, LANES), 1)
    slot_at = (scene_id // scn) * 8 + rank % per_group
    local = tiles - row * tile_rows
    slot_at = jnp.where((local >= 0) & (local < tile_rows), slot_at, -1)
    deep = scenes // scn * 8
    select = jnp.zeros((deep, tile_rows), F32)
    for t in range(groups):
        to_row = jnp.where(iota((tile_rows, LANES), 0) == local[t : t + 1, :], 1.0, 0.0).astype(BF16)
        from_slot = jnp.where(iota((deep, LANES), 0) == slot_at[t : t + 1, :], 1.0, 0.0).astype(BF16)
        select = select + lax.dot_general(from_slot, to_row, CONTRACT_LAST, preferred_element_type=F32)
    return jnp.concatenate([select, pltpu.roll(select, 4, 0)], axis=1).astype(BF16)


def assemble_kernel(
    row_count, col_count, cam_in, pt_in, res_in, partner_in, row_in, count_in, map_in, send_ref,
    select_ref,
    vals_ref, own_ref, acc_ref, links_ref, flat_ref, extra_ref, perm_ref,
    cam_ref, pt_ref, res_ref, partner_ref, map_ref, count_sm, map_sm, slab_sem, whole_sem,
):
    scn = partner_ref.shape[0]
    points = partner_ref.shape[1]
    scenes = map_ref.shape[1]
    wholes = [
        pltpu.make_async_copy(source, target, whole_sem.at[k])
        for k, (source, target) in enumerate(
            [(count_in, count_sm), (map_in, map_sm), (row_in, map_ref), (partner_in, partner_ref)]
        )
    ]

    def slab_copies(step):
        lanes = pl.ds(step * LANES, LANES)
        return [
            pltpu.make_async_copy(
                source.at[..., lanes], target.at[..., lanes], slab_sem.at[k, step]
            )
            for k, (source, target) in enumerate([(cam_in, cam_ref), (pt_in, pt_ref), (res_in, res_ref)])
        ]

    wholes[0].start()
    for step in range(points // LANES):
        for copy in slab_copies(step):
            copy.start()
    for copy in wholes[1:]:
        copy.start()
    per_group = scn // row_count
    device = lax.axis_index("row") * col_count + lax.axis_index("col")
    slab = (scn, LANES)
    pitch = scn + 1

    own_ref[...] = jnp.zeros_like(own_ref)
    acc_ref[...] = jnp.zeros_like(acc_ref)
    extra_ref[...] = jnp.zeros_like(extra_ref)
    vals_ref[:, pl.ds(63 * pitch, scn), :] = jnp.zeros((points // LANES, scn, LANES), F32)

    wholes[0].wait()
    sub = iota(slab, 0)
    counts = jnp.zeros(slab, jnp.int32)
    for s in range(scn):
        counts = jnp.where(sub == s, count_sm[s], counts)

    def slab_step(step):
        for copy in slab_copies(step):
            copy.wait()
        lanes = pl.ds(step * LANES, LANES)

        def get(ref, *where):
            return ref[where + (slice(None), lanes)].astype(F32)

        ja = [[get(cam_ref, 0, m, x) for x in range(6)] for m in range(2)]
        jb = [[get(cam_ref, 1, m, x) for x in range(6)] for m in range(2)]
        pa = [[get(pt_ref, 0, m, x) for x in range(3)] for m in range(2)]
        pb = [[get(pt_ref, 1, m, x) for x in range(3)] for m in range(2)]
        ea = [get(res_ref, 0, m) for m in range(2)]
        eb = [get(res_ref, 1, m) for m in range(2)]
        live = (iota(slab, 1) + step * LANES) < counts
        diag_own, diag_other, link, grad_own, grad_other = point_values(ja, jb, pa, pb, ea, eb, live)

        def put(q, value):
            vals_ref[step, pl.ds(q * pitch, scn), :] = value

        def put_own(q, value):
            own_ref[pl.ds(q * pitch, scn), :] += value

        for x in range(3):
            for y in range(6):
                put(x * 6 + y, link[x, y])
                put(24 + x * 6 + y, link[x + 3, y])
        for x in range(6):
            put(18 + x, grad_other[x])
            put_own(2 + x, grad_own[x])
        for q in range(21):
            put(42 + q, diag_other[q])
            put_own(10 + q, diag_own[q])

    for step in range(points // LANES):
        slab_step(step)

    for copy in wholes[1:]:
        copy.wait()
    select_ref[...] = selection(row_count, map_ref, scn, scenes // row_count, per_group)
    spots = iota((points, scenes), 1).astype(jnp.int16)
    mates = jnp.transpose(partner_ref[...]).astype(jnp.int16)

    def scene_step(s):
        values = jnp.concatenate(
            [vals_ref.at[t][pl.ds(s, 64, stride=pitch), :] for t in range(points // LANES)], axis=1
        )
        high, low = split_two(values)
        left = jnp.concatenate([high, low], axis=0)
        onehot = jnp.where(spots == mates[:, s : s + 1], jnp.asarray(1, BF16), jnp.asarray(0, BF16))
        both = jnp.dot(left, onehot, preferred_element_type=F32)
        total = both[:64] + both[64:]
        acc_ref[...] += total
        mine = map_sm[device * scn + s]
        rank = jnp.int32(0)
        for other in range(scn):
            rank = rank + (map_sm[device * scn + other] < mine).astype(jnp.int32)
        base = lax.div(rank, per_group) * (36 * per_group) + lax.rem(rank, per_group)
        for t in range(scenes // LANES):
            cols = slice(t * LANES, (t + 1) * LANES)
            links_ref.at[t][pl.ds(base, 18, stride=per_group), :] = total[0:18, cols]
            links_ref.at[t][pl.ds(base + 18 * per_group, 18, stride=per_group), :] = total[24:42, cols]

    for s in range(scn):
        scene_step(s)

    lane = iota((32, LANES), 1)
    own = jnp.zeros((32, LANES), F32)
    for s in range(scn):
        column = jnp.sum(own_ref[pl.ds(s, 32, stride=pitch), :], axis=1, keepdims=True)
        own = own + jnp.where(lane == s, column, 0.0)
    start = device * scn
    own = pltpu.roll(own, lax.rem(start, LANES), 1)
    tile_at = lax.div(start, LANES)
    for t in range(scenes // LANES):
        cols = pl.ds(t * LANES, LANES)
        whole = jnp.concatenate([acc_ref[16:24, cols], acc_ref[40:64, cols]], axis=0)
        whole = whole + jnp.where(tile_at == t, own, 0.0)
        high, low = split_two(whole)
        flat_ref[0:32, cols] = high.astype(F32)
        flat_ref[32:64, cols] = low.astype(F32)
    per_col = -(-21 // col_count)
    for c in range(col_count):
        for i in range(per_col):
            q = c * per_col + i
            if q < 21:
                extra_ref[c * 8 + 2 * i : c * 8 + 2 * i + 1, :] = flat_ref[10 + q : 11 + q, :]
                extra_ref[c * 8 + 2 * i + 1 : c * 8 + 2 * i + 2, :] = flat_ref[42 + q : 43 + q, :]
    base = col_count * 8
    extra_ref[base : base + 8, :] = flat_ref[0:8, :]
    extra_ref[base + 8 : base + 16, :] = flat_ref[32:40, :]

    places = jnp.transpose(jnp.broadcast_to(map_ref[...], (8, scenes)))[:, :1]
    onto = jnp.where(iota((scenes, scenes), 1) == places, 1.0, 0.0).astype(BF16)
    links = jnp.concatenate([links_ref[t] for t in range(scenes // LANES)], axis=1)
    left = jnp.concatenate([links.astype(BF16), extra_ref[...].astype(BF16)], axis=0)
    perm_ref[...] = jnp.dot(left, onto, preferred_element_type=F32)

    top = scn * 36
    side = 18 * per_group
    first = iota((8, LANES), 1) < HALF
    head_rows = iota((8, LANES), 0) < 2
    first_side = iota((side, LANES), 1) < HALF

    def merge(low_part, high_part, mask):
        even = jnp.where(mask, low_part, pltpu.roll(high_part, HALF, 1))
        odd = jnp.where(mask, pltpu.roll(low_part, HALF, 1), high_part)
        return even, odd

    grads = [pl.ds(top + base + 8 * k, 8) for k in range(2)]
    for j in range(col_count // 2):
        cols = pl.ds(j * LANES, LANES)
        grad_cols = merge(perm_ref[grads[0], cols], perm_ref[grads[1], cols], first)
        for r in range(row_count):
            rows = pl.ds(r * LANES, LANES)
            at = r * 2 * side
            pieces = merge(perm_ref[at : at + side, cols], perm_ref[at + side : at + 2 * side, cols], first_side)
            for k in range(2):
                c = 2 * j + k
                spot = r * col_count + c
                send_ref[spot, 0:side, :] = pieces[k].astype(BF16)
                own = perm_ref[top + c * 8 : top + c * 8 + 8, rows]
                tails = [perm_ref[grads[0], rows], perm_ref[grads[1], rows], grad_cols[k]]
                for i, tail in enumerate(tails):
                    turned = own if i == 0 else pltpu.roll(own, 8 - 2 * i, 0)
                    block = jnp.where(head_rows, turned, tail)
                    send_ref[spot, side + 8 * i : side + 8 * i + 8, :] = block.astype(BF16)


def tile_matvec(tile_ref, own_ref, rows_part, cols_part, rows_ref):
    which = iota((8, LANES), 0)
    turned = jnp.transpose(cols_part)[:HALF]
    forward = [jnp.zeros((8, LANES), F32) for _ in range(6)]
    backward = []
    for y in range(6):
        column = jnp.broadcast_to(turned[:, y : y + 1], (HALF, LANES))
        total = jnp.zeros((HALF, LANES), F32)
        for x in range(6):
            block = tile_ref[x * 6 + y].astype(F32)
            forward[x] = forward[x] + jnp.sum((block * column).reshape(HALF // 8, 8, LANES), axis=0)
            total = total + block * rows_part[x : x + 1, :]
        backward.append(total)
    sides = []
    for y in range(3):
        pair = jnp.concatenate([backward[y], backward[y + 3]], axis=0)
        sides.append(jnp.sum(jnp.transpose(pair), axis=0, keepdims=True))
    out = jnp.zeros((8, LANES), F32)
    for x in range(6):
        out = jnp.where(which == x, jnp.sum(forward[x], axis=0, keepdims=True), out)
    rows_ref[...] = rows_part
    col = lax.axis_index("col")
    per_col = -(-21 // lax.axis_size("col"))
    for i in range(per_col):
        q = jnp.minimum(col * per_col + i, 20)
        x = jnp.int32(0)
        start = jnp.int32(0)
        for line in range(1, 6):
            past = (q >= PAIRS.index((line, line))).astype(jnp.int32)
            x = x + past
            start = start + past * (7 - line)
        y = q - start + x
        weight = own_ref[i : i + 1, :]
        at_x = rows_ref[pl.ds(x, 1), :] * weight
        at_y = rows_ref[pl.ds(y, 1), :] * weight
        out = out + jnp.where(which == x, at_y, 0.0)
        out = out + jnp.where((which == y) & (x != y), at_x, 0.0)
    return out, sides


def write_partials(out, sides, line, part_ref):
    rows = [out[x : x + 1, :] for x in range(6)] + sides
    if line is not None:
        rows.append(line)
    for n in range(part_ref.shape[0]):
        for k, row in enumerate(rows):
            part_ref[n, :, k * LANES : (k + 1) * LANES] = row


def first_kernel(
    row_count, col_count, got_ref, select_ref, tile_ref, own_ref, part_ref, rows_ref,
):
    devices = got_ref.shape[0]
    deep, tile_rows = select_ref.shape[0], select_ref.shape[1] // 2
    per_group = tile_rows // devices
    select = select_ref[...]
    for k in range(9):
        picked = got_ref[:, k * 8 : k * 8 + 8, :].reshape(deep, LANES)
        block = lax.dot_general(picked, select, (((0,), (0,)), ((), ())), preferred_element_type=F32)
        block = block.astype(BF16)
        for e in range(2):
            cols = slice(e * tile_rows, (e + 1) * tile_rows)
            tile_ref[2 * k + e] = block[:HALF, cols]
            tile_ref[2 * k + e + 18] = block[HALF:, cols]
    extras = []
    for i in range(3):
        rows = pl.ds(18 * per_group + 8 * i, 8)
        total = got_ref[0, rows, :].astype(F32)
        for n in range(1, devices):
            total = total + got_ref[n, rows, :].astype(F32)
        own_ref[i : i + 1, :] = total[0:1] + total[1:2]
        extras.append(pltpu.roll(total, 6, 0))
    used = iota((8, LANES), 0) < 6
    rows_part = jnp.where(used, extras[0] + extras[1], 0.0)
    cols_part = jnp.where(used, extras[2] + pltpu.roll(extras[2], HALF, 1), 0.0)
    out, sides = tile_matvec(tile_ref, own_ref, rows_part, cols_part, rows_ref)
    rows_ref[...] = rows_part
    line = rows_ref[pl.ds(jnp.minimum(lax.axis_index("col"), 5), 1), :]
    write_partials(out, sides, line, part_ref)


def gather_image(row_count, col_count, got_ref, image_ref):
    first = iota((1, LANES), 1) < HALF
    side = 6 * LANES
    cols = []
    for c in range(col_count):
        total = got_ref[c, :, side : side + 3 * LANES]
        for r in range(1, row_count):
            total = total + got_ref[r * col_count + c, :, side : side + 3 * LANES]
        cols.append(total)
    for r in range(row_count):
        total = got_ref[r * col_count, :, 0:side]
        for c in range(1, col_count):
            total = total + got_ref[r * col_count + c, :, 0:side]
        image_ref[r] = jnp.zeros((8, LANES), F32)
        for t in range(3):
            left = cols[2 * r][:, t * LANES : (t + 1) * LANES]
            right = cols[2 * r + 1][:, t * LANES : (t + 1) * LANES]
            low = jnp.where(first, left, pltpu.roll(right, HALF, 1))
            high = jnp.where(first, pltpu.roll(left, HALF, 1), right)
            image_ref[r, t : t + 1, :] = total[:, t * LANES : (t + 1) * LANES] + low
            image_ref[r, t + 3 : t + 4, :] = total[:, (t + 3) * LANES : (t + 4) * LANES] + high


def inner_all(left, right):
    return jnp.sum(jnp.sum(left * right, axis=0), keepdims=True)


def step_kernel(
    row_count, col_count, begin, got_ref, tile_ref, own_ref, state_ref, next_ref, part_ref,
    *rest,
):
    if begin:
        coupling_ref, image_ref, rows_ref, copy_sem = rest
        copy = pltpu.make_async_copy(tile_ref, coupling_ref, copy_sem)
        copy.start()
    else:
        image_ref, rows_ref = rest
    gather_image(row_count, col_count, got_ref, image_ref)
    if begin:
        for r in range(row_count):
            next_ref[1, r] = jnp.zeros((8, LANES), F32)
            for x in range(6):
                next_ref[1, r, x : x + 1, :] = got_ref[r * col_count + x, :, 9 * LANES : 10 * LANES]
        remainder = next_ref[1]
        direction = remainder
        answer = jnp.zeros_like(remainder)
    else:
        answer, remainder, direction = state_ref[0], state_ref[1], state_ref[2]
    norm_now = inner_all(remainder, remainder)
    image = CAMERA_DAMPING * direction + image_ref[...]
    alpha = norm_now / inner_all(direction, image)
    answer = answer + alpha * direction
    remainder = remainder - alpha * image
    norm_next = inner_all(remainder, remainder)
    direction = remainder + norm_next / norm_now * direction
    next_ref[0] = answer
    next_ref[1] = remainder
    next_ref[2] = direction
    col = lax.axis_index("col")
    rows_part = next_ref[2, lax.axis_index("row")]
    wide = next_ref[2, lax.div(col, 2)]
    turned = pltpu.roll(wide, HALF, 1)
    cols_part = jnp.where(iota((8, LANES), 0) * 0 == lax.rem(col, 2), wide, turned)
    out, sides = tile_matvec(tile_ref, own_ref, rows_part, cols_part, rows_ref)
    write_partials(out, sides, None, part_ref)
    if begin:
        copy.wait()


def last_kernel(row_count, col_count, got_ref, state_ref, answer_ref, remainder_ref, image_ref):
    gather_image(row_count, col_count, got_ref, image_ref)
    remainder, direction = state_ref[1], state_ref[2]
    norm_now = inner_all(remainder, remainder)
    image_ref[...] = CAMERA_DAMPING * direction + image_ref[...]
    alpha = norm_now / inner_all(direction, image_ref[...])
    row = lax.axis_index("row")
    answer_ref[...] = (state_ref[0, row] + alpha * state_ref[2, row])[:6]
    remainder_ref[...] = (state_ref[1, row] - alpha * image_ref[row])[:6]


def vmem():
    return pl.BlockSpec(memory_space=pltpu.VMEM)


def hbm():
    return pl.BlockSpec(memory_space=pltpu.HBM)


def small_limit(mib):
    return pltpu.CompilerParams(vmem_limit_bytes=mib << 20)


def packed_shards(cam_jac, pt_jac, resid, partner, count, tile_map):
    row_count = lax.axis_size("row")
    col_count = lax.axis_size("col")
    devices = row_count * col_count
    scenes = tile_map.shape[0]
    scn, points = partner.shape
    map_row = tile_map.reshape(1, scenes)

    def bind(kernel, *fixed):
        def run(*refs):
            return kernel(row_count, col_count, *fixed, *refs)

        return run

    extra_rows = col_count * 8 + 16
    tile_rows = scenes // row_count
    send, select = pl.pallas_call(
        bind(assemble_kernel),
        out_shape=(
            jax.ShapeDtypeStruct((devices, 96, LANES), BF16),
            jax.ShapeDtypeStruct((devices * 8, 2 * tile_rows), BF16),
        ),
        in_specs=[hbm()] * 7,
        out_specs=(vmem(),) * 2,
        scratch_shapes=[
            pltpu.VMEM((points // LANES, 64 * (scn + 1), LANES), F32),
            pltpu.VMEM((32 * (scn + 1), LANES), F32),
            pltpu.VMEM((64, scenes), F32),
            pltpu.VMEM((scenes // LANES, 36 * scn, LANES), F32),
            pltpu.VMEM((64, scenes), F32),
            pltpu.VMEM((extra_rows, scenes), F32),
            pltpu.VMEM((36 * scn + extra_rows, scenes), F32),
            pltpu.VMEM(cam_jac.shape, BF16),
            pltpu.VMEM(pt_jac.shape, BF16),
            pltpu.VMEM(resid.shape, BF16),
            pltpu.VMEM(partner.shape, jnp.int32),
            pltpu.VMEM(map_row.shape, jnp.int32),
            pltpu.SMEM(count.shape, jnp.int32),
            pltpu.SMEM(tile_map.shape, jnp.int32),
            pltpu.SemaphoreType.DMA((3, points // LANES)),
            pltpu.SemaphoreType.DMA((4,)),
        ],
        compiler_params=small_limit(36),
        name="assemble",
    )(
        *[
            pltpu.with_memory_space_constraint(value, pltpu.HBM)
            for value in (cam_jac, pt_jac, resid, partner, map_row, count, tile_map)
        ]
    )
    got = lax.all_to_all(send, AXES, 0, 0, tiled=True)
    tile, own, part = pl.pallas_call(
        bind(first_kernel),
        out_shape=(
            jax.ShapeDtypeStruct((36, HALF, tile_rows), BF16),
            jax.ShapeDtypeStruct((8, LANES), F32),
            jax.ShapeDtypeStruct((devices, 1, 10 * LANES), F32),
        ),
        in_specs=[vmem()] * 2,
        out_specs=(vmem(),) * 3,
        scratch_shapes=[pltpu.VMEM((8, LANES), F32)],
        compiler_params=small_limit(16),
        name="first",
    )(got, select)
    state = jnp.zeros((3, row_count, 8, LANES), F32)
    for turn in range(ITERS - 1):
        got = lax.all_to_all(part, AXES, 0, 0, tiled=True)
        begin = turn == 0
        outs = [
            jax.ShapeDtypeStruct((3, row_count, 8, LANES), F32),
            jax.ShapeDtypeStruct((devices, 1, 9 * LANES), F32),
        ]
        places = [vmem()] * 2
        scratch = [pltpu.VMEM((row_count, 8, LANES), F32), pltpu.VMEM((8, LANES), F32)]
        if begin:
            outs.append(jax.ShapeDtypeStruct(tile.shape, BF16))
            places.append(hbm())
            scratch.append(pltpu.SemaphoreType.DMA(()))
        state, part, *rest = pl.pallas_call(
            bind(step_kernel, begin),
            out_shape=outs,
            in_specs=[vmem()] * 4,
            out_specs=places,
            scratch_shapes=scratch,
            compiler_params=small_limit(8),
            name="step",
        )(got, tile, own, state)
        if begin:
            coupling = rest[0]
    got = lax.all_to_all(part, AXES, 0, 0, tiled=True)
    answer, remainder = pl.pallas_call(
        bind(last_kernel),
        out_shape=(jax.ShapeDtypeStruct((6, tile_rows), F32),) * 2,
        in_specs=[vmem()] * 2,
        out_specs=(vmem(),) * 2,
        scratch_shapes=[pltpu.VMEM((row_count, 8, LANES), F32)],
        compiler_params=small_limit(4),
        name="last",
    )(got, state)
    return jnp.swapaxes(coupling.reshape(6, 6, HALF, tile_rows), 2, 3), answer, remainder


def cross_product(first_vec, second_vec):
    return jnp.stack(
        [
            first_vec[1] * second_vec[2] - first_vec[2] * second_vec[1],
            first_vec[2] * second_vec[0] - first_vec[0] * second_vec[2],
            first_vec[0] * second_vec[1] - first_vec[1] * second_vec[0],
        ],
        axis=0,
    )


def point_terms(camera, points_jac, errors):
    camera = camera.astype(jnp.float32)
    points_jac = points_jac.astype(jnp.float32)
    errors = errors.astype(jnp.float32)
    own_jac, other_jac = (camera[0], camera[1])
    own_point, other_point = (points_jac[0], points_jac[1])
    own_error, other_error = (errors[0], errors[1])
    point_hessian = jnp.sum(own_point[:, :, None] * own_point[:, None, :], axis=0)
    point_hessian = point_hessian + jnp.sum(
        other_point[:, :, None] * other_point[:, None, :], axis=0
    )
    point_hessian = point_hessian + POINT_DAMPING * jnp.eye(3, dtype=jnp.float32)[:, :, None, None]
    first_row, second_row, third_row = (point_hessian[0], point_hessian[1], point_hessian[2])
    cofactor_first = cross_product(second_row, third_row)
    cofactor_second = cross_product(third_row, first_row)
    cofactor_third = cross_product(first_row, second_row)
    determinant = jnp.sum(first_row * cofactor_first, axis=0)
    inverse = jnp.stack([cofactor_first, cofactor_second, cofactor_third], axis=1) / determinant
    w_own = jnp.sum(own_jac[:, :, None] * own_point[:, None, :], axis=0)
    w_other = jnp.sum(other_jac[:, :, None] * other_point[:, None, :], axis=0)
    point_rhs = -(
        jnp.sum(own_point * own_error[:, None], axis=0)
        + jnp.sum(other_point * other_error[:, None], axis=0)
    )
    own_vi = jnp.sum(w_own[:, :, None] * inverse[None, :, :], axis=1)
    other_vi = jnp.sum(w_other[:, :, None] * inverse[None, :, :], axis=1)
    diag_own = jnp.sum(own_jac[:, :, None] * own_jac[:, None, :], axis=0) - jnp.sum(
        own_vi[:, None, :] * w_own[None, :, :], axis=2
    )
    diag_other = jnp.sum(other_jac[:, :, None] * other_jac[:, None, :], axis=0) - jnp.sum(
        other_vi[:, None, :] * w_other[None, :, :], axis=2
    )
    link = -jnp.sum(own_vi[:, None, :] * w_other[None, :, :], axis=2)
    grad_own = -jnp.sum(own_jac * own_error[:, None], axis=0) - jnp.sum(
        own_vi * point_rhs[None], axis=1
    )
    grad_other = -jnp.sum(other_jac * other_error[:, None], axis=0) - jnp.sum(
        other_vi * point_rhs[None], axis=1
    )
    return (diag_own, diag_other, link, grad_own, grad_other)


def conjugate_steps(right_side, apply_operator, inner_product):
    solution = jnp.zeros_like(right_side)
    remainder = right_side
    direction = right_side
    norm_now = inner_product(remainder, remainder)
    for iteration in range(ITERS):
        product_vec = apply_operator(direction)
        step_size = norm_now / inner_product(direction, product_vec)
        solution = solution + step_size * direction
        remainder = remainder - step_size * product_vec
        norm_next = inner_product(remainder, remainder)
        direction = remainder + norm_next / norm_now * direction
        norm_now = norm_next
    return (solution, remainder)


def plain_shards(cam_jac, pt_jac, resid, partner, count, tile_map):
    row_count = lax.axis_size("row")
    col_count = lax.axis_size("col")
    scenes = tile_map.shape[0]
    scn_local = partner.shape[0]
    points = partner.shape[1]
    tile_rows = scenes // row_count
    tile_cols = scenes // col_count
    per_group = scn_local // row_count
    row_index = lax.axis_index("row")
    col_index = lax.axis_index("col")
    device = row_index * col_count + col_index
    positions = jnp.arange(scenes, dtype=jnp.int32)
    tile_own = lax.dynamic_slice_in_dim(tile_map, device * scn_local, scn_local)
    local_rank = jnp.sum((tile_own[None, :] < tile_own[:, None]).astype(jnp.int32), axis=1)
    active = (jnp.arange(points, dtype=jnp.int32)[None, :] < count[:, None]).astype(jnp.float32)
    diag_own, diag_other, link, grad_own, grad_other = point_terms(cam_jac, pt_jac, resid)
    values = (
        jnp.concatenate(
            [
                link.reshape(36, scn_local, points),
                diag_other.reshape(36, scn_local, points),
                grad_other,
            ],
            axis=0,
        )
        * active[None]
    )
    values = jnp.moveaxis(values, 1, 0)

    def scene_sums(item):
        scene_values, scene_partner = item
        hits = scene_partner[:, None] == positions[None, :]
        tile_other = jnp.sum(jnp.where(hits, tile_map[None, :], 0), axis=1)
        onehot = (tile_other[:, None] == positions[None, :]).astype(jnp.float32)
        return jnp.dot(
            scene_values,
            onehot,
            precision=lax.Precision.HIGHEST,
            preferred_element_type=jnp.float32,
        )

    per_scene = lax.map(scene_sums, (values, partner))
    link_rows = per_scene[:, :36, :]
    other_sum = jnp.sum(per_scene[:, 36:, :], axis=0)
    ordering = (local_rank[None, :] == jnp.arange(scn_local, dtype=jnp.int32)[:, None]).astype(
        jnp.float32
    )
    panel = jnp.einsum("rs,sxc->xrc", ordering, link_rows, precision=lax.Precision.HIGHEST)
    panel = panel.reshape(36, row_count, per_group, col_count, tile_cols).transpose(0, 1, 3, 2, 4)
    panel_short = panel.astype(jnp.bfloat16)
    own_onehot = (tile_own[:, None] == positions[None, :]).astype(jnp.float32)
    own_diag = jnp.sum(diag_own * active, axis=-1).reshape(36, scn_local)
    own_grad = jnp.sum(grad_own * active, axis=-1)
    own_both = jnp.concatenate([own_diag, own_grad], axis=0)
    own_spread = jnp.dot(
        own_both, own_onehot, precision=lax.Precision.HIGHEST, preferred_element_type=jnp.float32
    )
    both_part = own_spread + other_sum
    diag_part = both_part[:36]
    grad_part = both_part[36:]
    shaped = panel_short.reshape(36, row_count * col_count, per_group, tile_cols)
    received = lax.all_to_all(shaped, ("row", "col"), split_axis=1, concat_axis=1, tiled=True)
    received = received.reshape(36, tile_rows, tile_cols)
    diag_all, grad_all = lax.psum((diag_part, grad_part), ("row", "col"))
    row_start = row_index * tile_rows
    col_start = col_index * tile_cols
    devices = scenes // scn_local
    tiles_grid = tile_map.reshape(devices, scn_local)
    inblock = (tiles_grid >= row_start) & (tiles_grid < row_start + tile_rows)
    lower = (tiles_grid[:, None, :] < tiles_grid[:, :, None]) & inblock[:, None, :]
    within_all = jnp.sum(lower.astype(jnp.int32), axis=2)
    slot_from = (jnp.arange(devices, dtype=jnp.int32)[:, None] * per_group + within_all).reshape(-1)
    slot_to = (tiles_grid - row_start).reshape(-1)
    slots = jnp.arange(tile_rows, dtype=jnp.int32)
    to_table = ((slot_to[:, None] == slots[None, :]) & inblock.reshape(-1)[:, None]).astype(
        jnp.bfloat16
    )
    from_table = (slot_from[:, None] == slots[None, :]).astype(jnp.bfloat16)
    selection = jnp.dot(to_table.T, from_table, preferred_element_type=jnp.float32).astype(
        jnp.bfloat16
    )
    coupling_tile = jnp.einsum(
        "pk,xkc->xpc", selection, received, preferred_element_type=jnp.float32
    )
    coupling_tile = coupling_tile.astype(jnp.bfloat16).reshape(6, 6, tile_rows, tile_cols)
    coupling_wide = coupling_tile.astype(jnp.float32)
    zero_at = row_index * 0

    def tile_products(rows_part, cols_part):
        forward = jnp.einsum(
            "xyij,yj->xi", coupling_wide, cols_part, precision=lax.Precision.HIGHEST
        )
        backward = jnp.einsum(
            "xyij,xi->yj", coupling_wide, rows_part, precision=lax.Precision.HIGHEST
        )
        empty = jnp.zeros((6, scenes), jnp.float32)
        spread = lax.dynamic_update_slice(empty, forward, (zero_at, row_start))
        spread = spread + lax.dynamic_update_slice(empty, backward, (zero_at, col_start))
        return lax.psum(spread, ("row", "col"))

    diag_blocks = diag_all.reshape(6, 6, scenes)

    def apply_full(direction):
        rows_part = lax.dynamic_slice_in_dim(direction, row_start, tile_rows, 1)
        cols_part = lax.dynamic_slice_in_dim(direction, col_start, tile_cols, 1)
        summed = tile_products(rows_part, cols_part)
        result = CAMERA_DAMPING * direction
        result = result + jnp.einsum(
            "xyi,yi->xi", diag_blocks, direction, precision=lax.Precision.HIGHEST
        )
        return result + summed

    def inner_full(first_vec, second_vec):
        return jnp.sum(first_vec * second_vec)

    whole_solution, whole_remainder = conjugate_steps(grad_all, apply_full, inner_full)
    solution = lax.dynamic_slice_in_dim(whole_solution, row_start, tile_rows, 1)
    remainder = lax.dynamic_slice_in_dim(whole_remainder, row_start, tile_rows, 1)
    return (coupling_tile, solution, remainder)


def shards(cam_jac, pt_jac, resid, partner, count, tile_map):
    row_count = lax.axis_size("row")
    col_count = lax.axis_size("col")
    scenes = tile_map.shape[0]
    scn, points = partner.shape
    packs = (
        scenes == col_count * HALF
        and scenes == row_count * LANES
        and scn == row_count * 4
        and LANES % scn == 0
        and points % LANES == 0
        and col_count >= 7
    )
    run = packed_shards if packs else plain_shards
    return run(cam_jac, pt_jac, resid, partner, count, tile_map)


def solution(mesh):
    return jax.shard_map(
        shards,
        mesh=mesh,
        in_specs=(
            P(None, None, None, AXES, None),
            P(None, None, None, AXES, None),
            P(None, None, AXES, None),
            P(AXES, None),
            P(AXES),
            P(),
        ),
        out_specs=(P(None, None, "row", "col"), P(None, "row"), P(None, "row")),
        check_vma=False,
    )
```

```python
import jax
import jax.numpy as jnp
from jax import lax
from jax.experimental import pallas as pl
from jax.experimental.pallas import tpu as pltpu
from jax.sharding import PartitionSpec as P

ITERS = 3
CAMERA_DAMPING = 1.0
POINT_DAMPING = 1.0
AXES = ("row", "col")
LANES = 128
HALF = 64
F32 = jnp.float32
BF16 = jnp.bfloat16
PAIRS = [(x, y) for x in range(6) for y in range(x, 6)]
CONTRACT_LAST = (((1,), (1,)), ((), ()))


def iota(shape, dim):
    return lax.broadcasted_iota(jnp.int32, shape, dim)


def split_two(value):
    high = value.astype(BF16)
    low = (value - high.astype(F32)).astype(BF16)
    return high, low


def point_values(ja, jb, pa, pb, ea, eb, live):
    one = POINT_DAMPING
    hess = {}
    for x in range(3):
        for y in range(x, 3):
            h = pa[0][x] * pa[0][y] + pa[1][x] * pa[1][y]
            h = h + (pb[0][x] * pb[0][y] + pb[1][x] * pb[1][y])
            hess[x, y] = h + one if x == y else h
    a, b, c = hess[0, 0], hess[0, 1], hess[0, 2]
    d, e, f = hess[1, 1], hess[1, 2], hess[2, 2]
    c00 = d * f - e * e
    c01 = c * e - b * f
    c02 = b * e - c * d
    c11 = a * f - c * c
    c12 = b * c - a * e
    c22 = a * d - b * b
    det = a * c00 + b * c01 + c * c02
    inv = 1.0 / det
    vi = [[c00 * inv, c01 * inv, c02 * inv], [None, c11 * inv, c12 * inv], [None, None, c22 * inv]]
    vi[1][0], vi[2][0], vi[2][1] = vi[0][1], vi[0][2], vi[1][2]
    q = [
        -((pa[0][k] * ea[0] + pa[1][k] * ea[1]) + (pb[0][k] * eb[0] + pb[1][k] * eb[1]))
        for k in range(3)
    ]
    viq = [vi[k][0] * q[0] + vi[k][1] * q[1] + vi[k][2] * q[2] for k in range(3)]

    def times_vi(p):
        return [
            [p[m][0] * vi[0][k] + p[m][1] * vi[1][k] + p[m][2] * vi[2][k] for k in range(3)]
            for m in range(2)
        ]

    def inner(left, right):
        return left[0] * right[0] + left[1] * right[1] + left[2] * right[2]

    def keep(value):
        return jnp.where(live, value, 0.0)

    av = times_vi(pa)
    bv = times_vi(pb)
    m_ab = [[keep(-inner(av[m], pb[k])) for k in range(2)] for m in range(2)]
    g_aa = [keep(1.0 - inner(av[0], pa[0])), keep(-inner(av[0], pa[1])), keep(1.0 - inner(av[1], pa[1]))]
    g_bb = [keep(1.0 - inner(bv[0], pb[0])), keep(-inner(bv[0], pb[1])), keep(1.0 - inner(bv[1], pb[1]))]
    h_a = [keep(-(ea[m] + inner(pa[m], viq))) for m in range(2)]
    h_b = [keep(-(eb[m] + inner(pb[m], viq))) for m in range(2)]

    mj = [[m_ab[m][0] * jb[0][y] + m_ab[m][1] * jb[1][y] for y in range(6)] for m in range(2)]
    link = {}
    for x in range(6):
        for y in range(6):
            link[x, y] = ja[0][x] * mj[0][y] + ja[1][x] * mj[1][y]

    def diagonal(j, g):
        gj = [
            [g[0] * j[0][y] + g[1] * j[1][y] for y in range(6)],
            [g[1] * j[0][y] + g[2] * j[1][y] for y in range(6)],
        ]
        return [j[0][x] * gj[0][y] + j[1][x] * gj[1][y] for x, y in PAIRS]

    diag_own = diagonal(ja, g_aa)
    diag_other = diagonal(jb, g_bb)
    grad_own = [ja[0][x] * h_a[0] + ja[1][x] * h_a[1] for x in range(6)]
    grad_other = [jb[0][x] * h_b[0] + jb[1][x] * h_b[1] for x in range(6)]
    return diag_own, diag_other, link, grad_own, grad_other


def selection(row_count, map_ref, scn, tile_rows, per_group):
    scenes = map_ref.shape[1]
    row = lax.axis_index("row")
    tiles = jnp.concatenate(
        [map_ref[:, t * LANES : (t + 1) * LANES] for t in range(scenes // LANES)], axis=0
    )
    groups = scenes // LANES
    place = iota((groups, LANES), 1) % scn
    rank = jnp.zeros((groups, LANES), jnp.int32)
    for shift in range(1, scn):
        before = pltpu.roll(tiles, shift, 1)
        after = pltpu.roll(tiles, LANES - shift, 1)
        rank = rank + ((before < tiles) & (place >= shift)).astype(jnp.int32)
        rank = rank + ((after < tiles) & (place + shift < scn)).astype(jnp.int32)
    scene_id = iota((groups, LANES), 0) * LANES + iota((groups, LANES), 1)
    slot_at = (scene_id // scn) * 8 + rank % per_group
    local = tiles - row * tile_rows
    slot_at = jnp.where((local >= 0) & (local < tile_rows), slot_at, -1)
    deep = scenes // scn * 8
    select = jnp.zeros((deep, tile_rows), F32)
    for t in range(groups):
        to_row = jnp.where(iota((tile_rows, LANES), 0) == local[t : t + 1, :], 1.0, 0.0).astype(BF16)
        from_slot = jnp.where(iota((deep, LANES), 0) == slot_at[t : t + 1, :], 1.0, 0.0).astype(BF16)
        select = select + lax.dot_general(from_slot, to_row, CONTRACT_LAST, preferred_element_type=F32)
    return jnp.concatenate([select, pltpu.roll(select, 4, 0)], axis=1).astype(BF16)


def assemble_kernel(
    row_count, col_count, cam_in, pt_in, res_in, partner_in, row_in, count_in, map_in, send_ref,
    select_ref,
    vals_ref, own_ref, acc_ref, links_ref, flat_ref, extra_ref, perm_ref,
    cam_ref, pt_ref, res_ref, partner_ref, map_ref, count_sm, map_sm, slab_sem, whole_sem,
):
    scn = partner_ref.shape[0]
    points = partner_ref.shape[1]
    scenes = map_ref.shape[1]
    wholes = [
        pltpu.make_async_copy(source, target, whole_sem.at[k])
        for k, (source, target) in enumerate(
            [(count_in, count_sm), (map_in, map_sm), (row_in, map_ref), (partner_in, partner_ref)]
        )
    ]

    def slab_copies(step):
        lanes = pl.ds(pl.multiple_of(step * LANES, LANES), LANES)
        return [
            pltpu.make_async_copy(
                source.at[..., lanes], target.at[..., lanes], slab_sem.at[k, step]
            )
            for k, (source, target) in enumerate([(cam_in, cam_ref), (pt_in, pt_ref), (res_in, res_ref)])
        ]

    wholes[0].start()
    for step in range(points // LANES):
        for copy in slab_copies(step):
            copy.start()
    for copy in wholes[1:]:
        copy.start()
    per_group = scn // row_count
    device = lax.axis_index("row") * col_count + lax.axis_index("col")
    slab = (scn, LANES)
    pitch = scn + 1

    own_ref[...] = jnp.zeros_like(own_ref)
    acc_ref[...] = jnp.zeros_like(acc_ref)
    extra_ref[...] = jnp.zeros_like(extra_ref)
    vals_ref[:, pl.ds(63 * pitch, scn), :] = jnp.zeros((points // LANES, scn, LANES), F32)

    wholes[0].wait()
    sub = iota(slab, 0)
    counts = jnp.zeros(slab, jnp.int32)
    for s in range(scn):
        counts = jnp.where(sub == s, count_sm[s], counts)

    def slab_step(step, carry):
        for copy in slab_copies(step):
            copy.wait()
        lanes = pl.ds(pl.multiple_of(step * LANES, LANES), LANES)

        def get(ref, *where):
            return ref[where + (slice(None), lanes)].astype(F32)

        ja = [[get(cam_ref, 0, m, x) for x in range(6)] for m in range(2)]
        jb = [[get(cam_ref, 1, m, x) for x in range(6)] for m in range(2)]
        pa = [[get(pt_ref, 0, m, x) for x in range(3)] for m in range(2)]
        pb = [[get(pt_ref, 1, m, x) for x in range(3)] for m in range(2)]
        ea = [get(res_ref, 0, m) for m in range(2)]
        eb = [get(res_ref, 1, m) for m in range(2)]
        live = (iota(slab, 1) + step * LANES) < counts
        diag_own, diag_other, link, grad_own, grad_other = point_values(ja, jb, pa, pb, ea, eb, live)

        def put(q, value):
            vals_ref[step, pl.ds(q * pitch, scn), :] = value

        def put_own(q, value):
            own_ref[pl.ds(q * pitch, scn), :] += value

        for x in range(3):
            for y in range(6):
                put(x * 6 + y, link[x, y])
                put(24 + x * 6 + y, link[x + 3, y])
        for x in range(6):
            put(18 + x, grad_other[x])
            put_own(2 + x, grad_own[x])
        for q in range(21):
            put(42 + q, diag_other[q])
            put_own(10 + q, diag_own[q])
        return carry

    lax.fori_loop(0, points // LANES, slab_step, 0)

    for copy in wholes[1:]:
        copy.wait()
    select_ref[...] = selection(row_count, map_ref, scn, scenes // row_count, per_group)
    spots = iota((points, scenes), 1).astype(jnp.int16)
    mates = jnp.transpose(partner_ref[...]).astype(jnp.int16)

    def scene_step(s):
        values = jnp.concatenate(
            [vals_ref.at[t][pl.ds(s, 64, stride=pitch), :] for t in range(points // LANES)], axis=1
        )
        high, low = split_two(values)
        left = jnp.concatenate([high, low], axis=0)
        onehot = jnp.where(spots == mates[:, s : s + 1], jnp.asarray(1, BF16), jnp.asarray(0, BF16))
        both = jnp.dot(left, onehot, preferred_element_type=F32)
        total = both[:64] + both[64:]
        acc_ref[...] += total
        mine = map_sm[device * scn + s]
        rank = jnp.int32(0)
        for other in range(scn):
            rank = rank + (map_sm[device * scn + other] < mine).astype(jnp.int32)
        base = lax.div(rank, per_group) * (36 * per_group) + lax.rem(rank, per_group)
        for t in range(scenes // LANES):
            cols = slice(t * LANES, (t + 1) * LANES)
            links_ref.at[t][pl.ds(base, 18, stride=per_group), :] = total[0:18, cols]
            links_ref.at[t][pl.ds(base + 18 * per_group, 18, stride=per_group), :] = total[24:42, cols]

    for s in range(scn):
        scene_step(s)

    lane = iota((32, LANES), 1)
    own = jnp.zeros((32, LANES), F32)
    for s in range(scn):
        column = jnp.sum(own_ref[pl.ds(s, 32, stride=pitch), :], axis=1, keepdims=True)
        own = own + jnp.where(lane == s, column, 0.0)
    start = device * scn
    own = pltpu.roll(own, lax.rem(start, LANES), 1)
    tile_at = lax.div(start, LANES)
    for t in range(scenes // LANES):
        cols = pl.ds(t * LANES, LANES)
        whole = jnp.concatenate([acc_ref[16:24, cols], acc_ref[40:64, cols]], axis=0)
        whole = whole + jnp.where(tile_at == t, own, 0.0)
        high, low = split_two(whole)
        flat_ref[0:32, cols] = high.astype(F32)
        flat_ref[32:64, cols] = low.astype(F32)
    per_col = -(-21 // col_count)
    for c in range(col_count):
        for i in range(per_col):
            q = c * per_col + i
            if q < 21:
                extra_ref[c * 8 + 2 * i : c * 8 + 2 * i + 1, :] = flat_ref[10 + q : 11 + q, :]
                extra_ref[c * 8 + 2 * i + 1 : c * 8 + 2 * i + 2, :] = flat_ref[42 + q : 43 + q, :]
    base = col_count * 8
    extra_ref[base : base + 8, :] = flat_ref[0:8, :]
    extra_ref[base + 8 : base + 16, :] = flat_ref[32:40, :]

    places = jnp.transpose(jnp.broadcast_to(map_ref[...], (8, scenes)))[:, :1]
    onto = jnp.where(iota((scenes, scenes), 1) == places, 1.0, 0.0).astype(BF16)
    links = jnp.concatenate([links_ref[t] for t in range(scenes // LANES)], axis=1)
    left = jnp.concatenate([links.astype(BF16), extra_ref[...].astype(BF16)], axis=0)
    perm_ref[...] = jnp.dot(left, onto, preferred_element_type=F32)

    top = scn * 36
    side = 18 * per_group
    first = iota((8, LANES), 1) < HALF
    head_rows = iota((8, LANES), 0) < 2
    first_side = iota((side, LANES), 1) < HALF

    def merge(low_part, high_part, mask):
        even = jnp.where(mask, low_part, pltpu.roll(high_part, HALF, 1))
        odd = jnp.where(mask, pltpu.roll(low_part, HALF, 1), high_part)
        return even, odd

    grads = [pl.ds(top + base + 8 * k, 8) for k in range(2)]
    for j in range(col_count // 2):
        cols = pl.ds(j * LANES, LANES)
        grad_cols = merge(perm_ref[grads[0], cols], perm_ref[grads[1], cols], first)
        for r in range(row_count):
            rows = pl.ds(r * LANES, LANES)
            at = r * 2 * side
            pieces = merge(perm_ref[at : at + side, cols], perm_ref[at + side : at + 2 * side, cols], first_side)
            for k in range(2):
                c = 2 * j + k
                spot = r * col_count + c
                send_ref[spot, 0:side, :] = pieces[k].astype(BF16)
                own = perm_ref[top + c * 8 : top + c * 8 + 8, rows]
                tails = [perm_ref[grads[0], rows], perm_ref[grads[1], rows], grad_cols[k]]
                for i, tail in enumerate(tails):
                    turned = own if i == 0 else pltpu.roll(own, 8 - 2 * i, 0)
                    block = jnp.where(head_rows, turned, tail)
                    send_ref[spot, side + 8 * i : side + 8 * i + 8, :] = block.astype(BF16)


def tile_matvec(tile_ref, own_ref, rows_part, cols_part, rows_ref):
    which = iota((8, LANES), 0)
    turned = jnp.transpose(cols_part)[:HALF]
    forward = [jnp.zeros((8, LANES), F32) for _ in range(6)]
    backward = []
    for y in range(6):
        column = jnp.broadcast_to(turned[:, y : y + 1], (HALF, LANES))
        total = jnp.zeros((HALF, LANES), F32)
        for x in range(6):
            block = tile_ref[x * 6 + y].astype(F32)
            forward[x] = forward[x] + jnp.sum((block * column).reshape(HALF // 8, 8, LANES), axis=0)
            total = total + block * rows_part[x : x + 1, :]
        backward.append(total)
    sides = []
    for y in range(3):
        pair = jnp.concatenate([backward[y], backward[y + 3]], axis=0)
        sides.append(jnp.sum(jnp.transpose(pair), axis=0, keepdims=True))
    out = jnp.zeros((8, LANES), F32)
    for x in range(6):
        out = jnp.where(which == x, jnp.sum(forward[x], axis=0, keepdims=True), out)
    rows_ref[...] = rows_part
    col = lax.axis_index("col")
    per_col = -(-21 // lax.axis_size("col"))
    for i in range(per_col):
        q = jnp.minimum(col * per_col + i, 20)
        x = jnp.int32(0)
        start = jnp.int32(0)
        for line in range(1, 6):
            past = (q >= PAIRS.index((line, line))).astype(jnp.int32)
            x = x + past
            start = start + past * (7 - line)
        y = q - start + x
        weight = own_ref[i : i + 1, :]
        at_x = rows_ref[pl.ds(x, 1), :] * weight
        at_y = rows_ref[pl.ds(y, 1), :] * weight
        out = out + jnp.where(which == x, at_y, 0.0)
        out = out + jnp.where((which == y) & (x != y), at_x, 0.0)
    return out, sides


def write_partials(out, sides, line, part_ref):
    rows = [out[x : x + 1, :] for x in range(6)] + sides
    if line is not None:
        rows.append(line)
    for n in range(part_ref.shape[0]):
        for k, row in enumerate(rows):
            part_ref[n, :, k * LANES : (k + 1) * LANES] = row


def first_kernel(
    row_count, col_count, got_ref, select_ref, tile_ref, own_ref, part_ref, rows_ref,
):
    devices = got_ref.shape[0]
    deep, tile_rows = select_ref.shape[0], select_ref.shape[1] // 2
    per_group = tile_rows // devices
    select = select_ref[...]
    for k in range(9):
        picked = got_ref[:, k * 8 : k * 8 + 8, :].reshape(deep, LANES)
        block = lax.dot_general(picked, select, (((0,), (0,)), ((), ())), preferred_element_type=F32)
        block = block.astype(BF16)
        for e in range(2):
            cols = slice(e * tile_rows, (e + 1) * tile_rows)
            tile_ref[2 * k + e] = block[:HALF, cols]
            tile_ref[2 * k + e + 18] = block[HALF:, cols]
    extras = []
    for i in range(3):
        rows = pl.ds(18 * per_group + 8 * i, 8)
        total = got_ref[0, rows, :].astype(F32)
        for n in range(1, devices):
            total = total + got_ref[n, rows, :].astype(F32)
        own_ref[i : i + 1, :] = total[0:1] + total[1:2]
        extras.append(pltpu.roll(total, 6, 0))
    used = iota((8, LANES), 0) < 6
    rows_part = jnp.where(used, extras[0] + extras[1], 0.0)
    cols_part = jnp.where(used, extras[2] + pltpu.roll(extras[2], HALF, 1), 0.0)
    out, sides = tile_matvec(tile_ref, own_ref, rows_part, cols_part, rows_ref)
    rows_ref[...] = rows_part
    line = rows_ref[pl.ds(jnp.minimum(lax.axis_index("col"), 5), 1), :]
    write_partials(out, sides, line, part_ref)


def gather_image(row_count, col_count, got_ref, image_ref):
    first = iota((1, LANES), 1) < HALF
    side = 6 * LANES
    cols = []
    for c in range(col_count):
        total = got_ref[c, :, side : side + 3 * LANES]
        for r in range(1, row_count):
            total = total + got_ref[r * col_count + c, :, side : side + 3 * LANES]
        cols.append(total)
    for r in range(row_count):
        total = got_ref[r * col_count, :, 0:side]
        for c in range(1, col_count):
            total = total + got_ref[r * col_count + c, :, 0:side]
        image_ref[r] = jnp.zeros((8, LANES), F32)
        for t in range(3):
            left = cols[2 * r][:, t * LANES : (t + 1) * LANES]
            right = cols[2 * r + 1][:, t * LANES : (t + 1) * LANES]
            low = jnp.where(first, left, pltpu.roll(right, HALF, 1))
            high = jnp.where(first, pltpu.roll(left, HALF, 1), right)
            image_ref[r, t : t + 1, :] = total[:, t * LANES : (t + 1) * LANES] + low
            image_ref[r, t + 3 : t + 4, :] = total[:, (t + 3) * LANES : (t + 4) * LANES] + high


def inner_all(left, right):
    return jnp.sum(jnp.sum(left * right, axis=0), keepdims=True)


def step_kernel(
    row_count, col_count, begin, got_ref, tile_ref, own_ref, state_ref, next_ref, part_ref,
    *rest,
):
    if begin:
        coupling_ref, image_ref, rows_ref, copy_sem = rest
        quarter = tile_ref.shape[0] // 4
        copies = [
            pltpu.make_async_copy(
                tile_ref.at[pl.ds(k * quarter, quarter)],
                coupling_ref.at[pl.ds(k * quarter, quarter)],
                copy_sem.at[k],
            )
            for k in range(4)
        ]
        for copy in copies:
            copy.start()
    else:
        image_ref, rows_ref = rest
    gather_image(row_count, col_count, got_ref, image_ref)
    if begin:
        for r in range(row_count):
            next_ref[1, r] = jnp.zeros((8, LANES), F32)
            for x in range(6):
                next_ref[1, r, x : x + 1, :] = got_ref[r * col_count + x, :, 9 * LANES : 10 * LANES]
        remainder = next_ref[1]
        direction = remainder
        answer = jnp.zeros_like(remainder)
    else:
        answer, remainder, direction = state_ref[0], state_ref[1], state_ref[2]
    norm_now = inner_all(remainder, remainder)
    image = CAMERA_DAMPING * direction + image_ref[...]
    alpha = norm_now / inner_all(direction, image)
    answer = answer + alpha * direction
    remainder = remainder - alpha * image
    norm_next = inner_all(remainder, remainder)
    direction = remainder + norm_next / norm_now * direction
    next_ref[0] = answer
    next_ref[1] = remainder
    next_ref[2] = direction
    col = lax.axis_index("col")
    rows_part = next_ref[2, lax.axis_index("row")]
    wide = next_ref[2, lax.div(col, 2)]
    turned = pltpu.roll(wide, HALF, 1)
    cols_part = jnp.where(iota((8, LANES), 0) * 0 == lax.rem(col, 2), wide, turned)
    out, sides = tile_matvec(tile_ref, own_ref, rows_part, cols_part, rows_ref)
    write_partials(out, sides, None, part_ref)
    if begin:
        for copy in copies:
            copy.wait()


def last_kernel(row_count, col_count, got_ref, state_ref, answer_ref, remainder_ref, image_ref):
    gather_image(row_count, col_count, got_ref, image_ref)
    remainder, direction = state_ref[1], state_ref[2]
    norm_now = inner_all(remainder, remainder)
    image_ref[...] = CAMERA_DAMPING * direction + image_ref[...]
    alpha = norm_now / inner_all(direction, image_ref[...])
    row = lax.axis_index("row")
    answer_ref[...] = (state_ref[0, row] + alpha * state_ref[2, row])[:6]
    remainder_ref[...] = (state_ref[1, row] - alpha * image_ref[row])[:6]


def vmem():
    return pl.BlockSpec(memory_space=pltpu.VMEM)


def hbm():
    return pl.BlockSpec(memory_space=pltpu.HBM)


def small_limit(mib):
    return pltpu.CompilerParams(vmem_limit_bytes=mib << 20)


def packed_shards(cam_jac, pt_jac, resid, partner, count, tile_map):
    row_count = lax.axis_size("row")
    col_count = lax.axis_size("col")
    devices = row_count * col_count
    scenes = tile_map.shape[0]
    scn, points = partner.shape
    map_row = tile_map.reshape(1, scenes)

    def bind(kernel, *fixed):
        def run(*refs):
            return kernel(row_count, col_count, *fixed, *refs)

        return run

    extra_rows = col_count * 8 + 16
    tile_rows = scenes // row_count
    send, select = pl.pallas_call(
        bind(assemble_kernel),
        out_shape=(
            jax.ShapeDtypeStruct((devices, 96, LANES), BF16),
            jax.ShapeDtypeStruct((devices * 8, 2 * tile_rows), BF16),
        ),
        in_specs=[hbm()] * 7,
        out_specs=(vmem(),) * 2,
        scratch_shapes=[
            pltpu.VMEM((points // LANES, 64 * (scn + 1), LANES), F32),
            pltpu.VMEM((32 * (scn + 1), LANES), F32),
            pltpu.VMEM((64, scenes), F32),
            pltpu.VMEM((scenes // LANES, 36 * scn, LANES), F32),
            pltpu.VMEM((64, scenes), F32),
            pltpu.VMEM((extra_rows, scenes), F32),
            pltpu.VMEM((36 * scn + extra_rows, scenes), F32),
            pltpu.VMEM(cam_jac.shape, BF16),
            pltpu.VMEM(pt_jac.shape, BF16),
            pltpu.VMEM(resid.shape, BF16),
            pltpu.VMEM(partner.shape, jnp.int32),
            pltpu.VMEM(map_row.shape, jnp.int32),
            pltpu.SMEM(count.shape, jnp.int32),
            pltpu.SMEM(tile_map.shape, jnp.int32),
            pltpu.SemaphoreType.DMA((3, points // LANES)),
            pltpu.SemaphoreType.DMA((4,)),
        ],
        compiler_params=small_limit(36),
        name="assemble",
    )(
        *[
            pltpu.with_memory_space_constraint(value, pltpu.HBM)
            for value in (cam_jac, pt_jac, resid, partner, map_row, count, tile_map)
        ]
    )
    got = lax.all_to_all(send, AXES, 0, 0, tiled=True)
    tile, own, part = pl.pallas_call(
        bind(first_kernel),
        out_shape=(
            jax.ShapeDtypeStruct((36, HALF, tile_rows), BF16),
            jax.ShapeDtypeStruct((8, LANES), F32),
            jax.ShapeDtypeStruct((devices, 1, 10 * LANES), F32),
        ),
        in_specs=[vmem()] * 2,
        out_specs=(vmem(),) * 3,
        scratch_shapes=[pltpu.VMEM((8, LANES), F32)],
        compiler_params=small_limit(16),
        name="first",
    )(got, select)
    state = jnp.zeros((3, row_count, 8, LANES), F32)
    for turn in range(ITERS - 1):
        got = lax.all_to_all(part, AXES, 0, 0, tiled=True)
        begin = turn == 0
        outs = [
            jax.ShapeDtypeStruct((3, row_count, 8, LANES), F32),
            jax.ShapeDtypeStruct((devices, 1, 9 * LANES), F32),
        ]
        places = [vmem()] * 2
        scratch = [pltpu.VMEM((row_count, 8, LANES), F32), pltpu.VMEM((8, LANES), F32)]
        if begin:
            outs.append(jax.ShapeDtypeStruct(tile.shape, BF16))
            places.append(hbm())
            scratch.append(pltpu.SemaphoreType.DMA((4,)))
        state, part, *rest = pl.pallas_call(
            bind(step_kernel, begin),
            out_shape=outs,
            in_specs=[vmem()] * 4,
            out_specs=places,
            scratch_shapes=scratch,
            compiler_params=small_limit(8),
            name="step",
        )(got, tile, own, state)
        if begin:
            coupling = rest[0]
    got = lax.all_to_all(part, AXES, 0, 0, tiled=True)
    answer, remainder = pl.pallas_call(
        bind(last_kernel),
        out_shape=(jax.ShapeDtypeStruct((6, tile_rows), F32),) * 2,
        in_specs=[vmem()] * 2,
        out_specs=(vmem(),) * 2,
        scratch_shapes=[pltpu.VMEM((row_count, 8, LANES), F32)],
        compiler_params=small_limit(4),
        name="last",
    )(got, state)
    return jnp.swapaxes(coupling.reshape(6, 6, HALF, tile_rows), 2, 3), answer, remainder


def cross_product(first_vec, second_vec):
    return jnp.stack(
        [
            first_vec[1] * second_vec[2] - first_vec[2] * second_vec[1],
            first_vec[2] * second_vec[0] - first_vec[0] * second_vec[2],
            first_vec[0] * second_vec[1] - first_vec[1] * second_vec[0],
        ],
        axis=0,
    )


def point_terms(camera, points_jac, errors):
    camera = camera.astype(jnp.float32)
    points_jac = points_jac.astype(jnp.float32)
    errors = errors.astype(jnp.float32)
    own_jac, other_jac = (camera[0], camera[1])
    own_point, other_point = (points_jac[0], points_jac[1])
    own_error, other_error = (errors[0], errors[1])
    point_hessian = jnp.sum(own_point[:, :, None] * own_point[:, None, :], axis=0)
    point_hessian = point_hessian + jnp.sum(
        other_point[:, :, None] * other_point[:, None, :], axis=0
    )
    point_hessian = point_hessian + POINT_DAMPING * jnp.eye(3, dtype=jnp.float32)[:, :, None, None]
    first_row, second_row, third_row = (point_hessian[0], point_hessian[1], point_hessian[2])
    cofactor_first = cross_product(second_row, third_row)
    cofactor_second = cross_product(third_row, first_row)
    cofactor_third = cross_product(first_row, second_row)
    determinant = jnp.sum(first_row * cofactor_first, axis=0)
    inverse = jnp.stack([cofactor_first, cofactor_second, cofactor_third], axis=1) / determinant
    w_own = jnp.sum(own_jac[:, :, None] * own_point[:, None, :], axis=0)
    w_other = jnp.sum(other_jac[:, :, None] * other_point[:, None, :], axis=0)
    point_rhs = -(
        jnp.sum(own_point * own_error[:, None], axis=0)
        + jnp.sum(other_point * other_error[:, None], axis=0)
    )
    own_vi = jnp.sum(w_own[:, :, None] * inverse[None, :, :], axis=1)
    other_vi = jnp.sum(w_other[:, :, None] * inverse[None, :, :], axis=1)
    diag_own = jnp.sum(own_jac[:, :, None] * own_jac[:, None, :], axis=0) - jnp.sum(
        own_vi[:, None, :] * w_own[None, :, :], axis=2
    )
    diag_other = jnp.sum(other_jac[:, :, None] * other_jac[:, None, :], axis=0) - jnp.sum(
        other_vi[:, None, :] * w_other[None, :, :], axis=2
    )
    link = -jnp.sum(own_vi[:, None, :] * w_other[None, :, :], axis=2)
    grad_own = -jnp.sum(own_jac * own_error[:, None], axis=0) - jnp.sum(
        own_vi * point_rhs[None], axis=1
    )
    grad_other = -jnp.sum(other_jac * other_error[:, None], axis=0) - jnp.sum(
        other_vi * point_rhs[None], axis=1
    )
    return (diag_own, diag_other, link, grad_own, grad_other)


def conjugate_steps(right_side, apply_operator, inner_product):
    solution = jnp.zeros_like(right_side)
    remainder = right_side
    direction = right_side
    norm_now = inner_product(remainder, remainder)
    for iteration in range(ITERS):
        product_vec = apply_operator(direction)
        step_size = norm_now / inner_product(direction, product_vec)
        solution = solution + step_size * direction
        remainder = remainder - step_size * product_vec
        norm_next = inner_product(remainder, remainder)
        direction = remainder + norm_next / norm_now * direction
        norm_now = norm_next
    return (solution, remainder)


def plain_shards(cam_jac, pt_jac, resid, partner, count, tile_map):
    row_count = lax.axis_size("row")
    col_count = lax.axis_size("col")
    scenes = tile_map.shape[0]
    scn_local = partner.shape[0]
    points = partner.shape[1]
    tile_rows = scenes // row_count
    tile_cols = scenes // col_count
    per_group = scn_local // row_count
    row_index = lax.axis_index("row")
    col_index = lax.axis_index("col")
    device = row_index * col_count + col_index
    positions = jnp.arange(scenes, dtype=jnp.int32)
    tile_own = lax.dynamic_slice_in_dim(tile_map, device * scn_local, scn_local)
    local_rank = jnp.sum((tile_own[None, :] < tile_own[:, None]).astype(jnp.int32), axis=1)
    active = (jnp.arange(points, dtype=jnp.int32)[None, :] < count[:, None]).astype(jnp.float32)
    diag_own, diag_other, link, grad_own, grad_other = point_terms(cam_jac, pt_jac, resid)
    values = (
        jnp.concatenate(
            [
                link.reshape(36, scn_local, points),
                diag_other.reshape(36, scn_local, points),
                grad_other,
            ],
            axis=0,
        )
        * active[None]
    )
    values = jnp.moveaxis(values, 1, 0)

    def scene_sums(item):
        scene_values, scene_partner = item
        hits = scene_partner[:, None] == positions[None, :]
        tile_other = jnp.sum(jnp.where(hits, tile_map[None, :], 0), axis=1)
        onehot = (tile_other[:, None] == positions[None, :]).astype(jnp.float32)
        return jnp.dot(
            scene_values,
            onehot,
            precision=lax.Precision.HIGHEST,
            preferred_element_type=jnp.float32,
        )

    per_scene = lax.map(scene_sums, (values, partner))
    link_rows = per_scene[:, :36, :]
    other_sum = jnp.sum(per_scene[:, 36:, :], axis=0)
    ordering = (local_rank[None, :] == jnp.arange(scn_local, dtype=jnp.int32)[:, None]).astype(
        jnp.float32
    )
    panel = jnp.einsum("rs,sxc->xrc", ordering, link_rows, precision=lax.Precision.HIGHEST)
    panel = panel.reshape(36, row_count, per_group, col_count, tile_cols).transpose(0, 1, 3, 2, 4)
    panel_short = panel.astype(jnp.bfloat16)
    own_onehot = (tile_own[:, None] == positions[None, :]).astype(jnp.float32)
    own_diag = jnp.sum(diag_own * active, axis=-1).reshape(36, scn_local)
    own_grad = jnp.sum(grad_own * active, axis=-1)
    own_both = jnp.concatenate([own_diag, own_grad], axis=0)
    own_spread = jnp.dot(
        own_both, own_onehot, precision=lax.Precision.HIGHEST, preferred_element_type=jnp.float32
    )
    both_part = own_spread + other_sum
    diag_part = both_part[:36]
    grad_part = both_part[36:]
    shaped = panel_short.reshape(36, row_count * col_count, per_group, tile_cols)
    received = lax.all_to_all(shaped, ("row", "col"), split_axis=1, concat_axis=1, tiled=True)
    received = received.reshape(36, tile_rows, tile_cols)
    diag_all, grad_all = lax.psum((diag_part, grad_part), ("row", "col"))
    row_start = row_index * tile_rows
    col_start = col_index * tile_cols
    devices = scenes // scn_local
    tiles_grid = tile_map.reshape(devices, scn_local)
    inblock = (tiles_grid >= row_start) & (tiles_grid < row_start + tile_rows)
    lower = (tiles_grid[:, None, :] < tiles_grid[:, :, None]) & inblock[:, None, :]
    within_all = jnp.sum(lower.astype(jnp.int32), axis=2)
    slot_from = (jnp.arange(devices, dtype=jnp.int32)[:, None] * per_group + within_all).reshape(-1)
    slot_to = (tiles_grid - row_start).reshape(-1)
    slots = jnp.arange(tile_rows, dtype=jnp.int32)
    to_table = ((slot_to[:, None] == slots[None, :]) & inblock.reshape(-1)[:, None]).astype(
        jnp.bfloat16
    )
    from_table = (slot_from[:, None] == slots[None, :]).astype(jnp.bfloat16)
    selection = jnp.dot(to_table.T, from_table, preferred_element_type=jnp.float32).astype(
        jnp.bfloat16
    )
    coupling_tile = jnp.einsum(
        "pk,xkc->xpc", selection, received, preferred_element_type=jnp.float32
    )
    coupling_tile = coupling_tile.astype(jnp.bfloat16).reshape(6, 6, tile_rows, tile_cols)
    coupling_wide = coupling_tile.astype(jnp.float32)
    zero_at = row_index * 0

    def tile_products(rows_part, cols_part):
        forward = jnp.einsum(
            "xyij,yj->xi", coupling_wide, cols_part, precision=lax.Precision.HIGHEST
        )
        backward = jnp.einsum(
            "xyij,xi->yj", coupling_wide, rows_part, precision=lax.Precision.HIGHEST
        )
        empty = jnp.zeros((6, scenes), jnp.float32)
        spread = lax.dynamic_update_slice(empty, forward, (zero_at, row_start))
        spread = spread + lax.dynamic_update_slice(empty, backward, (zero_at, col_start))
        return lax.psum(spread, ("row", "col"))

    diag_blocks = diag_all.reshape(6, 6, scenes)

    def apply_full(direction):
        rows_part = lax.dynamic_slice_in_dim(direction, row_start, tile_rows, 1)
        cols_part = lax.dynamic_slice_in_dim(direction, col_start, tile_cols, 1)
        summed = tile_products(rows_part, cols_part)
        result = CAMERA_DAMPING * direction
        result = result + jnp.einsum(
            "xyi,yi->xi", diag_blocks, direction, precision=lax.Precision.HIGHEST
        )
        return result + summed

    def inner_full(first_vec, second_vec):
        return jnp.sum(first_vec * second_vec)

    whole_solution, whole_remainder = conjugate_steps(grad_all, apply_full, inner_full)
    solution = lax.dynamic_slice_in_dim(whole_solution, row_start, tile_rows, 1)
    remainder = lax.dynamic_slice_in_dim(whole_remainder, row_start, tile_rows, 1)
    return (coupling_tile, solution, remainder)


def shards(cam_jac, pt_jac, resid, partner, count, tile_map):
    row_count = lax.axis_size("row")
    col_count = lax.axis_size("col")
    scenes = tile_map.shape[0]
    scn, points = partner.shape
    packs = (
        scenes == col_count * HALF
        and scenes == row_count * LANES
        and scn == row_count * 4
        and LANES % scn == 0
        and points % LANES == 0
        and col_count >= 7
    )
    run = packed_shards if packs else plain_shards
    return run(cam_jac, pt_jac, resid, partner, count, tile_map)


def solution(mesh):
    return jax.shard_map(
        shards,
        mesh=mesh,
        in_specs=(
            P(None, None, None, AXES, None),
            P(None, None, None, AXES, None),
            P(None, None, AXES, None),
            P(AXES, None),
            P(AXES),
            P(),
        ),
        out_specs=(P(None, None, "row", "col"), P(None, "row"), P(None, "row")),
        check_vma=False,
    )
```
